16 devices in a mesh: fsdp: 16 (over z, y, x, core).
Axes of the slice: x: 2, y: 2, z: 2, core: 2. Of those that a mesh axis runs over, the one named last changes fastest.
Arguments:
- hidden: bfloat16 [16, 128, 1024], P('fsdp')
- grad_out: bfloat16 [16, 128, 1024], P('fsdp')
- positions: int32 [16, 128], P('fsdp')
- norm1_gain: bfloat16 [1024], P('fsdp')
- norm2_gain: bfloat16 [1024], P('fsdp')
- q_norm_gain: bfloat16 [128], replicated
- k_norm_gain: bfloat16 [128], replicated
- w_q: bfloat16 [1024, 2048], P('fsdp')
- w_k: bfloat16 [1024, 1024], P('fsdp')
- w_v: bfloat16 [1024, 1024], P('fsdp')
- w_o: bfloat16 [2048, 1024], P('fsdp')
- w_gate: bfloat16 [1024, 3072], P('fsdp')
- w_up: bfloat16 [1024, 3072], P('fsdp')
- w_down: bfloat16 [3072, 1024], P('fsdp')
Outputs:
- output 1: bfloat16 [16, 128, 1024], P('fsdp')
- output 2: bfloat16 [16, 128, 1024], P('fsdp')
- output 3: float32 [1024], P('fsdp')
- output 4: float32 [1024], P('fsdp')
- output 5: float32 [128], replicated
- output 6: float32 [128], replicated
- output 7: float32 [1024, 2048], P('fsdp')
- output 8: float32 [1024, 1024], P('fsdp')
- output 9: float32 [1024, 1024], P('fsdp')
- output 10: float32 [2048, 1024], P('fsdp')
- output 11: float32 [1024, 3072], P('fsdp')
- output 12: float32 [1024, 3072], P('fsdp')
- output 13: float32 [3072, 1024], P('fsdp')
All inputs are finite; a program needn't handle non-finite values.
Results may differ from the reference program's by a relative error of at most 0.02.
Values are sent between devices in bfloat16 or wider.
A program may use at most 1 GiB of HBM per device.

```python
import functools
import jax
import jax.numpy as jnp
from jax import lax

D = 1024
HEADS = 16
KV_HEADS = 8
HEAD = 128
FF = 3072
BATCH = 16
SEQ = 128
RMS_EPS = 1e-6
ROPE_THETA = 1000000.0
KV_GROUP = HEADS // KV_HEADS
TOKENS = BATCH * SEQ


def setup_inputs(seed: int = 0) -> dict:
    key_list = jax.random.split(jax.random.key(seed), 16)

    def normal_draw(key_index, arr_shape, std_scale):
        return (jax.random.normal(key_list[key_index], arr_shape, jnp.float32) * std_scale).astype(jnp.bfloat16)

    def gain_draw(key_index, arr_shape):
        return (1.0 + 0.3 * jax.random.normal(key_list[key_index], arr_shape, jnp.float32)).astype(jnp.bfloat16)

    start_key, stride_key = jax.random.split(key_list[2])
    start_pos = jax.random.randint(start_key, (BATCH, 1), 0, 4096)
    stride_pos = jax.random.randint(stride_key, (BATCH, SEQ), 1, 5)
    positions = (start_pos + jnp.cumsum(stride_pos, axis=1)).astype(jnp.int32)
    return {
        "hidden": normal_draw(0, (BATCH, SEQ, D), 1.0),
        "grad_out": normal_draw(1, (BATCH, SEQ, D), 1.0),
        "positions": positions,
        "norm1_gain": gain_draw(3, (D,)),
        "norm2_gain": gain_draw(4, (D,)),
        "q_norm_gain": gain_draw(5, (HEAD,)),
        "k_norm_gain": gain_draw(6, (HEAD,)),
        "w_q": normal_draw(7, (D, HEADS * HEAD), D ** -0.5),
        "w_k": normal_draw(8, (D, KV_HEADS * HEAD), D ** -0.5),
        "w_v": normal_draw(9, (D, KV_HEADS * HEAD), D ** -0.5),
        "w_o": normal_draw(10, (HEADS * HEAD, D), (HEADS * HEAD) ** -0.5),
        "w_gate": normal_draw(11, (D, FF), D ** -0.5),
        "w_up": normal_draw(12, (D, FF), D ** -0.5),
        "w_down": normal_draw(13, (FF, D), FF ** -0.5),
    }


def rms_scale(tensor):
    return lax.rsqrt(jnp.mean(tensor * tensor, axis=-1, keepdims=True) + RMS_EPS)


def rotate_half(tensor):
    half_dim = tensor.shape[-1] // 2
    return jnp.concatenate([-tensor[..., half_dim:], tensor[..., :half_dim]], axis=-1)


def attend_one(operands):
    q_seq, k_seq, v_seq = operands
    scores = jnp.einsum("skgd,tkd->kgst", q_seq.astype(jnp.float32), k_seq.astype(jnp.float32)) * (HEAD ** -0.5)
    causal = jnp.arange(SEQ)[:, None] >= jnp.arange(SEQ)[None, :]
    scores = jnp.where(causal, scores, -1e30)
    attn_probs = jax.nn.softmax(scores, axis=-1).astype(jnp.bfloat16)
    return jnp.einsum("kgst,tkd->skgd", attn_probs.astype(jnp.float32), v_seq.astype(jnp.float32)).astype(jnp.bfloat16)


def head_norm_rope(projected, num_heads, gain_vec, cos_t, sin_t):
    heads_float = projected.reshape(TOKENS, num_heads, HEAD).astype(jnp.float32)
    scaled = heads_float * rms_scale(heads_float) * gain_vec.astype(jnp.float32)
    return (scaled * cos_t + rotate_half(scaled) * sin_t).astype(jnp.bfloat16)


def layer_forward(positions, hidden, norm1_gain, norm2_gain, q_norm_gain, k_norm_gain, w_q, w_k, w_v, w_o, w_gate, w_up, w_down):
    x_float = hidden.reshape(TOKENS, D).astype(jnp.float32)
    normed = (x_float * rms_scale(x_float) * norm1_gain.astype(jnp.float32)).astype(jnp.bfloat16)
    q_proj = jnp.dot(normed, w_q, preferred_element_type=jnp.float32).astype(jnp.bfloat16)
    k_proj = jnp.dot(normed, w_k, preferred_element_type=jnp.float32).astype(jnp.bfloat16)
    v_proj = jnp.dot(normed, w_v, preferred_element_type=jnp.float32).astype(jnp.bfloat16)
    inv_freq = ROPE_THETA ** (-2.0 * jnp.arange(HEAD // 2, dtype=jnp.float32) / HEAD)
    rope_angle = positions.reshape(TOKENS, 1).astype(jnp.float32) * inv_freq
    cos_t = jnp.concatenate([jnp.cos(rope_angle), jnp.cos(rope_angle)], axis=-1)[:, None, :]
    sin_t = jnp.concatenate([jnp.sin(rope_angle), jnp.sin(rope_angle)], axis=-1)[:, None, :]
    q_rot = head_norm_rope(q_proj, HEADS, q_norm_gain, cos_t, sin_t)
    k_rot = head_norm_rope(k_proj, KV_HEADS, k_norm_gain, cos_t, sin_t)
    attn_ctx = lax.map(attend_one, (q_rot.reshape(BATCH, SEQ, KV_HEADS, KV_GROUP, HEAD), k_rot.reshape(BATCH, SEQ, KV_HEADS, HEAD), v_proj.reshape(BATCH, SEQ, KV_HEADS, HEAD)))
    attn_out = jnp.dot(attn_ctx.reshape(TOKENS, HEADS * HEAD), w_o, preferred_element_type=jnp.float32).astype(jnp.bfloat16)
    resid_float = (x_float + attn_out.astype(jnp.float32)).astype(jnp.bfloat16).astype(jnp.float32)
    mlp_in = (resid_float * rms_scale(resid_float) * norm2_gain.astype(jnp.float32)).astype(jnp.bfloat16)
    gate_proj = jnp.dot(mlp_in, w_gate, preferred_element_type=jnp.float32).astype(jnp.bfloat16)
    up_proj = jnp.dot(mlp_in, w_up, preferred_element_type=jnp.float32).astype(jnp.bfloat16)
    mlp_act = (jax.nn.silu(gate_proj.astype(jnp.float32)) * up_proj.astype(jnp.float32)).astype(jnp.bfloat16)
    down_proj = jnp.dot(mlp_act, w_down, preferred_element_type=jnp.float32).astype(jnp.bfloat16)
    layer_out = (resid_float + down_proj.astype(jnp.float32)).astype(jnp.bfloat16)
    return layer_out.reshape(BATCH, SEQ, D)


def mean_grad(grad_val):
    return grad_val.astype(jnp.float32) / TOKENS


def reference(hidden, grad_out, positions, norm1_gain, norm2_gain, q_norm_gain, k_norm_gain, w_q, w_k, w_v, w_o, w_gate, w_up, w_down):
    layer_out, pullback = jax.vjp(functools.partial(layer_forward, positions), hidden, norm1_gain, norm2_gain, q_norm_gain, k_norm_gain, w_q, w_k, w_v, w_o, w_gate, w_up, w_down)
    all_grads = pullback(grad_out)
    return (layer_out, all_grads[0].astype(jnp.bfloat16), mean_grad(all_grads[1]), mean_grad(all_grads[2]), mean_grad(all_grads[3]), mean_grad(all_grads[4]), mean_grad(all_grads[5]), mean_grad(all_grads[6]), mean_grad(all_grads[7]), mean_grad(all_grads[8]), mean_grad(all_grads[9]), mean_grad(all_grads[10]), mean_grad(all_grads[11]))
```

```python
import jax
import jax.numpy as jnp
from jax import lax
from jax.experimental import pallas as pl
from jax.experimental.pallas import tpu as pltpu
from jax.sharding import PartitionSpec as P

RMS_EPS = 1e-6
ROPE_THETA = 1000000.0
MESH = pl.DeviceIdType.MESH
F32 = jnp.float32
BF16 = jnp.bfloat16
T = 128
D = 1024
NQ = 2048
FF = 3072
HD = 128
Z, Y, X, C = 0, 1, 2, 3
STRIDE = (8, 4, 2, 1)
ALL = slice(None)
VM = pltpu.VMEM
HIGH_VMEM = 67043328


def nn(left_op, right_op):
    return jnp.dot(left_op, right_op, preferred_element_type=F32)


def nt(left_op, right_op):
    return lax.dot_general(left_op, right_op, (((1,), (1,)), ((), ())), preferred_element_type=F32)


def tn(left_op, right_op):
    return lax.dot_general(left_op, right_op, (((0,), (0,)), ((), ())), preferred_element_type=F32)


def rms(val):
    return lax.rsqrt(jnp.mean(val * val, axis=-1, keepdims=True) + RMS_EPS)


def norm_backward(d_unit, unit_val, scale_val):
    return scale_val * (d_unit - unit_val * jnp.mean(d_unit * unit_val, axis=-1, keepdims=True))


class Place:
    def __init__(self):
        self.me = lax.axis_index("fsdp")
        self.bit = [lax.rem(lax.div(self.me, s), 2) for s in STRIDE]

    def near(self, dim):
        return (self.me + STRIDE[dim] * (1 - 2 * self.bit[dim]),)

    def greet(self, dims):
        barrier = pltpu.get_barrier_semaphore()
        for dim in dims:
            pl.semaphore_signal(barrier, inc=1, device_id=self.near(dim), device_id_type=MESH)
        pl.semaphore_wait(barrier, len(dims))


class Spread:
    def __init__(self, place, src, buf, sub, order, axes, sems, part):
        self.place, self.src, self.buf, self.sub, self.order, self.axes = place, src, buf, sub, order, axes
        self.link_send, self.link_recv, self.core_send, self.core_recv, self.local_sem = sems
        self.part, self.last = part, len(order)

    def block(self, full, flip=None):
        index = []
        for dim in self.axes:
            if dim in full:
                index.append(ALL)
            elif dim == flip:
                index.append(1 - self.place.bit[dim])
            else:
                index.append(self.place.bit[dim])
        return self.buf.at[tuple(index) + self.sub]

    def own(self):
        return pltpu.make_async_copy(self.src.at[self.sub], self.block(()), self.local_sem.at[self.part])

    def link(self, step):
        dst = self.block(self.order[:step])
        return pltpu.make_async_remote_copy(
            src_ref=self.src.at[self.sub] if step == 0 else dst,
            dst_ref=dst,
            send_sem=self.link_send.at[self.part, step],
            recv_sem=self.link_recv.at[self.part, step],
            device_id=self.place.near(self.order[step]),
            device_id_type=MESH,
        )

    def core(self, step):
        dst = self.block(()) if step == 0 else self.block(self.order[: step - 1], self.order[step - 1])
        return pltpu.make_async_remote_copy(
            src_ref=self.src.at[self.sub] if step == 0 else dst,
            dst_ref=dst,
            send_sem=self.core_send.at[self.part, step],
            recv_sem=self.core_recv.at[self.part, step],
            device_id=self.place.near(C),
            device_id_type=MESH,
        )

    def begin(self):
        self.link(0).start()
        self.own().start()
        self.core(0).start()

    def advance(self, step):
        if step == 0:
            self.own().wait()
        self.link(step).wait_recv()
        if step + 1 < self.last:
            self.link(step + 1).start()
        self.core(step + 1).start()

    def arrived(self):
        for step in range(self.last + 1):
            self.core(step).wait_recv()

    def drain(self):
        for step in range(self.last):
            self.link(step).wait_send()
        for step in range(self.last + 1):
            self.core(step).wait_send()


class Group:
    def __init__(self, place, third):
        self.place, self.third = place, third
        self.axes = tuple(dim for dim in (Z, Y, X, C) if dim != third)
        bits = [place.bit[dim] for dim in self.axes]
        self.position = 4 * bits[0] + 2 * bits[1] + bits[2]
        chips = [dim for dim in self.axes if dim != C]
        self.orders = (tuple(chips), tuple(chips[::-1]))

    def members(self):
        flips = [(1, 1, 1), (1, 1, 0), (1, 0, 1), (0, 1, 1), (1, 0, 0), (0, 1, 0), (0, 0, 1), (0, 0, 0)]
        for flip in flips:
            bit = list(self.place.bit)
            for dim, turned in zip(self.axes, flip):
                if turned:
                    bit[dim] = 1 - bit[dim]
            yield bit

    def spot(self, bit):
        first, second, third = (bit[dim] for dim in self.axes)
        return 4 * first + 2 * second + third

    def across(self, bit):
        return tuple(ALL if dim == self.third else bit[dim] for dim in range(4))

    def side(self, mine):
        bit = self.place.bit[self.third]
        return tuple((bit if mine else 1 - bit) if dim == self.third else ALL for dim in range(4))


def device_of(bit):
    return (8 * bit[Z] + 4 * bit[Y] + 2 * bit[X] + bit[C],)


class Exchange:
    def __init__(self, group, number, piece, slot, blocks, sems):
        self.group, self.piece, self.slot, self.blocks = group, piece, slot, blocks
        self.send, self.recv, self.local = (sem.at[number] for sem in sems)

    def own(self):
        return pltpu.make_async_copy(self.piece(self.group.place.bit), self.slot, self.local)

    def begin(self):
        *others, _ = self.group.members()
        for bit in others:
            pltpu.make_async_remote_copy(
                src_ref=self.piece(bit),
                dst_ref=self.slot,
                send_sem=self.send,
                recv_sem=self.recv,
                device_id=device_of(bit),
                device_id_type=MESH,
            ).start()
        self.own().start()

    def arrived(self):
        self.own().wait()
        pltpu.make_async_copy(self.blocks, self.blocks, self.recv).wait()

    def drain(self):
        pltpu.make_async_copy(self.blocks, self.blocks, self.send).wait()


ORDERS = ((X, Y, Z), (Y, Z, X), (Z, X, Y))


def head_forward(proj, gain, cos, sin):
    val = proj.astype(F32)
    scaled = val * rms(val) * gain
    return (scaled * cos + pltpu.roll(scaled, 64, axis=1) * sin).astype(BF16)


def head_backward(d_rot, proj, gain, cos, sin):
    val = proj.astype(F32)
    scale = rms(val)
    unit = val * scale
    d_scaled = d_rot * cos - pltpu.roll(d_rot, 64, axis=1) * sin
    d_gain = jnp.sum(d_scaled * unit, axis=0, keepdims=True)
    return norm_backward(d_scaled * gain, unit, scale).astype(BF16), d_gain


def cols(i, width):
    return pl.ds(pl.multiple_of(i * width, width), width)


def spread_pair(i):
    return lax.div(i, 4), lax.rem(lax.div(i, 2), 2), lax.rem(i, 2)


def layer_kernel(
    x_ref, dy_ref, cos_ref, sin_ref, gq_ref, gk_ref, gains, wq, wk, wv, wo, wg, wu, wd,
    y_ref, dh_ref, oqkv, ogu, owo, owd, ogain,
    gbuf, bq, bk, bv, bo, bg, bu, bd, g1, g2,
    nt_ref, mt_ref, dres_ref, at_ref, ct_ref, dqkv_ref, dgu_ref, gpart_ref,
    nbuf, mbuf, dybuf, drbuf, gubuf, qkvbuf, abuf, cbuf, zgu, zqkv, zwd, zwo, gainbuf,
    link_send, link_recv, core_send, core_recv, local_sem, one_send, one_recv, one_local, far_send, far_recv,
):
    place = Place()
    me = place.me
    sems = (link_send, link_recv, core_send, core_recv, local_sem)
    one = (one_send, one_recv, one_local)
    count = [0]

    def part(src, buf, sub, order, axes=(Z, Y, X, C)):
        made = Spread(place, src, buf, sub, order, axes, sems, count[0])
        count[0] += 1
        return made

    rows_all = (ALL, ALL)
    gain_part = part(gains, gbuf, rows_all, ORDERS[0])
    p_q = part(wq, bq, rows_all, ORDERS[0])
    p_k = part(wk, bk, rows_all, ORDERS[1])
    p_v = part(wv, bv, rows_all, ORDERS[1])
    p_o = part(wo, bo, rows_all, ORDERS[2])
    early = [p_q, p_k, p_v, p_o]
    p_d = [part(wd, bd, (pl.ds(64 * i, 64), ALL), ORDERS[i]) for i in range(3)]
    p_g = [part(wg, bg, (ALL, pl.ds(1024 * i, 1024)), ORDERS[i]) for i in range(3)]
    p_u = [part(wu, bu, (ALL, pl.ds(1024 * i, 1024)), ORDERS[i]) for i in range(3)]
    late = p_d + p_g + p_u

    grp_gu, grp_qkv, grp_row = Group(place, Z), Group(place, Y), Group(place, X)

    def halves(src, buf, group):
        size = src.shape[0] // 2
        return [part(src, buf, (pl.ds(i * size, size), ALL), group.orders[i], group.axes) for i in range(2)]

    p_m = halves(mt_ref, mbuf, grp_gu)
    p_n = halves(nt_ref, nbuf, grp_qkv)
    p_dy = halves(dy_ref, dybuf, grp_row)
    p_dr = halves(dres_ref, drbuf, grp_row)

    def share(number, group, piece, buf):
        return Exchange(group, number, piece, buf.at[group.position], buf.at[pl.ds(0, 7)], one)

    def cols_for(group, ref, width):
        return lambda bit: ref.at[:, pl.ds(pl.multiple_of(group.spot(bit) * width, 128), width)]

    e_gu = share(0, grp_gu, cols_for(grp_gu, dgu_ref, 768), gubuf)
    e_qkv = share(1, grp_qkv, cols_for(grp_qkv, dqkv_ref, 512), qkvbuf)
    e_a = share(2, grp_row, lambda bit: at_ref.at[grp_row.across(bit)], abuf)
    e_c = share(3, grp_row, lambda bit: ct_ref.at[grp_row.across(bit)], cbuf)

    barrier = pltpu.get_barrier_semaphore()

    def other(k):
        return (lax.rem(me + k, 16),)

    def greet(k, _):
        pl.semaphore_signal(barrier, inc=1, device_id=other(k), device_id_type=MESH)
        return 0

    lax.fori_loop(1, 16, greet, 0)
    pl.semaphore_wait(barrier, 15)

    def gain_copy(k):
        return pltpu.make_async_remote_copy(
            src_ref=gpart_ref, dst_ref=gainbuf.at[me], send_sem=one_send.at[9], recv_sem=one_recv.at[9],
            device_id=other(k), device_id_type=MESH,
        )

    def far(group, number, source, target):
        return pltpu.make_async_remote_copy(
            src_ref=source, dst_ref=target, send_sem=far_send.at[number], recv_sem=far_recv.at[number],
            device_id=place.near(group.third), device_id_type=MESH,
        )

    for item in [gain_part] + early + late:
        item.begin()
    for item in [gain_part] + early:
        item.advance(0)
    for item in [gain_part] + early:
        item.advance(1)
    for item in late:
        item.advance(0)

    def local_pass(n_s, q_s, k_s, v_s, qr, kr, probs, ctx, h_s, m_s, gate, act, dact, dm, dres, dctx):
        gain_part.advance(2)
        gain_part.arrived()
        lane = lax.broadcasted_iota(jnp.int32, (8, 128), 1) < 64
        for i in range(8):
            first = gbuf[i // 4, (i // 2) % 2, i % 2, 0]
            second = gbuf[i // 4, (i // 2) % 2, i % 2, 1]
            g1[:, 128 * i : 128 * i + 128] = jnp.where(lane, first, pltpu.roll(second, 64, axis=1))[:1]
            g2[:, 128 * i : 128 * i + 128] = jnp.where(lane, pltpu.roll(first, 64, axis=1), second)[:1]

        def norm_rows(i, _):
            rows = cols(i, 32)
            val = x_ref[rows].astype(F32)
            n_s[rows] = (val * rms(val) * g1[...]).astype(BF16)
            return 0

        lax.fori_loop(0, 4, norm_rows, 0)

        def transpose_into(src, dst, blocks):
            def body(i, _):
                dst[cols(i, 128)] = src[:, cols(i, 128)].astype(F32).T.astype(BF16)
                return 0

            lax.fori_loop(0, blocks, body, 0)

        transpose_into(n_s, nt_ref, 8)

        for item in early:
            item.advance(2)

        def project(src, buf, dst, depth, width, tiles):
            def body(j, _):
                weight = buf[:, :, :, :, :, cols(j, width)].reshape(depth, width)
                dst[:, cols(j, width)] = nn(src[...], weight).astype(BF16)
                return 0

            lax.fori_loop(0, tiles, body, 0)

        p_q.arrived()
        project(n_s, bq, q_s, D, 512, 4)
        p_k.arrived()
        project(n_s, bk, k_s, D, 512, 2)
        p_v.arrived()
        project(n_s, bv, v_s, D, 512, 2)

        cos, sin = cos_ref, sin_ref
        scale = HD ** -0.5

        def attend(j, _):
            kv = cols(j, HD)
            pair = cols(j, 2 * HD)
            k_rot = head_forward(k_s[:, kv], gk_ref[...], cos[...], sin[...])
            kr[:, kv] = k_rot
            q_pair = q_s[:, pair]
            q_rot = jnp.concatenate(
                [head_forward(q_pair[:, HD * i : HD * i + HD], gq_ref[...], cos[...], sin[...]) for i in range(2)], axis=0
            )
            qr[j] = q_rot
            scores = nt(q_rot, k_rot) * scale
            row = lax.rem(lax.broadcasted_iota(jnp.int32, (2 * T, T), 0), T)
            col = lax.broadcasted_iota(jnp.int32, (2 * T, T), 1)
            scores = jnp.where(row >= col, scores, -1e30)
            expd = jnp.exp(scores - jnp.max(scores, axis=-1, keepdims=True))
            prob = expd / jnp.sum(expd, axis=-1, keepdims=True)
            probs[j] = prob
            out = nn(prob.astype(BF16), v_s[:, kv])
            ctx[:, pair] = jnp.concatenate([out[:T], out[T:]], axis=1).astype(BF16)
            return 0

        lax.fori_loop(0, 8, attend, 0)
        for item in late:
            item.advance(1)

        def ctx_turned(i, _):
            ct_ref[spread_pair(i)] = ctx[:, cols(i, 256)].astype(F32).T.astype(BF16).reshape(2, 128, T)
            return 0

        lax.fori_loop(0, 8, ctx_turned, 0)

        p_o.arrived()

        def out_proj(j, _):
            tile = cols(j, 256)
            weight = bo[:, :, :, :, :, tile].reshape(NQ, 256)
            attn = nn(ctx[...], weight).astype(BF16)
            h_s[:, tile] = (x_ref[:, tile].astype(F32) + attn.astype(F32)).astype(BF16).astype(F32)
            return 0

        lax.fori_loop(0, 4, out_proj, 0)

        def norm2_rows(i, _):
            rows = cols(i, 32)
            val = h_s[rows]
            m_s[rows] = (val * rms(val) * g2[...]).astype(BF16)
            return 0

        lax.fori_loop(0, 4, norm2_rows, 0)
        transpose_into(m_s, mt_ref, 8)
        for item in p_m + p_dy + p_n:
            item.begin()
        e_c.begin()

        for item in p_d:
            item.advance(2)
        for item in p_d:
            item.arrived()

        def d_act(i, _):
            weight = bd[lax.div(i, 4), lax.rem(lax.div(i, 2), 2), lax.rem(i, 2)].reshape(384, D)
            dact[:, cols(i, 384)] = nt(dy_ref[...], weight)
            return 0

        lax.fori_loop(0, 8, d_act, 0)
        for item in p_g:
            item.advance(2)
        for item in p_g:
            item.arrived()
        project(m_s, bg, gate, D, 512, 6)
        for item in p_u:
            item.advance(2)
        for item in p_u:
            item.arrived()

        def up_tile(j, _):
            tile = cols(j, 256)
            weight = bu[:, :, :, :, :, tile].reshape(D, 256)
            up_val = nn(m_s[...], weight).astype(BF16).astype(F32)
            gate_val = gate[:, tile].astype(F32)
            sig = jax.nn.sigmoid(gate_val)
            act_val = (gate_val * sig * up_val).astype(BF16)
            act[:, tile] = act_val
            d_act_val = dact[:, tile]
            d_gate = (d_act_val * up_val * sig * (1.0 + gate_val * (1.0 - sig))).astype(BF16)
            dgu_ref[:, tile] = d_gate
            dgu_ref[:, cols(j + FF // 256, 256)] = (d_act_val * gate_val * sig).astype(BF16)
            return 0

        lax.fori_loop(0, FF // 256, up_tile, 0)
        e_gu.begin()

        def act_turned(i, _):
            at_ref[spread_pair(i)] = act[:, cols(i, 384)].astype(F32).T.astype(BF16).reshape(2, 192, T)
            return 0

        lax.fori_loop(0, 8, act_turned, 0)
        for item in p_m + p_dy + p_n:
            item.advance(0)
        e_a.begin()

        def d_mlp_in(i, _):
            zi, yi = lax.div(i, 2), lax.rem(i, 2)
            grad = nt(dgu_ref[:, :FF], bg[zi, yi].reshape(256, FF))
            dm[:, cols(i, 256)] = grad + nt(dgu_ref[:, FF:], bu[zi, yi].reshape(256, FF))
            return 0

        lax.fori_loop(0, 4, d_mlp_in, 0)
        for item in p_m + p_dy + p_n:
            item.advance(1)

        def d_res_rows(i, total):
            rows = cols(i, 32)
            val = h_s[rows]
            r_scale = rms(val)
            unit = val * r_scale
            grad = dm[rows]
            out = dy_ref[rows].astype(F32) + norm_backward(grad * g2[...], unit, r_scale)
            dres[rows] = out
            dres_ref[rows] = out.astype(BF16)
            return total + jnp.sum(grad * unit, axis=0, keepdims=True)

        d_g2 = lax.fori_loop(0, 4, d_res_rows, jnp.zeros((1, D), F32))
        for i in range(8):
            gpart_ref[8 + i : 9 + i, :] = d_g2[:, 128 * i : 128 * i + 128]

        for item in p_dr:
            item.begin()

        def d_ctx(i, _):
            weight = bo[lax.div(i, 2), lax.rem(i, 2)].reshape(512, D)
            dctx[:, cols(i, 512)] = nt(dres_ref[...], weight).astype(BF16)
            return 0

        lax.fori_loop(0, 4, d_ctx, 0)
        for item in p_dr:
            item.advance(0)

        def attend_back(j, carry):
            q_total, k_total = carry
            kv = cols(j, HD)
            pair = cols(j, 2 * HD)
            d_out = dctx[:, pair]
            d_out = jnp.concatenate([d_out[:, :HD], d_out[:, HD:]], axis=0)
            prob = probs[j]
            d_value = tn(prob.astype(BF16), d_out).astype(BF16)
            d_prob = nt(d_out, v_s[:, kv])
            d_score = prob * (d_prob - jnp.sum(prob * d_prob, axis=-1, keepdims=True))
            d_score = (d_score * scale).astype(BF16)
            d_q_rot = nn(d_score, kr[:, kv])
            d_k_rot = tn(d_score, qr[j])
            q_pair = q_s[:, pair]
            d_q0, g_q0 = head_backward(d_q_rot[:T], q_pair[:, :HD], gq_ref[...], cos[...], sin[...])
            d_q1, g_q1 = head_backward(d_q_rot[T:], q_pair[:, HD:], gq_ref[...], cos[...], sin[...])
            d_k, g_k = head_backward(d_k_rot, k_s[:, kv], gk_ref[...], cos[...], sin[...])
            dqkv_ref[:, pair] = jnp.concatenate([d_q0, d_q1], axis=1)
            dqkv_ref[:, cols(j + 16, HD)] = d_k
            dqkv_ref[:, cols(j + 24, HD)] = d_value
            return q_total + g_q0 + g_q1, k_total + g_k

        zero = jnp.zeros((1, HD), F32)
        q_total, k_total = lax.fori_loop(0, 8, attend_back, (zero, zero))
        e_qkv.begin()
        for item in p_dr:
            item.advance(1)
        gpart_ref[16:17, :] = q_total
        gpart_ref[17:18, :] = k_total
        gpart_ref[18:24, :] = jnp.zeros((6, 128), F32)

        def d_normed(i, _):
            zi, yi = lax.div(i, 2), lax.rem(i, 2)
            grad = nt(dqkv_ref[:, :NQ], bq[zi, yi].reshape(256, NQ))
            grad += nt(dqkv_ref[:, NQ : NQ + D], bk[zi, yi].reshape(256, D))
            dm[:, cols(i, 256)] = grad + nt(dqkv_ref[:, NQ + D :], bv[zi, yi].reshape(256, D))
            return 0

        lax.fori_loop(0, 4, d_normed, 0)

        def d_hidden_rows(i, total):
            rows = cols(i, 32)
            val = x_ref[rows].astype(F32)
            x_scale = rms(val)
            unit = val * x_scale
            grad = dm[rows]
            dh_ref[rows] = (dres[rows] + norm_backward(grad * g1[...], unit, x_scale)).astype(BF16)
            return total + jnp.sum(grad * unit, axis=0, keepdims=True)

        d_g1 = lax.fori_loop(0, 4, d_hidden_rows, jnp.zeros((1, D), F32))
        for i in range(8):
            gpart_ref[i : i + 1, :] = d_g1[:, 128 * i : 128 * i + 128]

        def gain_send(k, _):
            gain_copy(k).start()
            return 0

        lax.fori_loop(1, 16, gain_send, 0)

        def down(j, _):
            tile = cols(j, 256)
            weight = bd[:, :, :, :, :, tile].reshape(FF, 256)
            out = nn(act[...], weight).astype(BF16).astype(F32)
            y_ref[:, tile] = (h_s[:, tile] + out).astype(BF16)
            return 0

        lax.fori_loop(0, 4, down, 0)

    pl.run_scoped(
        local_pass,
        VM((T, D), BF16), VM((T, NQ), BF16), VM((T, D), BF16), VM((T, D), BF16),
        VM((8, 2 * T, HD), BF16), VM((T, D), BF16), VM((8, 2 * T, T), F32), VM((T, NQ), BF16), VM((T, D), F32),
        VM((T, D), BF16), VM((T, FF), BF16), VM((T, FF), BF16), VM((T, FF), F32),
        VM((T, D), F32), VM((T, D), F32), VM((T, NQ), BF16),
    )

    inv_tokens = 1.0 / (16 * T)

    def lanes(buf, rows):
        blocks = [buf[i // 4, (i // 2) % 2, i % 2, rows] for i in range(8)]
        return jnp.concatenate(blocks, axis=1)

    def gradients(rgu, rqkv, rwd, rwo):
        def column_chunk(acts, grads, out, chunk):
            def tile(i, _):
                right = grads[:, :, 256 * chunk : 256 * chunk + 256].reshape(8 * T, 256)
                block = nn(lanes(acts, cols(i, 128)), right) * inv_tokens
                out[(chunk,) + spread_pair(i)] = block.reshape(2, 64, 256)
                return 0

            lax.fori_loop(0, 8, tile, 0)

        def send_chunk(group, result, target, chunk, number):
            return far(group, number, result.at[(chunk,) + group.side(False)], target.at[chunk])

        for item in p_m:
            item.arrived()
        e_gu.arrived()
        gu_far = [send_chunk(grp_gu, rgu, zgu, chunk, chunk) for chunk in range(3)]
        for chunk in range(3):
            column_chunk(mbuf, gubuf, rgu, chunk)
            gu_far[chunk].start()

        for item in p_dy:
            item.arrived()
        e_a.arrived()
        e_c.arrived()

        def row_tile(left_buf, right_buf, out, height):
            def body(j, _):
                tile = cols(lax.rem(j, 4), 256)
                half = lax.div(j, 4)
                left = jnp.concatenate([left_buf[i, half] for i in range(8)], axis=1)
                right = right_buf[:, :, :, :, tile].reshape(8 * T, 256)
                out[half, :, tile] = nn(left, right) * inv_tokens
                return 0

            lax.fori_loop(0, 8, body, 0)

        side = place.bit[X]
        row_tile(abuf, dybuf, rwd, 192)
        wd_far = far(grp_row, 5, rwd.at[1 - side], zwd)
        wd_far.start()

        for item in p_n:
            item.arrived()
        e_qkv.arrived()
        qkv_far = [send_chunk(grp_qkv, rqkv, zqkv, chunk, 3 + chunk) for chunk in range(2)]
        for chunk in range(2):
            column_chunk(nbuf, qkvbuf, rqkv, chunk)
            qkv_far[chunk].start()

        for item in p_dr:
            item.arrived()
        row_tile(cbuf, drbuf, rwo, 128)
        wo_far = far(grp_row, 6, rwo.at[1 - side], zwo)
        wo_far.start()

        def final(group, number, result, target, out, chunk, width):
            for bit in group.members():
                index = (chunk,) + tuple(bit)
                result[index] = result[index] + target[(chunk,) + tuple(bit[dim] for dim in group.axes)]
            where = pl.ds(pl.multiple_of(group.position * width + 256 * chunk, 128), 256)
            move = Exchange(
                group, number, lambda bit: result.at[(chunk,) + tuple(bit)], out.at[:, where],
                out.at[:, pl.ds(0, 7 * 256)], one,
            )
            move.begin()
            return move

        moves = []
        for kind, chunk in ((0, 0), (1, 0), (0, 1), (1, 1), (0, 2)):
            if kind == 0:
                gu_far[chunk].wait_recv()
                moves.append(final(grp_gu, 4 + chunk, rgu, zgu, ogu, chunk, 768))
            else:
                qkv_far[chunk].wait_recv()
                moves.append(final(grp_qkv, 7 + chunk, rqkv, zqkv, oqkv, chunk, 512))
        wd_far.wait_recv()
        owd[...] = rwd[side] + zwd[...]
        wo_far.wait_recv()
        owo[...] = rwo[side] + zwo[...]

        pltpu.make_async_copy(gainbuf.at[pl.ds(0, 15)], gainbuf.at[pl.ds(0, 15)], one_recv.at[9]).wait()
        gainbuf[me] = gpart_ref[...]
        total = gainbuf[0]
        for i in range(1, 16):
            total = total + gainbuf[i]
        ogain[...] = total * inv_tokens
        for move in moves:
            move.arrived()
            move.drain()
        for copy in gu_far + qkv_far + [wd_far, wo_far]:
            copy.wait_send()

    pl.run_scoped(
        gradients,
        VM((3, 2, 2, 2, 2, 64, 256), F32), VM((2, 2, 2, 2, 2, 64, 256), F32), VM((2, 192, D), F32), VM((2, 128, D), F32),
    )
    pltpu.make_async_copy(gainbuf.at[pl.ds(0, 15)], gainbuf.at[pl.ds(0, 15)], one_send.at[9]).wait()
    for item in (e_gu, e_qkv, e_a, e_c):
        item.drain()
    for item in [gain_part] + early + late + p_m + p_n + p_dy + p_dr:
        item.drain()


def gather_sems(parts):
    dma = pltpu.SemaphoreType.DMA
    return [dma((parts, 3)), dma((parts, 3)), dma((parts, 4)), dma((parts, 4)), dma((parts,))]


def cube(rows, width, dtype):
    return VM((2, 2, 2, 2, rows, width), dtype)


def square(rows, width):
    return VM((2, 2, 2, rows, width), BF16)


def shape(rows, width, dtype):
    return jax.ShapeDtypeStruct((rows, width), dtype)


def layer_call(x, dy, cos, sin, gq, gk, gains, *weights):
    vmem = pl.BlockSpec(memory_space=VM)
    hbm = pl.BlockSpec(memory_space=pl.ANY)
    dma = pltpu.SemaphoreType.DMA
    return pl.pallas_call(
        layer_kernel,
        name="layer",
        out_shape=(
            shape(T, D, BF16), shape(T, D, BF16), shape(64, NQ + 2 * D, F32), shape(64, 2 * FF, F32),
            shape(128, D, F32), shape(192, D, F32), shape(24, 128, F32),
        ),
        in_specs=[vmem] * 6 + [hbm] * 8,
        out_specs=(vmem, vmem, hbm, hbm, vmem, vmem, vmem),
        scratch_shapes=[
            cube(8, 128, F32), cube(64, NQ, BF16), cube(64, D, BF16), cube(64, D, BF16), cube(128, D, BF16),
            cube(64, FF, BF16), cube(64, FF, BF16), cube(192, D, BF16), VM((1, D), F32), VM((1, D), F32),
            VM((D, T), BF16), VM((D, T), BF16), VM((T, D), BF16), cube(192, T, BF16), cube(128, T, BF16),
            VM((T, NQ + 2 * D), BF16), VM((T, 2 * FF), BF16), VM((24, 128), F32),
            square(D, T), square(D, T), square(T, D), square(T, D),
            VM((8, T, 768), BF16), VM((8, T, 512), BF16), VM((8, 2, 192, T), BF16), VM((8, 2, 128, T), BF16),
            VM((3, 2, 2, 2, 64, 256), F32), VM((2, 2, 2, 2, 64, 256), F32), VM((192, D), F32), VM((128, D), F32),
            VM((16, 24, 128), F32),
        ] + gather_sems(22) + [dma((10,)), dma((10,)), dma((10,)), dma((7,)), dma((7,))],
        compiler_params=pltpu.CompilerParams(collective_id=0, has_side_effects=True, vmem_limit_bytes=HIGH_VMEM),
    )(x, dy, cos, sin, gq, gk, gains, *weights)


def rope_tables(positions):
    inv_freq = ROPE_THETA ** (-2.0 * jnp.arange(HD // 2, dtype=F32) / HD)
    angle = positions.reshape(-1, 1).astype(F32) * inv_freq
    cos_half, sin_half = jnp.cos(angle), jnp.sin(angle)
    return jnp.concatenate([cos_half, cos_half], axis=-1), jnp.concatenate([-sin_half, sin_half], axis=-1)


def solution(mesh):
    axis_name = mesh.axis_names[0]
    sharded = P(axis_name)
    in_specs = (sharded,) * 5 + (P(), P()) + (sharded,) * 7
    out_specs = (sharded,) * 4 + (P(), P()) + (sharded,) * 7

    def device_step(hidden, grad_out, positions, norm1, norm2, gain_q, gain_k, w_q, w_k, w_v, w_o, w_gate, w_up, w_down):
        cos, sin = rope_tables(positions)
        gains = jnp.broadcast_to(jnp.concatenate([norm1, norm2]).astype(F32)[None, :], (8, 128))
        x, dy = hidden.reshape(T, D), grad_out.reshape(T, D)
        gq, gk = gain_q.astype(F32)[None, :], gain_k.astype(F32)[None, :]
        out, d_hidden, d_qkv, d_gate_up, d_wo, d_wd, g_sum = layer_call(
            x, dy, cos, sin, gq, gk, gains, w_q, w_k, w_v, w_o, w_gate, w_up, w_down
        )
        start = lax.axis_index(axis_name) * 64
        d_norm1 = lax.dynamic_slice(g_sum[:8].reshape(D), (start,), (64,))
        d_norm2 = lax.dynamic_slice(g_sum[8:16].reshape(D), (start,), (64,))
        return (
            out.reshape(hidden.shape), d_hidden.reshape(hidden.shape), d_norm1, d_norm2, g_sum[16], g_sum[17],
            d_qkv[:, :NQ], d_qkv[:, NQ : NQ + D], d_qkv[:, NQ + D :], d_wo, d_gate_up[:, :FF], d_gate_up[:, FF:], d_wd,
        )

    return jax.shard_map(device_step, mesh=mesh, in_specs=in_specs, out_specs=out_specs, check_vma=False)
```

```python
import jax
import jax.numpy as jnp
from jax import lax
from jax.experimental import pallas as pl
from jax.experimental.pallas import tpu as pltpu
from jax.sharding import PartitionSpec as P

RMS_EPS = 1e-6
ROPE_THETA = 1000000.0
MESH = pl.DeviceIdType.MESH
F32 = jnp.float32
BF16 = jnp.bfloat16
T = 128
D = 1024
NQ = 2048
FF = 3072
HD = 128
Z, Y, X, C = 0, 1, 2, 3
STRIDE = (8, 4, 2, 1)
ALL = slice(None)
VM = pltpu.VMEM
HIGH_VMEM = 67043328


def nn(left_op, right_op):
    return jnp.dot(left_op, right_op, preferred_element_type=F32)


def nt(left_op, right_op):
    return lax.dot_general(left_op, right_op, (((1,), (1,)), ((), ())), preferred_element_type=F32)


def tn(left_op, right_op):
    return lax.dot_general(left_op, right_op, (((0,), (0,)), ((), ())), preferred_element_type=F32)


def rms(val):
    return lax.rsqrt(jnp.mean(val * val, axis=-1, keepdims=True) + RMS_EPS)


def norm_backward(d_unit, unit_val, scale_val):
    return scale_val * (d_unit - unit_val * jnp.mean(d_unit * unit_val, axis=-1, keepdims=True))


class Place:
    def __init__(self):
        self.me = lax.axis_index("fsdp")
        self.bit = [lax.rem(lax.div(self.me, s), 2) for s in STRIDE]

    def near(self, dim):
        return (self.me + STRIDE[dim] * (1 - 2 * self.bit[dim]),)

    def greet(self, dims):
        barrier = pltpu.get_barrier_semaphore()
        for dim in dims:
            pl.semaphore_signal(barrier, inc=1, device_id=self.near(dim), device_id_type=MESH)
        pl.semaphore_wait(barrier, len(dims))


class Spread:
    def __init__(self, place, own, first, buf, sub, order, axes, sems, part):
        self.place, self.buf, self.sub, self.order, self.axes = place, buf, sub, order, axes
        self.link_send, self.link_recv, self.core_send, self.core_recv, self.local_sem = sems
        self.part, self.last = part, len(order)
        self.source = own
        self.mine = self.block(()) if own is None else own
        self.first = self.mine if first is None else first

    def block(self, full, flip=None):
        index = []
        for dim in self.axes:
            if dim in full:
                index.append(ALL)
            elif dim == flip:
                index.append(1 - self.place.bit[dim])
            else:
                index.append(self.place.bit[dim])
        return self.buf.at[tuple(index) + self.sub]

    def copy_own(self):
        return pltpu.make_async_copy(self.source, self.block(()), self.local_sem.at[self.part])

    def link(self, step):
        dst = self.block(self.order[:step])
        return pltpu.make_async_remote_copy(
            src_ref=self.first if step == 0 else dst,
            dst_ref=dst,
            send_sem=self.link_send.at[self.part, step],
            recv_sem=self.link_recv.at[self.part, step],
            device_id=self.place.near(self.order[step]),
            device_id_type=MESH,
        )

    def core(self, step):
        dst = self.block(()) if step == 0 else self.block(self.order[: step - 1], self.order[step - 1])
        return pltpu.make_async_remote_copy(
            src_ref=self.mine if step == 0 else dst,
            dst_ref=dst,
            send_sem=self.core_send.at[self.part, step],
            recv_sem=self.core_recv.at[self.part, step],
            device_id=self.place.near(C),
            device_id_type=MESH,
        )

    def begin(self):
        self.link(0).start()
        if self.source is not None:
            self.copy_own().start()
        self.core(0).start()

    def advance(self, step):
        if step == 0 and self.source is not None:
            self.copy_own().wait()
        self.link(step).wait_recv()
        if step + 1 < self.last:
            self.link(step + 1).start()
        self.core(step + 1).start()

    def arrived(self):
        for step in range(self.last + 1):
            self.core(step).wait_recv()

    def drain(self):
        for step in range(self.last):
            self.link(step).wait_send()
        for step in range(self.last + 1):
            self.core(step).wait_send()


class Group:
    def __init__(self, place, axes):
        self.place, self.axes = place, axes
        self.position = self.spot(place.bit)

    def others(self):
        for number in range(2 ** len(self.axes) - 1, 0, -1):
            bit = list(self.place.bit)
            for i, dim in enumerate(self.axes):
                if number >> i & 1:
                    bit[dim] = 1 - bit[dim]
            yield bit

    def spot(self, bit):
        total = 0
        for dim in self.axes:
            total = total * 2 + bit[dim]
        return total


def device_of(bit):
    return (sum(stride * value for stride, value in zip(STRIDE, bit)),)


class Exchange:
    def __init__(self, group, number, piece, slot, blocks, sems):
        self.group, self.piece, self.slot, self.blocks = group, piece, slot, blocks
        self.send, self.recv, self.local = (sem.at[number] for sem in sems)

    def own(self):
        return pltpu.make_async_copy(self.piece(self.group.place.bit), self.slot, self.local)

    def begin(self):
        for bit in self.group.others():
            pltpu.make_async_remote_copy(
                src_ref=self.piece(bit),
                dst_ref=self.slot,
                send_sem=self.send,
                recv_sem=self.recv,
                device_id=device_of(bit),
                device_id_type=MESH,
            ).start()
        self.own().start()

    def arrived(self):
        self.own().wait()
        pltpu.make_async_copy(self.blocks, self.blocks, self.recv).wait()

    def drain(self):
        pltpu.make_async_copy(self.blocks, self.blocks, self.send).wait()


def head_forward(proj, gain, cos, sin):
    val = proj.astype(F32)
    scaled = val * rms(val) * gain
    return (scaled * cos + pltpu.roll(scaled, 64, axis=1) * sin).astype(BF16)


def head_backward(d_rot, proj, gain, cos, sin):
    val = proj.astype(F32)
    scale = rms(val)
    unit = val * scale
    d_scaled = d_rot * cos - pltpu.roll(d_rot, 64, axis=1) * sin
    d_gain = jnp.sum(d_scaled * unit, axis=0, keepdims=True)
    return norm_backward(d_scaled * gain, unit, scale).astype(BF16), d_gain


def cols(i, width):
    return pl.ds(pl.multiple_of(i * width, width), width)


def loop(count, body, init=0):
    return lax.fori_loop(0, count, body, init)


def each(count):
    def run(body):
        def step(i, _):
            body(i)
            return 0

        loop(count, step)

    return run


def two(i):
    return lax.div(i, 2), lax.rem(i, 2)


def three(i):
    return two(lax.div(i, 2)) + (lax.rem(i, 2),)


def layer_kernel(
    x_ref, dy_ref, trig_ref, gq_ref, gk_ref, gains, wq, wk, wv, wo, wg, wu, wd,
    y_ref, dh_ref, oqkv, ogu, owo, owd, ogain,
    gbuf, bq, bk, bv, bo, bg, bu, bd, g1, g2,
    xp, trig, n_s, q_s, k_s, v_s, qr, kr, probs, ctx, h_s, m_s, spare, act, dact, dctx, dres,
    part_a, part_y, part_m, part_n, land_a, land_y, land_m, land_n,
    at_ref, ct_ref, dqkv, dgu, gpart,
    nbuf, mbuf, dybuf, drbuf, gubuf, qkvbuf, abuf, cbuf,
    rgu, rqkv, rwd, rwo, zgu, zqkv, zwd, zwo, gainbuf,
    link_send, link_recv, core_send, core_recv, local_sem, one_send, one_recv, one_local, far_send, far_recv,
):
    place = Place()
    me = place.me
    z, y, x, c = place.bit
    sems = (link_send, link_recv, core_send, core_recv, local_sem)
    one = (one_send, one_recv, one_local)
    parts = []

    def spread(own, first, buf, sub, order, axes):
        parts.append(Spread(place, own, first, buf, sub, order, axes, sems, len(parts)))
        return parts[-1]

    both = (ALL, ALL)
    turns = ((Y, X), (X, Y))

    def by_columns(src, buf):
        half = src.shape[1] // 2
        size = half // 2
        made = []
        for i in range(2):
            mine, theirs = (src.at[:, pl.ds(pl.multiple_of(side * half + i * size, size), size)] for side in (z, 1 - z))
            made.append(spread(mine, theirs, buf, (ALL, pl.ds(i * size, size)), (Z,) + turns[i], (Z, Y, X, C)))
        return made

    def by_rows(src, buf):
        size = src.shape[0] // 2
        made = []
        for i in range(2):
            rows = pl.ds(i * size, size)
            made.append(spread(src.at[rows], None, buf, (rows, ALL), turns[i], (Y, X, C)))
        return made

    gain_part = spread(gains, None, gbuf, both, (X, Y, Z), (Z, Y, X, C))
    p_qkv = by_columns(wq, bq) + by_columns(wk, bk) + by_columns(wv, bv)
    p_o, p_d = by_rows(wo, bo), by_rows(wd, bd)
    p_g, p_u = by_columns(wg, bg), by_columns(wu, bu)
    p_m = spread(None, None, mbuf, both, (X,), (X, C))
    p_n = spread(None, None, nbuf, both, (Y,), (Y, C))
    p_dy = spread(None, None, dybuf, (ALL, ALL, ALL), (Y,), (Y, C))
    p_dr = spread(None, None, drbuf, (ALL, ALL, ALL), (X,), (X, C))

    grp_x, grp_y = Group(place, (X, C)), Group(place, (Y, C))

    def share(number, group, piece, buf):
        return Exchange(group, number, piece, buf.at[group.position], buf.at[pl.ds(0, 3)], one)

    def cols_for(group, ref, width):
        return lambda bit: ref.at[:, pl.ds(pl.multiple_of(group.spot(bit) * width, 128), width)]

    e_gu = share(0, grp_x, cols_for(grp_x, dgu, 768), gubuf)
    e_qkv = share(1, grp_y, cols_for(grp_y, dqkv, 512), qkvbuf)
    e_a = share(2, grp_y, lambda bit: at_ref.at[bit[Y], :, bit[C]], abuf)
    e_c = share(3, grp_x, lambda bit: ct_ref.at[:, bit[X], bit[C]], cbuf)
    gain_number = 9
    sent = []

    def near_copy(dim, source, target):
        number = len(sent)
        sent.append(
            pltpu.make_async_remote_copy(
                src_ref=source, dst_ref=target, send_sem=far_send.at[number], recv_sem=far_recv.at[number],
                device_id=place.near(dim), device_id_type=MESH,
            )
        )
        return sent[-1]

    mine, theirs = cols(z, T), cols(1 - z, T)
    barrier = pltpu.get_barrier_semaphore()

    def other(k):
        return (lax.rem(me + k, 16),)

    @each(15)
    def _(k):
        pl.semaphore_signal(barrier, inc=1, device_id=other(k + 1), device_id_type=MESH)

    pl.semaphore_wait(barrier, 15)

    def gain_copy(k):
        return pltpu.make_async_remote_copy(
            src_ref=gpart, dst_ref=gainbuf.at[me], send_sem=one_send.at[gain_number],
            recv_sem=one_recv.at[gain_number], device_id=other(k), device_id_type=MESH,
        )

    gain_part.begin()
    for item in p_qkv + p_o:
        item.begin()
    x_copy = near_copy(Z, x_ref, xp.at[mine])
    trig_copy = near_copy(Z, trig_ref, trig.at[z])
    x_copy.start()
    trig_copy.start()
    xp[mine] = x_ref[...]
    trig[z] = trig_ref[...]
    for step in range(3):
        gain_part.advance(step)
    for item in p_o + p_qkv:
        item.advance(0)
    for item in p_g + p_u:
        item.begin()
    dy_copy = near_copy(Z, dy_ref, dybuf.at[y, c, z])
    dy_copy.start()
    dybuf[y, c, z] = dy_ref[...]
    gain_part.arrived()
    lane = lax.broadcasted_iota(jnp.int32, (8, 128), 1) < 64
    for i in range(8):
        first, second = gbuf[i // 4, (i // 2) % 2, i % 2, 0], gbuf[i // 4, (i // 2) % 2, i % 2, 1]
        tile = slice(128 * i, 128 * i + 128)
        g1[:, tile] = jnp.where(lane, first, pltpu.roll(second, 64, axis=1))[:1]
        g2[:, tile] = jnp.where(lane, pltpu.roll(first, 64, axis=1), second)[:1]
    for item in p_qkv:
        item.advance(1)
    x_copy.wait_recv()

    @each(8)
    def _(i):
        rows = cols(i, 32)
        val = xp[rows].astype(F32)
        n_s[rows] = (val * rms(val) * g1[...]).astype(BF16)

    def turned(val):
        return val.astype(F32).T.astype(BF16)

    for item in p_o:
        item.advance(1)
    for item in p_d:
        item.begin()

    @each(4)
    def _(i):
        nbuf[y, c, cols(i, 256)] = turned(n_s[:, cols(i, 256)])

    for item in p_qkv:
        item.advance(2)
    for item in p_d + p_g + p_u:
        item.advance(0)
    trig_copy.wait_recv()

    def weight(buf, tile):
        block = buf[(ALL,) * (len(buf.shape) - 1) + (tile,)]
        return block.reshape(-1, block.shape[-1])

    def project(buf, dst, width, tiles):
        @each(tiles)
        def _(j):
            tile = cols(j, width)
            dst[:, tile] = nn(n_s[...], weight(buf, tile)).astype(BF16)

    for item in p_qkv:
        item.arrived()
    project(bq, q_s, 512, 2)
    project(bk, k_s, 512, 1)
    project(bv, v_s, 512, 1)
    scale = HD ** -0.5

    def sequence_head(j):
        seq, head = lax.div(j, 4), lax.rem(j, 4)
        return seq, head, cols(seq, T), cols(head, HD), cols(head, 2 * HD)

    @each(8)
    def _(j):
        seq, _, rows, kv, pair = sequence_head(j)
        cos, sin = trig[seq, :, :HD], trig[seq, :, HD:]
        k_rot = head_forward(k_s[rows, kv], gk_ref[...], cos, sin)
        kr[rows, kv] = k_rot
        q_pair = q_s[rows, pair]
        q_rot = jnp.concatenate(
            [head_forward(half, gq_ref[...], cos, sin) for half in (q_pair[:, :HD], q_pair[:, HD:])], axis=0
        )
        qr[j] = q_rot
        scores = nt(q_rot, k_rot) * scale
        row = lax.rem(lax.broadcasted_iota(jnp.int32, (2 * T, T), 0), T)
        col = lax.broadcasted_iota(jnp.int32, (2 * T, T), 1)
        scores = jnp.where(row >= col, scores, -1e30)
        expd = jnp.exp(scores - jnp.max(scores, axis=-1, keepdims=True))
        prob = expd / jnp.sum(expd, axis=-1, keepdims=True)
        probs[j] = prob
        out = nn(prob.astype(BF16), v_s[rows, kv])
        ctx[rows, pair] = jnp.concatenate([out[:T], out[T:]], axis=1).astype(BF16)

    def pair_sum(partial, landing, compute):
        copies = []
        for half in range(2):
            @each(2)
            def _(j):
                i = j + 2 * half
                partial[:, :, cols(i, 256)] = compute(i).reshape(2, T, 256)

            span = (ALL, pl.ds(512 * half, 512))
            copies.append(near_copy(Z, partial.at[(1 - z,) + span], landing.at[span]))
            copies[-1].start()
        return copies

    def received(copies):
        for copy in copies:
            copy.wait_recv()

    for item in p_o:
        item.arrived()
    a_copies = pair_sum(part_a, land_a, lambda i: nn(ctx[...], weight(bo, cols(i, 256))))
    for item in p_g + p_u:
        item.advance(1)
    for item in p_d:
        item.advance(1)

    @each(4)
    def _(i):
        ct_ref[two(i)] = turned(ctx[:, cols(i, 256)]).reshape(2, 128, 2 * T)

    received(a_copies)

    @each(4)
    def _(i):
        rows = cols(i, 32)
        attn = (part_a[z, rows] + land_a[rows]).astype(BF16)
        val = (x_ref[rows].astype(F32) + attn.astype(F32)).astype(BF16).astype(F32)
        h_s[rows] = val
        m_s[pl.ds(pl.multiple_of(z * T + i * 32, 32), 32)] = (val * rms(val) * g2[...]).astype(BF16)

    m_copy = near_copy(Z, m_s.at[mine], m_s.at[mine])
    m_copy.start()
    for item in p_d:
        item.arrived()
    dy_copy.wait_recv()

    @each(4)
    def _(i):
        dact[:, cols(i, 384)] = nt(dybuf[y, c].reshape(2 * T, D), bd[two(i)].reshape(384, D))

    for item in p_g + p_u:
        item.advance(2)
    m_copy.wait_recv()
    for item in p_g + p_u:
        item.arrived()
    fh = FF // 2

    @each(fh // 256)
    def _(j):
        tile = cols(j, 256)
        gate_val = nn(m_s[...], weight(bg, tile)).astype(BF16).astype(F32)
        up_val = nn(m_s[...], weight(bu, tile)).astype(BF16).astype(F32)
        sig = jax.nn.sigmoid(gate_val)
        act[:, tile] = (gate_val * sig * up_val).astype(BF16)
        d_act = dact[:, tile]
        dgu[:, tile] = (d_act * up_val * sig * (1.0 + gate_val * (1.0 - sig))).astype(BF16)
        dgu[:, cols(j + fh // 256, 256)] = (d_act * gate_val * sig).astype(BF16)

    def d_mlp_in(i):
        rows = two(i)
        return nt(dgu[:, :fh], bg[rows].reshape(256, fh)) + nt(dgu[:, fh:], bu[rows].reshape(256, fh))

    m_copies = pair_sum(part_m, land_m, d_mlp_in)
    e_gu.begin()

    @each(4)
    def _(i):
        mbuf[x, c, cols(i, 256)] = turned(m_s[:, cols(i, 256)])

    p_m.begin()
    p_n.begin()
    p_dy.begin()

    @each(4)
    def _(i):
        at_ref[two(i)] = turned(act[:, cols(i, 384)]).reshape(2, 192, 2 * T)

    e_a.begin()
    e_c.begin()
    received(m_copies)

    def d_res_rows(i, total):
        rows = cols(i, 32)
        val = h_s[rows]
        r_scale = rms(val)
        unit = val * r_scale
        grad = part_m[z, rows] + land_m[rows]
        out = dy_ref[rows].astype(F32) + norm_backward(grad * g2[...], unit, r_scale)
        dres[rows] = out
        drbuf[x, c, z, rows] = out.astype(BF16)
        return total + jnp.sum(grad * unit, axis=0, keepdims=True)

    d_g2 = loop(4, d_res_rows, jnp.zeros((1, D), F32))
    r_copy = near_copy(Z, drbuf.at[x, c, z], drbuf.at[x, c, z])
    r_copy.start()
    y_copies = pair_sum(part_y, land_y, lambda i: nn(act[...], weight(bd, cols(i, 256))))
    r_copy.wait_recv()
    p_dr.begin()

    @each(2)
    def _(i):
        dctx[:, cols(i, 512)] = nt(drbuf[x, c].reshape(2 * T, D), bo[i].reshape(512, D)).astype(BF16)

    def attend_back(j, carry):
        q_total, k_total = carry
        seq, head, rows, kv, pair = sequence_head(j)
        cos, sin = trig[seq, :, :HD], trig[seq, :, HD:]
        d_out = dctx[rows, pair]
        d_out = jnp.concatenate([d_out[:, :HD], d_out[:, HD:]], axis=0)
        prob = probs[j]
        d_value = tn(prob.astype(BF16), d_out).astype(BF16)
        d_prob = nt(d_out, v_s[rows, kv])
        d_score = prob * (d_prob - jnp.sum(prob * d_prob, axis=-1, keepdims=True))
        d_score = (d_score * scale).astype(BF16)
        d_q_rot = nn(d_score, kr[rows, kv])
        d_k_rot = tn(d_score, qr[j])
        q_pair = q_s[rows, pair]
        d_q0, g_q0 = head_backward(d_q_rot[:T], q_pair[:, :HD], gq_ref[...], cos, sin)
        d_q1, g_q1 = head_backward(d_q_rot[T:], q_pair[:, HD:], gq_ref[...], cos, sin)
        d_k, g_k = head_backward(d_k_rot, k_s[rows, kv], gk_ref[...], cos, sin)
        dqkv[rows, pair] = jnp.concatenate([d_q0, d_q1], axis=1)
        dqkv[rows, cols(head + 8, HD)] = d_k
        dqkv[rows, cols(head + 12, HD)] = d_value
        return q_total + g_q0 + g_q1, k_total + g_k

    zero = jnp.zeros((1, HD), F32)
    q_total, k_total = loop(8, attend_back, (zero, zero))
    e_qkv.begin()

    def d_normed(i):
        rows = two(i)
        grad = nt(dqkv[:, :D], bq[rows].reshape(256, D)) + nt(dqkv[:, D : D + 512], bk[rows].reshape(256, 512))
        return grad + nt(dqkv[:, D + 512 :], bv[rows].reshape(256, 512))

    n_copies = pair_sum(part_n, land_n, d_normed)
    inv_tokens = 1.0 / (16 * T)

    def column_chunk(acts, grads, out, chunk):
        @each(8)
        def _(i):
            rows = cols(i, 128)
            left = jnp.concatenate([acts[k // 2, k % 2, rows] for k in range(4)], axis=1)
            right = grads[:, :, 256 * chunk : 256 * chunk + 256].reshape(8 * T, 256)
            out[(chunk,) + three(i)] = (nn(left, right) * inv_tokens).reshape(2, 64, 256)

    def half_of(dim, result, chunk):
        bit = place.bit[dim]
        return result.at[(chunk,) + tuple(1 - bit if k == dim else ALL for k in range(4))]

    def row_tiles(left_buf, right_buf, out):
        @each(8)
        def _(j):
            tile = cols(lax.rem(j, 4), 256)
            half = lax.div(j, 4)
            left = jnp.concatenate([left_buf[i, half] for i in range(4)], axis=1)
            out[half, :, tile] = nn(left, weight(right_buf, tile)) * inv_tokens

    p_m.advance(0)
    p_n.advance(0)
    p_dy.advance(0)
    p_dr.advance(0)
    p_m.arrived()
    e_gu.arrived()
    gu_far = []
    for chunk in range(3):
        column_chunk(mbuf, gubuf, rgu, chunk)
        gu_far.append(near_copy(Y, half_of(Y, rgu, chunk), zgu.at[chunk]))
        gu_far[-1].start()
    p_n.arrived()
    e_qkv.arrived()
    qkv_far = []
    for chunk in range(2):
        column_chunk(nbuf, qkvbuf, rqkv, chunk)
        qkv_far.append(near_copy(X, half_of(X, rqkv, chunk), zqkv.at[chunk]))
        qkv_far[-1].start()
    p_dy.arrived()
    e_a.arrived()
    row_tiles(abuf, dybuf, rwd)
    wd_far = near_copy(X, rwd.at[1 - x], zwd)
    wd_far.start()
    p_dr.arrived()
    e_c.arrived()
    row_tiles(cbuf, drbuf, rwo)
    wo_far = near_copy(Y, rwo.at[1 - y], zwo)
    wo_far.start()

    received(n_copies)

    def d_hidden_rows(i, total):
        rows = cols(i, 32)
        val = x_ref[rows].astype(F32)
        x_scale = rms(val)
        unit = val * x_scale
        grad = part_n[z, rows] + land_n[rows]
        dh_ref[rows] = (dres[rows] + norm_backward(grad * g1[...], unit, x_scale)).astype(BF16)
        return total + jnp.sum(grad * unit, axis=0, keepdims=True)

    d_g1 = loop(4, d_hidden_rows, jnp.zeros((1, D), F32))
    for i in range(8):
        tile = slice(128 * i, 128 * i + 128)
        gpart[i : i + 1, :] = d_g1[:, tile]
        gpart[8 + i : 9 + i, :] = d_g2[:, tile]
    gpart[16:17, :] = q_total
    gpart[17:18, :] = k_total
    gpart[18:24, :] = jnp.zeros((6, 128), F32)

    @each(15)
    def _(k):
        gain_copy(k + 1).start()

    received(y_copies)

    @each(4)
    def _(i):
        rows = cols(i, 32)
        out = (part_y[z, rows] + land_y[rows]).astype(BF16).astype(F32)
        y_ref[rows] = (h_s[rows] + out).astype(BF16)

    def final(dim, number, result, target, out, chunk, base):
        group = Group(place, tuple(k for k in range(4) if k != dim))
        for bit in list(group.others()) + [place.bit]:
            index = (chunk,) + tuple(bit)
            result[index] = result[index] + target[(chunk,) + tuple(bit[k] for k in group.axes)]
        where = pl.ds(pl.multiple_of(base + 256 * chunk, 128), 256)
        move = Exchange(
            group, number, lambda bit: result.at[(chunk,) + tuple(bit)], out.at[:, where],
            out.at[:, pl.ds(0, 7 * 256)], one,
        )
        move.begin()
        return move

    gu_base = x * FF + z * fh + c * 768
    qkv_base = (1 - y) * (z * D + c * 512) + y * (NQ + c * D + z * 512)
    moves = []
    for kind, chunk in ((0, 0), (1, 0), (0, 1), (1, 1), (0, 2)):
        if kind == 0:
            gu_far[chunk].wait_recv()
            moves.append(final(Y, 4 + chunk, rgu, zgu, ogu, chunk, gu_base))
        else:
            qkv_far[chunk].wait_recv()
            moves.append(final(X, 7 + chunk, rqkv, zqkv, oqkv, chunk, qkv_base))
    wd_far.wait_recv()
    owd[...] = rwd[x] + zwd[...]
    wo_far.wait_recv()
    owo[...] = rwo[y] + zwo[...]
    fifteen = gainbuf.at[pl.ds(0, 15)]
    pltpu.make_async_copy(fifteen, fifteen, one_recv.at[gain_number]).wait()
    gainbuf[me] = gpart[...]
    ogain[...] = loop(16, lambda i, total: total + gainbuf[i], jnp.zeros((24, 128), F32)) * inv_tokens
    for move in moves:
        move.arrived()
    for item in moves + [e_gu, e_qkv, e_a, e_c] + parts:
        item.drain()
    for copy in sent:
        copy.wait_send()
    pltpu.make_async_copy(fifteen, fifteen, one_send.at[gain_number]).wait()


def shape(rows, width, dtype):
    return jax.ShapeDtypeStruct((rows, width), dtype)


def many(count, *args):
    return [VM(*args)] * count


def layer_call(x, dy, trig, gq, gk, gains, *weights):
    vmem = pl.BlockSpec(memory_space=VM)
    hbm = pl.BlockSpec(memory_space=pl.ANY)
    dma = pltpu.SemaphoreType.DMA
    t2, kvh, fh = 2 * T, D // 2, FF // 2
    cube, square, line = (2, 2, 2, 2), (2, 2, 2), (2, 2)
    spreads = 19
    return pl.pallas_call(
        layer_kernel,
        name="layer",
        out_shape=(
            shape(T, D, BF16), shape(T, D, BF16), shape(64, NQ + 2 * D, F32), shape(64, 2 * FF, F32),
            shape(128, D, F32), shape(192, D, F32), shape(24, 128, F32),
        ),
        in_specs=[vmem] * 5 + [hbm] * 8,
        out_specs=(vmem, vmem, hbm, hbm, vmem, vmem, vmem),
        scratch_shapes=[
            VM(cube + (8, 128), F32), VM(cube + (64, D), BF16), *many(2, cube + (64, kvh), BF16),
            VM(square + (128, D), BF16), *many(2, cube + (64, fh), BF16), VM(square + (192, D), BF16),
            *many(2, (1, D), F32),
            VM((t2, D), BF16), VM((2, T, t2), F32), VM((t2, D), BF16), VM((t2, D), BF16), *many(2, (t2, kvh), BF16),
            VM((8, t2, HD), BF16), VM((t2, kvh), BF16), VM((8, t2, T), F32), VM((t2, D), BF16), VM((T, D), F32),
            VM((t2, D), BF16), VM((8, 128), BF16), VM((t2, fh), BF16), VM((t2, fh), F32), VM((t2, D), BF16),
            VM((T, D), F32), *many(4, (2, T, D), F32), *many(4, (T, D), F32),
            VM(square + (192, t2), BF16), VM(square + (128, t2), BF16), VM((t2, NQ), BF16), VM((t2, FF), BF16),
            VM((24, 128), F32), *many(2, line + (D, t2), BF16), *many(2, line + (2, T, D), BF16),
            VM((4, t2, 768), BF16), VM((4, t2, 512), BF16), VM((4, 2, 192, t2), BF16), VM((4, 2, 128, t2), BF16),
            VM((3,) + cube + (64, 256), F32), VM((2,) + cube + (64, 256), F32), VM((2, 192, D), F32),
            VM((2, 128, D), F32), VM((3,) + square + (64, 256), F32), VM((2,) + square + (64, 256), F32),
            VM((192, D), F32), VM((128, D), F32), VM((16, 24, 128), F32),
            *[dma((spreads, 3))] * 2, *[dma((spreads, 4))] * 2, dma((spreads,)), *[dma((10,))] * 3, *[dma((20,))] * 2,
        ],
        compiler_params=pltpu.CompilerParams(collective_id=0, has_side_effects=True, vmem_limit_bytes=HIGH_VMEM),
    )(x, dy, trig, gq, gk, gains, *weights)


def rope_tables(positions):
    inv_freq = ROPE_THETA ** (-2.0 * jnp.arange(HD // 2, dtype=F32) / HD)
    angle = positions.reshape(-1, 1).astype(F32) * inv_freq
    cos_half, sin_half = jnp.cos(angle), jnp.sin(angle)
    return jnp.concatenate([cos_half, cos_half, -sin_half, sin_half], axis=-1)


def solution(mesh):
    axis_name = mesh.axis_names[0]
    sharded = P(axis_name)
    in_specs = (sharded,) * 5 + (P(), P()) + (sharded,) * 7
    out_specs = (sharded,) * 4 + (P(), P()) + (sharded,) * 7

    def device_step(hidden, grad_out, positions, norm1, norm2, gain_q, gain_k, w_q, w_k, w_v, w_o, w_gate, w_up, w_down):
        trig = rope_tables(positions)
        gains = jnp.broadcast_to(jnp.concatenate([norm1, norm2]).astype(F32)[None, :], (8, 128))
        x, dy = hidden.reshape(T, D), grad_out.reshape(T, D)
        gq, gk = gain_q.astype(F32)[None, :], gain_k.astype(F32)[None, :]
        out, d_hidden, d_qkv, d_gate_up, d_wo, d_wd, g_sum = layer_call(
            x, dy, trig, gq, gk, gains, w_q, w_k, w_v, w_o, w_gate, w_up, w_down
        )
        start = lax.axis_index(axis_name) * 64
        d_norm1 = lax.dynamic_slice(g_sum[:8].reshape(D), (start,), (64,))
        d_norm2 = lax.dynamic_slice(g_sum[8:16].reshape(D), (start,), (64,))
        return (
            out.reshape(hidden.shape), d_hidden.reshape(hidden.shape), d_norm1, d_norm2, g_sum[16], g_sum[17],
            d_qkv[:, :NQ], d_qkv[:, NQ : NQ + D], d_qkv[:, NQ + D :], d_wo, d_gate_up[:, :FF], d_gate_up[:, FF:], d_wd,
        )

    return jax.shard_map(device_step, mesh=mesh, in_specs=in_specs, out_specs=out_specs, check_vma=False)
```

```python
import jax
import jax.numpy as jnp
from jax import lax
from jax.experimental import pallas as pl
from jax.experimental.pallas import tpu as pltpu
from jax.sharding import PartitionSpec as P

RMS_EPS = 1e-6
ROPE_THETA = 1000000.0
MESH = pl.DeviceIdType.MESH
F32 = jnp.float32
BF16 = jnp.bfloat16
T = 128
D = 1024
NQ = 2048
FF = 3072
HD = 128
Z, Y, X, C = 0, 1, 2, 3
STRIDE = (8, 4, 2, 1)
ALL = slice(None)
VM = pltpu.VMEM
HIGH_VMEM = 67043328


def nn(left_op, right_op):
    return jnp.dot(left_op, right_op, preferred_element_type=F32)


def nt(left_op, right_op):
    return lax.dot_general(left_op, right_op, (((1,), (1,)), ((), ())), preferred_element_type=F32)


def tn(left_op, right_op):
    return lax.dot_general(left_op, right_op, (((0,), (0,)), ((), ())), preferred_element_type=F32)


def rms(val):
    return lax.rsqrt(jnp.mean(val * val, axis=-1, keepdims=True) + RMS_EPS)


def norm_backward(d_unit, unit_val, scale_val):
    return scale_val * (d_unit - unit_val * jnp.mean(d_unit * unit_val, axis=-1, keepdims=True))


class Place:
    def __init__(self):
        self.me = lax.axis_index("fsdp")
        self.bit = [lax.rem(lax.div(self.me, s), 2) for s in STRIDE]

    def near(self, dim):
        return (self.me + STRIDE[dim] * (1 - 2 * self.bit[dim]),)

    def greet(self, dims):
        barrier = pltpu.get_barrier_semaphore()
        for dim in dims:
            pl.semaphore_signal(barrier, inc=1, device_id=self.near(dim), device_id_type=MESH)
        pl.semaphore_wait(barrier, len(dims))


class Spread:
    def __init__(self, place, own, first, buf, sub, order, axes, sems, part):
        self.place, self.buf, self.sub, self.order, self.axes = place, buf, sub, order, axes
        self.link_send, self.link_recv, self.core_send, self.core_recv, self.local_sem = sems
        self.part, self.last = part, len(order)
        self.source = own
        self.mine = self.block(()) if own is None else own
        self.first = self.mine if first is None else first

    def block(self, full, flip=None):
        index = []
        for dim in self.axes:
            if dim in full:
                index.append(ALL)
            elif dim == flip:
                index.append(1 - self.place.bit[dim])
            else:
                index.append(self.place.bit[dim])
        return self.buf.at[tuple(index) + self.sub]

    def copy_own(self):
        return pltpu.make_async_copy(self.source, self.block(()), self.local_sem.at[self.part])

    def link(self, step):
        dst = self.block(self.order[:step])
        return pltpu.make_async_remote_copy(
            src_ref=self.first if step == 0 else dst,
            dst_ref=dst,
            send_sem=self.link_send.at[self.part, step],
            recv_sem=self.link_recv.at[self.part, step],
            device_id=self.place.near(self.order[step]),
            device_id_type=MESH,
        )

    def core(self, step):
        dst = self.block(()) if step == 0 else self.block(self.order[: step - 1], self.order[step - 1])
        return pltpu.make_async_remote_copy(
            src_ref=self.mine if step == 0 else dst,
            dst_ref=dst,
            send_sem=self.core_send.at[self.part, step],
            recv_sem=self.core_recv.at[self.part, step],
            device_id=self.place.near(C),
            device_id_type=MESH,
        )

    def begin(self):
        self.link(0).start()
        if self.source is not None:
            self.copy_own().start()
        self.core(0).start()

    def advance(self, step):
        if step == 0 and self.source is not None:
            self.copy_own().wait()
        self.link(step).wait_recv()
        if step + 1 < self.last:
            self.link(step + 1).start()
        self.core(step + 1).start()

    def arrived(self):
        for step in range(self.last + 1):
            self.core(step).wait_recv()

    def drain(self):
        for step in range(self.last):
            self.link(step).wait_send()
        for step in range(self.last + 1):
            self.core(step).wait_send()


class Group:
    def __init__(self, place, axes):
        self.place, self.axes = place, axes
        self.position = self.spot(place.bit)

    def others(self):
        for number in range(2 ** len(self.axes) - 1, 0, -1):
            bit = list(self.place.bit)
            for i, dim in enumerate(self.axes):
                if number >> i & 1:
                    bit[dim] = 1 - bit[dim]
            yield bit

    def spot(self, bit):
        total = 0
        for dim in self.axes:
            total = total * 2 + bit[dim]
        return total


def device_of(bit):
    return (sum(stride * value for stride, value in zip(STRIDE, bit)),)


class Exchange:
    def __init__(self, group, number, piece, slot, blocks, sems):
        self.group, self.piece, self.slot, self.blocks = group, piece, slot, blocks
        self.send, self.recv, self.local = (sem.at[number] for sem in sems)

    def own(self):
        return pltpu.make_async_copy(self.piece(self.group.place.bit), self.slot, self.local)

    def begin(self):
        for bit in self.group.others():
            pltpu.make_async_remote_copy(
                src_ref=self.piece(bit),
                dst_ref=self.slot,
                send_sem=self.send,
                recv_sem=self.recv,
                device_id=device_of(bit),
                device_id_type=MESH,
            ).start()
        self.own().start()

    def arrived(self):
        self.own().wait()
        pltpu.make_async_copy(self.blocks, self.blocks, self.recv).wait()

    def drain(self):
        pltpu.make_async_copy(self.blocks, self.blocks, self.send).wait()


def head_forward(proj, gain, cos, sin):
    val = proj.astype(F32)
    scaled = val * rms(val) * gain
    return (scaled * cos + pltpu.roll(scaled, 64, axis=1) * sin).astype(BF16)


def head_backward(d_rot, proj, gain, cos, sin):
    val = proj.astype(F32)
    scale = rms(val)
    unit = val * scale
    d_scaled = d_rot * cos - pltpu.roll(d_rot, 64, axis=1) * sin
    d_gain = jnp.sum(d_scaled * unit, axis=0, keepdims=True)
    return norm_backward(d_scaled * gain, unit, scale).astype(BF16), d_gain


def cols(i, width):
    return pl.ds(pl.multiple_of(i * width, width), width)


def loop(count, body, init=0):
    return lax.fori_loop(0, count, body, init)


def each(count):
    def run(body):
        def step(i, _):
            body(i)
            return 0

        loop(count, step)

    return run


def two(i):
    return lax.div(i, 2), lax.rem(i, 2)


def three(i):
    return two(lax.div(i, 2)) + (lax.rem(i, 2),)


def layer_kernel(
    x_ref, dy_ref, trig_ref, gq_ref, gk_ref, gains, wq, wk, wv, wo, wg, wu, wd,
    y_ref, dh_ref, oqkv, ogu, owo, owd, ogain,
    gbuf, bq, bk, bv, bo, bg, bu, bd, g1, g2,
    xp, trig, n_s, q_s, k_s, v_s, qr, kr, probs, ctx, h_s, m_s, spare, act, dact, dctx, dres,
    part_a, part_y, part_m, part_n, land_a, land_y, land_m, land_n,
    at_ref, ct_ref, dqkv, dgu, gpart,
    nbuf, mbuf, dybuf, drbuf, gubuf, qkvbuf, abuf, cbuf,
    rgu, rqkv, rwd, rwo, zgu, zqkv, zwd, zwo, gainbuf,
    link_send, link_recv, core_send, core_recv, local_sem, one_send, one_recv, one_local, far_send, far_recv,
):
    place = Place()
    me = place.me
    z, y, x, c = place.bit
    sems = (link_send, link_recv, core_send, core_recv, local_sem)
    one = (one_send, one_recv, one_local)
    parts = []

    def spread(own, first, buf, sub, order, axes):
        parts.append(Spread(place, own, first, buf, sub, order, axes, sems, len(parts)))
        return parts[-1]

    both = (ALL, ALL)
    turns = ((Y, X), (X, Y))

    def by_columns(src, buf):
        half = src.shape[1] // 2
        size = half // 2
        made = []
        for i in range(2):
            mine, theirs = (src.at[:, pl.ds(pl.multiple_of(side * half + i * size, size), size)] for side in (z, 1 - z))
            made.append(spread(mine, theirs, buf, (ALL, pl.ds(i * size, size)), (Z,) + turns[i], (Z, Y, X, C)))
        return made

    def by_rows(src, buf):
        size = src.shape[0] // 2
        made = []
        for i in range(2):
            rows = pl.ds(i * size, size)
            made.append(spread(src.at[rows], None, buf, (rows, ALL), turns[i], (Y, X, C)))
        return made

    p_qkv = by_columns(wq, bq) + by_columns(wk, bk) + by_columns(wv, bv)
    p_o, p_d = by_rows(wo, bo), by_rows(wd, bd)
    p_g, p_u = by_columns(wg, bg), by_columns(wu, bu)
    p_m = spread(None, None, mbuf, both, (X,), (X, C))
    p_n = spread(None, None, nbuf, both, (Y,), (Y, C))
    p_dy = spread(None, None, dybuf, (ALL, ALL, ALL), (Y,), (Y, C))
    p_dr = spread(None, None, drbuf, (ALL, ALL, ALL), (X,), (X, C))

    grp_x, grp_y = Group(place, (X, C)), Group(place, (Y, C))

    def share(number, group, piece, buf):
        return Exchange(group, number, piece, buf.at[group.position], buf.at[pl.ds(0, 3)], one)

    def cols_for(group, ref, width):
        return lambda bit: ref.at[:, pl.ds(pl.multiple_of(group.spot(bit) * width, 128), width)]

    e_gu = share(0, grp_x, cols_for(grp_x, dgu, 768), gubuf)
    e_qkv = share(1, grp_y, cols_for(grp_y, dqkv, 512), qkvbuf)
    e_a = share(2, grp_y, lambda bit: at_ref.at[bit[Y], :, bit[C]], abuf)
    e_c = share(3, grp_x, lambda bit: ct_ref.at[:, bit[X], bit[C]], cbuf)
    gain_number, norm_number = 9, 10
    sent = []

    def near_copy(dim, source, target):
        number = len(sent)
        sent.append(
            pltpu.make_async_remote_copy(
                src_ref=source, dst_ref=target, send_sem=far_send.at[number], recv_sem=far_recv.at[number],
                device_id=place.near(dim), device_id_type=MESH,
            )
        )
        return sent[-1]

    mine, theirs = cols(z, T), cols(1 - z, T)
    barrier = pltpu.get_barrier_semaphore()

    def other(k):
        return (lax.rem(me + k, 16),)

    @each(15)
    def _(k):
        pl.semaphore_signal(barrier, inc=1, device_id=other(k + 1), device_id_type=MESH)

    pl.semaphore_wait(barrier, 15)

    def to_all(source, buf, number):
        @each(15)
        def _(k):
            pltpu.make_async_remote_copy(
                src_ref=source, dst_ref=buf.at[me], send_sem=one_send.at[number], recv_sem=one_recv.at[number],
                device_id=other(k + 1), device_id_type=MESH,
            ).start()

    def all_wait(buf, sem):
        fifteen = buf.at[pl.ds(0, 15)]
        pltpu.make_async_copy(fifteen, fifteen, sem).wait()

    to_all(gains, gbuf, norm_number)
    for item in p_qkv + p_o:
        item.begin()
    x_copy = near_copy(Z, x_ref, xp.at[mine])
    trig_copy = near_copy(Z, trig_ref, trig.at[z])
    x_copy.start()
    trig_copy.start()
    xp[mine] = x_ref[...]
    trig[z] = trig_ref[...]
    for item in p_d + p_g + p_u:
        item.begin()
    dy_copy = near_copy(Z, dy_ref, dybuf.at[y, c, z])
    dy_copy.start()
    dybuf[y, c, z] = dy_ref[...]
    for item in p_qkv + p_o:
        item.advance(0)
    all_wait(gbuf, one_recv.at[norm_number])
    gbuf[me] = gains[...]
    lane = lax.broadcasted_iota(jnp.int32, (8, 128), 1) < 64
    for i in range(8):
        first, second = gbuf[2 * i], gbuf[2 * i + 1]
        tile = slice(128 * i, 128 * i + 128)
        g1[:, tile] = jnp.where(lane, first, pltpu.roll(second, 64, axis=1))[:1]
        g2[:, tile] = jnp.where(lane, pltpu.roll(first, 64, axis=1), second)[:1]
    x_copy.wait_recv()

    @each(8)
    def _(i):
        rows = cols(i, 32)
        val = xp[rows].astype(F32)
        n_s[rows] = (val * rms(val) * g1[...]).astype(BF16)

    def turned(val):
        return val.astype(F32).T.astype(BF16)

    for item in p_qkv:
        item.advance(1)
    for item in p_d:
        item.advance(0)

    @each(4)
    def _(i):
        nbuf[y, c, cols(i, 256)] = turned(n_s[:, cols(i, 256)])

    for item in p_o:
        item.advance(1)
    for item in p_g + p_u:
        item.advance(0)
    for item in p_qkv:
        item.advance(2)
    trig_copy.wait_recv()

    def weight(buf, tile):
        block = buf[(ALL,) * (len(buf.shape) - 1) + (tile,)]
        return block.reshape(-1, block.shape[-1])

    def project(buf, dst, width, tiles):
        @each(tiles)
        def _(j):
            tile = cols(j, width)
            dst[:, tile] = nn(n_s[...], weight(buf, tile)).astype(BF16)

    for item in p_qkv:
        item.arrived()
    project(bq, q_s, 512, 2)
    project(bk, k_s, 512, 1)
    project(bv, v_s, 512, 1)
    scale = HD ** -0.5

    def sequence_head(j):
        seq, head = lax.div(j, 4), lax.rem(j, 4)
        return seq, head, cols(seq, T), cols(head, HD), cols(head, 2 * HD)

    @each(8)
    def _(j):
        seq, _, rows, kv, pair = sequence_head(j)
        cos, sin = trig[seq, :, :HD], trig[seq, :, HD:]
        k_rot = head_forward(k_s[rows, kv], gk_ref[...], cos, sin)
        kr[rows, kv] = k_rot
        q_pair = q_s[rows, pair]
        q_rot = jnp.concatenate(
            [head_forward(half, gq_ref[...], cos, sin) for half in (q_pair[:, :HD], q_pair[:, HD:])], axis=0
        )
        qr[j] = q_rot
        scores = nt(q_rot, k_rot) * scale
        row = lax.rem(lax.broadcasted_iota(jnp.int32, (2 * T, T), 0), T)
        col = lax.broadcasted_iota(jnp.int32, (2 * T, T), 1)
        scores = jnp.where(row >= col, scores, -1e30)
        expd = jnp.exp(scores - jnp.max(scores, axis=-1, keepdims=True))
        prob = expd / jnp.sum(expd, axis=-1, keepdims=True)
        probs[j] = prob
        out = nn(prob.astype(BF16), v_s[rows, kv])
        ctx[rows, pair] = jnp.concatenate([out[:T], out[T:]], axis=1).astype(BF16)

    def pair_sum(partial, landing, compute):
        copies = []
        for half in range(2):
            @each(2)
            def _(j):
                i = j + 2 * half
                partial[:, :, cols(i, 256)] = compute(i).reshape(2, T, 256)

            span = (ALL, pl.ds(512 * half, 512))
            copies.append(near_copy(Z, partial.at[(1 - z,) + span], landing.at[span]))
            copies[-1].start()
        return copies

    def received(copies):
        for copy in copies:
            copy.wait_recv()

    for item in p_o:
        item.arrived()
    a_copies = pair_sum(part_a, land_a, lambda i: nn(ctx[...], weight(bo, cols(i, 256))))
    for item in p_g + p_u:
        item.advance(1)
    for item in p_d:
        item.advance(1)

    @each(4)
    def _(i):
        ct_ref[two(i)] = turned(ctx[:, cols(i, 256)]).reshape(2, 128, 2 * T)

    received(a_copies)

    @each(4)
    def _(i):
        rows = cols(i, 32)
        attn = (part_a[z, rows] + land_a[rows]).astype(BF16)
        val = (x_ref[rows].astype(F32) + attn.astype(F32)).astype(BF16).astype(F32)
        h_s[rows] = val
        m_s[pl.ds(pl.multiple_of(z * T + i * 32, 32), 32)] = (val * rms(val) * g2[...]).astype(BF16)

    m_copy = near_copy(Z, m_s.at[mine], m_s.at[mine])
    m_copy.start()
    for item in p_d:
        item.arrived()
    dy_copy.wait_recv()

    @each(4)
    def _(i):
        dact[:, cols(i, 384)] = nt(dybuf[y, c].reshape(2 * T, D), bd[two(i)].reshape(384, D))

    for item in p_g + p_u:
        item.advance(2)
    m_copy.wait_recv()
    for item in p_g + p_u:
        item.arrived()
    fh = FF // 2

    @each(fh // 256)
    def _(j):
        tile = cols(j, 256)
        gate_val = nn(m_s[...], weight(bg, tile)).astype(BF16).astype(F32)
        up_val = nn(m_s[...], weight(bu, tile)).astype(BF16).astype(F32)
        sig = jax.nn.sigmoid(gate_val)
        act[:, tile] = (gate_val * sig * up_val).astype(BF16)
        d_act = dact[:, tile]
        dgu[:, tile] = (d_act * up_val * sig * (1.0 + gate_val * (1.0 - sig))).astype(BF16)
        dgu[:, cols(j + fh // 256, 256)] = (d_act * gate_val * sig).astype(BF16)

    def d_mlp_in(i):
        rows = two(i)
        return nt(dgu[:, :fh], bg[rows].reshape(256, fh)) + nt(dgu[:, fh:], bu[rows].reshape(256, fh))

    m_copies = pair_sum(part_m, land_m, d_mlp_in)
    e_gu.begin()

    @each(4)
    def _(i):
        mbuf[x, c, cols(i, 256)] = turned(m_s[:, cols(i, 256)])

    p_m.begin()
    p_n.begin()
    p_dy.begin()

    @each(4)
    def _(i):
        at_ref[two(i)] = turned(act[:, cols(i, 384)]).reshape(2, 192, 2 * T)

    e_a.begin()
    e_c.begin()
    received(m_copies)

    def d_res_rows(i, total):
        rows = cols(i, 32)
        val = h_s[rows]
        r_scale = rms(val)
        unit = val * r_scale
        grad = part_m[z, rows] + land_m[rows]
        out = dy_ref[rows].astype(F32) + norm_backward(grad * g2[...], unit, r_scale)
        dres[rows] = out
        drbuf[x, c, z, rows] = out.astype(BF16)
        return total + jnp.sum(grad * unit, axis=0, keepdims=True)

    d_g2 = loop(4, d_res_rows, jnp.zeros((1, D), F32))
    r_copy = near_copy(Z, drbuf.at[x, c, z], drbuf.at[x, c, z])
    r_copy.start()
    y_copies = pair_sum(part_y, land_y, lambda i: nn(act[...], weight(bd, cols(i, 256))))
    r_copy.wait_recv()
    p_dr.begin()

    @each(2)
    def _(i):
        dctx[:, cols(i, 512)] = nt(drbuf[x, c].reshape(2 * T, D), bo[i].reshape(512, D)).astype(BF16)

    def attend_back(j, carry):
        q_total, k_total = carry
        seq, head, rows, kv, pair = sequence_head(j)
        cos, sin = trig[seq, :, :HD], trig[seq, :, HD:]
        d_out = dctx[rows, pair]
        d_out = jnp.concatenate([d_out[:, :HD], d_out[:, HD:]], axis=0)
        prob = probs[j]
        d_value = tn(prob.astype(BF16), d_out).astype(BF16)
        d_prob = nt(d_out, v_s[rows, kv])
        d_score = prob * (d_prob - jnp.sum(prob * d_prob, axis=-1, keepdims=True))
        d_score = (d_score * scale).astype(BF16)
        d_q_rot = nn(d_score, kr[rows, kv])
        d_k_rot = tn(d_score, qr[j])
        q_pair = q_s[rows, pair]
        d_q0, g_q0 = head_backward(d_q_rot[:T], q_pair[:, :HD], gq_ref[...], cos, sin)
        d_q1, g_q1 = head_backward(d_q_rot[T:], q_pair[:, HD:], gq_ref[...], cos, sin)
        d_k, g_k = head_backward(d_k_rot, k_s[rows, kv], gk_ref[...], cos, sin)
        dqkv[rows, pair] = jnp.concatenate([d_q0, d_q1], axis=1)
        dqkv[rows, cols(head + 8, HD)] = d_k
        dqkv[rows, cols(head + 12, HD)] = d_value
        return q_total + g_q0 + g_q1, k_total + g_k

    zero = jnp.zeros((1, HD), F32)
    q_total, k_total = loop(8, attend_back, (zero, zero))
    e_qkv.begin()

    def d_normed(i):
        rows = two(i)
        grad = nt(dqkv[:, :D], bq[rows].reshape(256, D)) + nt(dqkv[:, D : D + 512], bk[rows].reshape(256, 512))
        return grad + nt(dqkv[:, D + 512 :], bv[rows].reshape(256, 512))

    n_copies = pair_sum(part_n, land_n, d_normed)
    inv_tokens = 1.0 / (16 * T)

    def column_chunk(acts, grads, out, chunk):
        @each(8)
        def _(i):
            rows = cols(i, 128)
            left = jnp.concatenate([acts[k // 2, k % 2, rows] for k in range(4)], axis=1)
            right = grads[:, :, 256 * chunk : 256 * chunk + 256].reshape(8 * T, 256)
            out[(chunk,) + three(i)] = (nn(left, right) * inv_tokens).reshape(2, 64, 256)

    def half_of(dim, result, chunk):
        bit = place.bit[dim]
        return result.at[(chunk,) + tuple(1 - bit if k == dim else ALL for k in range(4))]

    def row_tiles(left_buf, right_buf, out):
        @each(8)
        def _(j):
            tile = cols(lax.rem(j, 4), 256)
            half = lax.div(j, 4)
            left = jnp.concatenate([left_buf[i, half] for i in range(4)], axis=1)
            out[half, :, tile] = nn(left, weight(right_buf, tile)) * inv_tokens

    p_m.advance(0)
    p_m.arrived()
    e_gu.arrived()
    gu_far = []
    for chunk in range(3):
        column_chunk(mbuf, gubuf, rgu, chunk)
        gu_far.append(near_copy(Y, half_of(Y, rgu, chunk), zgu.at[chunk]))
        gu_far[-1].start()
    p_n.advance(0)
    p_n.arrived()
    e_qkv.arrived()
    qkv_far = []
    for chunk in range(2):
        column_chunk(nbuf, qkvbuf, rqkv, chunk)
        qkv_far.append(near_copy(X, half_of(X, rqkv, chunk), zqkv.at[chunk]))
        qkv_far[-1].start()
    p_dy.advance(0)
    p_dy.arrived()
    e_a.arrived()
    row_tiles(abuf, dybuf, rwd)
    wd_far = near_copy(X, rwd.at[1 - x], zwd)
    wd_far.start()
    p_dr.advance(0)
    p_dr.arrived()
    e_c.arrived()
    row_tiles(cbuf, drbuf, rwo)
    wo_far = near_copy(Y, rwo.at[1 - y], zwo)
    wo_far.start()

    received(n_copies)

    def d_hidden_rows(i, total):
        rows = cols(i, 32)
        val = x_ref[rows].astype(F32)
        x_scale = rms(val)
        unit = val * x_scale
        grad = part_n[z, rows] + land_n[rows]
        dh_ref[rows] = (dres[rows] + norm_backward(grad * g1[...], unit, x_scale)).astype(BF16)
        return total + jnp.sum(grad * unit, axis=0, keepdims=True)

    d_g1 = loop(4, d_hidden_rows, jnp.zeros((1, D), F32))
    for i in range(8):
        tile = slice(128 * i, 128 * i + 128)
        gpart[i : i + 1, :] = d_g1[:, tile]
        gpart[8 + i : 9 + i, :] = d_g2[:, tile]
    gpart[16:17, :] = q_total
    gpart[17:18, :] = k_total
    gpart[18:24, :] = jnp.zeros((6, 128), F32)

    to_all(gpart, gainbuf, gain_number)
    received(y_copies)

    @each(4)
    def _(i):
        rows = cols(i, 32)
        out = (part_y[z, rows] + land_y[rows]).astype(BF16).astype(F32)
        y_ref[rows] = (h_s[rows] + out).astype(BF16)

    def final(dim, number, result, target, out, chunk, base):
        group = Group(place, tuple(k for k in range(4) if k != dim))
        for bit in list(group.others()) + [place.bit]:
            index = (chunk,) + tuple(bit)
            result[index] = result[index] + target[(chunk,) + tuple(bit[k] for k in group.axes)]
        where = pl.ds(pl.multiple_of(base + 256 * chunk, 128), 256)
        move = Exchange(
            group, number, lambda bit: result.at[(chunk,) + tuple(bit)], out.at[:, where],
            out.at[:, pl.ds(0, 7 * 256)], one,
        )
        move.begin()
        return move

    gu_base = x * FF + z * fh + c * 768
    qkv_base = (1 - y) * (z * D + c * 512) + y * (NQ + c * D + z * 512)
    moves = []
    for kind, chunk in ((0, 0), (1, 0), (0, 1), (1, 1), (0, 2)):
        if kind == 0:
            gu_far[chunk].wait_recv()
            moves.append(final(Y, 4 + chunk, rgu, zgu, ogu, chunk, gu_base))
        else:
            qkv_far[chunk].wait_recv()
            moves.append(final(X, 7 + chunk, rqkv, zqkv, oqkv, chunk, qkv_base))
    wd_far.wait_recv()
    owd[...] = rwd[x] + zwd[...]
    wo_far.wait_recv()
    owo[...] = rwo[y] + zwo[...]
    all_wait(gainbuf, one_recv.at[gain_number])
    gainbuf[me] = gpart[...]
    gainbuf[0] = loop(16, lambda i, total: total + gainbuf[i], jnp.zeros((24, 128), F32)) * inv_tokens
    for i in range(2):
        row = gainbuf[0, pl.ds(8 * i + lax.div(me, 2), 1), :]
        ogain[i : i + 1, :] = jnp.where(c == 0, row, pltpu.roll(row, 64, axis=1))
    ogain[2:4, :] = gainbuf[0, 16:18, :]
    ogain[4:8, :] = jnp.zeros((4, 128), F32)
    for move in moves:
        move.arrived()
    for item in moves + [e_gu, e_qkv, e_a, e_c] + parts:
        item.drain()
    for copy in sent:
        copy.wait_send()
    all_wait(gainbuf, one_send.at[gain_number])
    all_wait(gbuf, one_send.at[norm_number])


def shape(rows, width, dtype):
    return jax.ShapeDtypeStruct((rows, width), dtype)


def many(count, *args):
    return [VM(*args)] * count


def layer_call(x, dy, trig, gq, gk, gains, *weights):
    vmem = pl.BlockSpec(memory_space=VM)
    hbm = pl.BlockSpec(memory_space=pl.ANY)
    dma = pltpu.SemaphoreType.DMA
    t2, kvh, fh = 2 * T, D // 2, FF // 2
    cube, square, line = (2, 2, 2, 2), (2, 2, 2), (2, 2)
    spreads = 18
    return pl.pallas_call(
        layer_kernel,
        name="layer",
        out_shape=(
            shape(T, D, BF16), shape(T, D, BF16), shape(64, NQ + 2 * D, F32), shape(64, 2 * FF, F32),
            shape(128, D, F32), shape(192, D, F32), shape(8, 128, F32),
        ),
        in_specs=[vmem] * 6 + [hbm] * 7,
        out_specs=(vmem, vmem, hbm, hbm, vmem, vmem, vmem),
        scratch_shapes=[
            VM((16, 8, 128), F32), VM(cube + (64, D), BF16), *many(2, cube + (64, kvh), BF16),
            VM(square + (128, D), BF16), *many(2, cube + (64, fh), BF16), VM(square + (192, D), BF16),
            *many(2, (1, D), F32),
            VM((t2, D), BF16), VM((2, T, t2), F32), VM((t2, D), BF16), VM((t2, D), BF16), *many(2, (t2, kvh), BF16),
            VM((8, t2, HD), BF16), VM((t2, kvh), BF16), VM((8, t2, T), F32), VM((t2, D), BF16), VM((T, D), F32),
            VM((t2, D), BF16), VM((8, 128), BF16), VM((t2, fh), BF16), VM((t2, fh), F32), VM((t2, D), BF16),
            VM((T, D), F32), *many(4, (2, T, D), F32), *many(4, (T, D), F32),
            VM(square + (192, t2), BF16), VM(square + (128, t2), BF16), VM((t2, NQ), BF16), VM((t2, FF), BF16),
            VM((24, 128), F32), *many(2, line + (D, t2), BF16), *many(2, line + (2, T, D), BF16),
            VM((4, t2, 768), BF16), VM((4, t2, 512), BF16), VM((4, 2, 192, t2), BF16), VM((4, 2, 128, t2), BF16),
            VM((3,) + cube + (64, 256), F32), VM((2,) + cube + (64, 256), F32), VM((2, 192, D), F32),
            VM((2, 128, D), F32), VM((3,) + square + (64, 256), F32), VM((2,) + square + (64, 256), F32),
            VM((192, D), F32), VM((128, D), F32), VM((16, 24, 128), F32),
            *[dma((spreads, 3))] * 2, *[dma((spreads, 4))] * 2, dma((spreads,)), *[dma((11,))] * 3, *[dma((20,))] * 2,
        ],
        compiler_params=pltpu.CompilerParams(collective_id=0, has_side_effects=True, vmem_limit_bytes=HIGH_VMEM),
    )(x, dy, trig, gq, gk, gains, *weights)


def deliver_kernel(y_in, dh_in, qkv_in, gu_in, wo_in, wd_in, gain_in, *refs):
    outs, gains_out, scratch, (in_sem, out_sem) = refs[:9], refs[9:13], refs[13:22], refs[22:]
    spans = ((qkv_in, 0, NQ), (qkv_in, NQ, D), (qkv_in, NQ + D, D), (gu_in, 0, FF), (gu_in, FF, FF))
    q_in, k_in, v_in, g_in, u_in = (ref.at[:, pl.ds(start, size)] for ref, start, size in spans)
    sources = (y_in, dh_in, q_in, k_in, v_in, wo_in, g_in, u_in, wd_in)
    loads = [pltpu.make_async_copy(src, buf, in_sem.at[i]) for i, (src, buf) in enumerate(zip(sources, scratch))]
    stores = [pltpu.make_async_copy(buf, out, out_sem.at[i]) for i, (buf, out) in enumerate(zip(scratch, outs))]
    for load in loads:
        load.start()
    for i, out in enumerate(gains_out):
        out[...] = gain_in[i : i + 1, : out.shape[0]].reshape(out.shape)
    for load, store in zip(loads, stores):
        load.wait()
        store.start()
    for store in stores:
        store.wait()


def deliver(*results):
    vmem = pl.BlockSpec(memory_space=VM)
    hbm = pl.BlockSpec(memory_space=pl.ANY)
    dma = pltpu.SemaphoreType.DMA
    sizes = [(T, D, BF16)] * 2 + [(64, width, F32) for width in (NQ, D, D)] + [(128, D, F32)]
    sizes += [(64, FF, F32)] * 2 + [(192, D, F32)]
    small = [jax.ShapeDtypeStruct((size,), F32) for size in (64, 64, 128, 128)]
    return pl.pallas_call(
        deliver_kernel,
        name="deliver",
        out_shape=tuple([shape(*size) for size in sizes] + small),
        in_specs=[hbm] * 6 + [vmem],
        out_specs=tuple([hbm] * 9 + [vmem] * 4),
        scratch_shapes=[VM(size[:2], size[2]) for size in sizes] + [dma((9,)), dma((9,))],
    )(*results)


def rope_tables(positions):
    inv_freq = ROPE_THETA ** (-2.0 * jnp.arange(HD // 2, dtype=F32) / HD)
    angle = positions.reshape(-1, 1).astype(F32) * inv_freq
    cos_half, sin_half = jnp.cos(angle), jnp.sin(angle)
    return jnp.concatenate([cos_half, cos_half, -sin_half, sin_half], axis=-1)


def solution(mesh):
    axis_name = mesh.axis_names[0]
    sharded = P(axis_name)
    in_specs = (sharded,) * 5 + (P(), P()) + (sharded,) * 7
    out_specs = (sharded,) * 4 + (P(), P()) + (sharded,) * 7

    def device_step(hidden, grad_out, positions, norm1, norm2, gain_q, gain_k, w_q, w_k, w_v, w_o, w_gate, w_up, w_down):
        trig = rope_tables(positions)
        gains = jnp.broadcast_to(jnp.concatenate([norm1, norm2]).astype(F32)[None, :], (8, 128))
        x, dy = hidden.reshape(T, D), grad_out.reshape(T, D)
        gq, gk = gain_q.astype(F32)[None, :], gain_k.astype(F32)[None, :]
        results = layer_call(x, dy, trig, gq, gk, gains, w_q, w_k, w_v, w_o, w_gate, w_up, w_down)
        out, d_hidden, d_wq, d_wk, d_wv, d_wo, d_wg, d_wu, d_wd, d_n1, d_n2, d_qn, d_kn = deliver(*results)
        out, d_hidden = out.reshape(hidden.shape), d_hidden.reshape(hidden.shape)
        return out, d_hidden, d_n1, d_n2, d_qn, d_kn, d_wq, d_wk, d_wv, d_wo, d_wg, d_wu, d_wd

    return jax.shard_map(device_step, mesh=mesh, in_specs=in_specs, out_specs=out_specs, check_vma=False)
```

```python
import jax
import jax.numpy as jnp
from jax import lax
from jax.experimental import pallas as pl
from jax.experimental.pallas import tpu as pltpu
from jax.sharding import PartitionSpec as P

RMS_EPS = 1e-6
ROPE_THETA = 1000000.0
MESH = pl.DeviceIdType.MESH
F32 = jnp.float32
BF16 = jnp.bfloat16
T = 128
D = 1024
NQ = 2048
FF = 3072
HD = 128
Z, Y, X, C = 0, 1, 2, 3
STRIDE = (8, 4, 2, 1)
ALL = slice(None)
VM = pltpu.VMEM
HIGH_VMEM = 67043328


def nn(left_op, right_op):
    return jnp.dot(left_op, right_op, preferred_element_type=F32)


def nt(left_op, right_op):
    return lax.dot_general(left_op, right_op, (((1,), (1,)), ((), ())), preferred_element_type=F32)


def tn(left_op, right_op):
    return lax.dot_general(left_op, right_op, (((0,), (0,)), ((), ())), preferred_element_type=F32)


def rms(val):
    return lax.rsqrt(jnp.mean(val * val, axis=-1, keepdims=True) + RMS_EPS)


def norm_backward(d_unit, unit_val, scale_val):
    return scale_val * (d_unit - unit_val * jnp.mean(d_unit * unit_val, axis=-1, keepdims=True))


class Place:
    def __init__(self):
        self.me = lax.axis_index("fsdp")
        self.bit = [lax.rem(lax.div(self.me, s), 2) for s in STRIDE]

    def near(self, dim):
        return (self.me + STRIDE[dim] * (1 - 2 * self.bit[dim]),)

    def greet(self, dims):
        barrier = pltpu.get_barrier_semaphore()
        for dim in dims:
            pl.semaphore_signal(barrier, inc=1, device_id=self.near(dim), device_id_type=MESH)
        pl.semaphore_wait(barrier, len(dims))


class Spread:
    def __init__(self, place, own, first, buf, sub, order, axes, sems, part):
        self.place, self.buf, self.sub, self.order, self.axes = place, buf, sub, order, axes
        self.link_send, self.link_recv, self.core_send, self.core_recv, self.local_sem = sems
        self.part, self.last = part, len(order)
        self.source = own
        self.mine = self.block(()) if own is None else own
        self.first = self.mine if first is None else first

    def block(self, full, flip=None):
        index = []
        for dim in self.axes:
            if dim in full:
                index.append(ALL)
            elif dim == flip:
                index.append(1 - self.place.bit[dim])
            else:
                index.append(self.place.bit[dim])
        return self.buf.at[tuple(index) + self.sub]

    def copy_own(self):
        return pltpu.make_async_copy(self.source, self.block(()), self.local_sem.at[self.part])

    def link(self, step):
        dst = self.block(self.order[:step])
        return pltpu.make_async_remote_copy(
            src_ref=self.first if step == 0 else dst,
            dst_ref=dst,
            send_sem=self.link_send.at[self.part, step],
            recv_sem=self.link_recv.at[self.part, step],
            device_id=self.place.near(self.order[step]),
            device_id_type=MESH,
        )

    def core(self, step):
        dst = self.block(()) if step == 0 else self.block(self.order[: step - 1], self.order[step - 1])
        return pltpu.make_async_remote_copy(
            src_ref=self.mine if step == 0 else dst,
            dst_ref=dst,
            send_sem=self.core_send.at[self.part, step],
            recv_sem=self.core_recv.at[self.part, step],
            device_id=self.place.near(C),
            device_id_type=MESH,
        )

    def begin(self):
        self.link(0).start()
        if self.source is not None:
            self.copy_own().start()
        self.core(0).start()

    def advance(self, step):
        if step == 0 and self.source is not None:
            self.copy_own().wait()
        self.link(step).wait_recv()
        if step + 1 < self.last:
            self.link(step + 1).start()
        self.core(step + 1).start()

    def arrived(self):
        for step in range(self.last + 1):
            self.core(step).wait_recv()

    def drain(self):
        for step in range(self.last):
            self.link(step).wait_send()
        for step in range(self.last + 1):
            self.core(step).wait_send()


class Group:
    def __init__(self, place, axes):
        self.place, self.axes = place, axes
        self.position = self.spot(place.bit)

    def others(self):
        for number in range(2 ** len(self.axes) - 1, 0, -1):
            bit = list(self.place.bit)
            for i, dim in enumerate(self.axes):
                if number >> i & 1:
                    bit[dim] = 1 - bit[dim]
            yield bit

    def spot(self, bit):
        total = 0
        for dim in self.axes:
            total = total * 2 + bit[dim]
        return total


def device_of(bit):
    return (sum(stride * value for stride, value in zip(STRIDE, bit)),)


class Exchange:
    def __init__(self, group, number, piece, slot, blocks, sems):
        self.group, self.piece, self.slot, self.blocks = group, piece, slot, blocks
        self.send, self.recv, self.local = (sem.at[number] for sem in sems)

    def own(self):
        return pltpu.make_async_copy(self.piece(self.group.place.bit), self.slot, self.local)

    def begin(self):
        for bit in self.group.others():
            pltpu.make_async_remote_copy(
                src_ref=self.piece(bit),
                dst_ref=self.slot,
                send_sem=self.send,
                recv_sem=self.recv,
                device_id=device_of(bit),
                device_id_type=MESH,
            ).start()
        self.own().start()

    def arrived(self):
        self.own().wait()
        pltpu.make_async_copy(self.blocks, self.blocks, self.recv).wait()

    def drain(self):
        pltpu.make_async_copy(self.blocks, self.blocks, self.send).wait()


def head_forward(proj, gain, cos, sin):
    val = proj.astype(F32)
    scaled = val * rms(val) * gain
    return (scaled * cos + pltpu.roll(scaled, 64, axis=1) * sin).astype(BF16)


def head_backward(d_rot, proj, gain, cos, sin):
    val = proj.astype(F32)
    scale = rms(val)
    unit = val * scale
    d_scaled = d_rot * cos - pltpu.roll(d_rot, 64, axis=1) * sin
    d_gain = jnp.sum(d_scaled * unit, axis=0, keepdims=True)
    return norm_backward(d_scaled * gain, unit, scale).astype(BF16), d_gain


def cols(i, width):
    return pl.ds(pl.multiple_of(i * width, width), width)


def loop(count, body, init=0):
    return lax.fori_loop(0, count, body, init)


def each(count):
    def run(body):
        def step(i, _):
            body(i)
            return 0

        loop(count, step)

    return run


def two(i):
    return lax.div(i, 2), lax.rem(i, 2)


def three(i):
    return two(lax.div(i, 2)) + (lax.rem(i, 2),)


def layer_kernel(
    cos_ref, sin_ref, n1_ref, n2_ref, qn_ref, kn_ref, x_ref, dy_ref, wq, wk, wv, wo, wg, wu, wd,
    y_ref, dh_ref, oqkv, ogu, owo, owd, ogain,
    gains, gbuf, bq, bk, bv, bo, bg, bu, bd, g1, g2,
    xp, trig, n_s, q_s, k_s, v_s, qr, kr, probs, ctx, h_s, m_s, spare, act, dact, dctx, dres,
    part_a, part_y, part_m, part_n, land_a, land_y, land_m, land_n,
    at_ref, ct_ref, dqkv, dgu, gpart,
    nbuf, mbuf, dybuf, drbuf, gubuf, qkvbuf, abuf, cbuf,
    rgu, rqkv, rwd, rwo, zgu, zqkv, zwd, zwo, gainbuf,
    link_send, link_recv, core_send, core_recv, local_sem, one_send, one_recv, one_local, far_send, far_recv,
):
    place = Place()
    me = place.me
    z, y, x, c = place.bit
    sems = (link_send, link_recv, core_send, core_recv, local_sem)
    one = (one_send, one_recv, one_local)
    parts = []

    def spread(own, first, buf, sub, order, axes):
        parts.append(Spread(place, own, first, buf, sub, order, axes, sems, len(parts)))
        return parts[-1]

    both = (ALL, ALL)
    turns = ((Y, X), (X, Y))

    def by_columns(src, buf):
        half = src.shape[1] // 2
        size = half // 2
        made = []
        for i in range(2):
            mine, theirs = (src.at[:, pl.ds(pl.multiple_of(side * half + i * size, size), size)] for side in (z, 1 - z))
            made.append(spread(mine, theirs, buf, (ALL, pl.ds(i * size, size)), (Z,) + turns[i], (Z, Y, X, C)))
        return made

    def by_rows(src, buf):
        size = src.shape[0] // 2
        made = []
        for i in range(2):
            rows = pl.ds(i * size, size)
            made.append(spread(src.at[rows], None, buf, (rows, ALL), turns[i], (Y, X, C)))
        return made

    p_qkv = by_columns(wq, bq) + by_columns(wk, bk) + by_columns(wv, bv)
    p_o, p_d = by_rows(wo, bo), by_rows(wd, bd)
    p_g, p_u = by_columns(wg, bg), by_columns(wu, bu)
    p_m = spread(None, None, mbuf, both, (X,), (X, C))
    p_n = spread(None, None, nbuf, both, (Y,), (Y, C))
    p_dy = spread(None, None, dybuf, (ALL, ALL, ALL), (Y,), (Y, C))
    p_dr = spread(None, None, drbuf, (ALL, ALL, ALL), (X,), (X, C))

    grp_x, grp_y = Group(place, (X, C)), Group(place, (Y, C))

    def share(number, group, piece, buf):
        return Exchange(group, number, piece, buf.at[group.position], buf.at[pl.ds(0, 3)], one)

    def cols_for(group, ref, width):
        return lambda bit: ref.at[:, pl.ds(pl.multiple_of(group.spot(bit) * width, 128), width)]

    e_gu = share(0, grp_x, cols_for(grp_x, dgu, 768), gubuf)
    e_qkv = share(1, grp_y, cols_for(grp_y, dqkv, 512), qkvbuf)
    e_a = share(2, grp_y, lambda bit: at_ref.at[bit[Y], :, bit[C]], abuf)
    e_c = share(3, grp_x, lambda bit: ct_ref.at[:, bit[X], bit[C]], cbuf)
    gain_number, norm_number = 9, 10
    sent = []

    def near_copy(dim, source, target):
        number = len(sent)
        sent.append(
            pltpu.make_async_remote_copy(
                src_ref=source, dst_ref=target, send_sem=far_send.at[number], recv_sem=far_recv.at[number],
                device_id=place.near(dim), device_id_type=MESH,
            )
        )
        return sent[-1]

    mine = cols(z, T)

    def pair_rows(i):
        return cols(4 * z + i, 32)

    barrier = pltpu.get_barrier_semaphore()

    def other(k):
        return (lax.rem(me + k, 16),)

    @each(15)
    def _(k):
        pl.semaphore_signal(barrier, inc=1, device_id=other(k + 1), device_id_type=MESH)

    gains[...] = jnp.zeros((8, 128), F32)
    halves = [ref[...].astype(F32).reshape(1, 64) for ref in (n1_ref, n2_ref)]
    gains[0:1, :] = jnp.concatenate(halves, axis=1)
    gains[1:2, :] = qn_ref[...].astype(F32).reshape(1, 128)
    gains[2:3, :] = kn_ref[...].astype(F32).reshape(1, 128)
    cos_half, sin_half = cos_ref[...], sin_ref[...]
    trig[z] = jnp.concatenate([cos_half, cos_half, -sin_half, sin_half], axis=1)
    pl.semaphore_wait(barrier, 15)

    def to_all(source, buf, number):
        @each(15)
        def _(k):
            pltpu.make_async_remote_copy(
                src_ref=source, dst_ref=buf.at[me], send_sem=one_send.at[number], recv_sem=one_recv.at[number],
                device_id=other(k + 1), device_id_type=MESH,
            ).start()

    def all_wait(buf, sem):
        fifteen = buf.at[pl.ds(0, 15)]
        pltpu.make_async_copy(fifteen, fifteen, sem).wait()

    to_all(gains, gbuf, norm_number)
    for item in p_qkv + p_o:
        item.begin()
    x_copy = near_copy(Z, x_ref, xp.at[mine])
    trig_copy = near_copy(Z, trig.at[z], trig.at[z])
    x_copy.start()
    own_x = pltpu.make_async_copy(x_ref, xp.at[mine], local_sem.at[len(parts)])
    own_x.start()
    for item in p_d + p_g + p_u:
        item.begin()
    trig_copy.start()
    dy_copy = near_copy(Z, dy_ref, dybuf.at[y, c, z])
    dy_copy.start()
    own_dy = pltpu.make_async_copy(dy_ref, dybuf.at[y, c, z], local_sem.at[len(parts) + 1])
    own_dy.start()
    for item in p_qkv + p_o:
        item.advance(0)
    gq, gk = gains[1:2, :], gains[2:3, :]
    all_wait(gbuf, one_recv.at[norm_number])
    gbuf[me] = gains[...]
    lane = lax.broadcasted_iota(jnp.int32, (8, 128), 1) < 64
    for i in range(8):
        first, second = gbuf[2 * i], gbuf[2 * i + 1]
        tile = slice(128 * i, 128 * i + 128)
        g1[:, tile] = jnp.where(lane, first, pltpu.roll(second, 64, axis=1))[:1]
        g2[:, tile] = jnp.where(lane, pltpu.roll(first, 64, axis=1), second)[:1]
    own_x.wait()
    x_copy.wait_recv()

    @each(8)
    def _(i):
        rows = cols(i, 32)
        val = xp[rows].astype(F32)
        n_s[rows] = (val * rms(val) * g1[...]).astype(BF16)

    def turned(val):
        return val.astype(F32).T.astype(BF16)

    for item in p_qkv:
        item.advance(1)
    for item in p_d:
        item.advance(0)

    @each(4)
    def _(i):
        nbuf[y, c, cols(i, 256)] = turned(n_s[:, cols(i, 256)])

    for item in p_o:
        item.advance(1)
    for item in p_g + p_u:
        item.advance(0)
    for item in p_qkv:
        item.advance(2)
    trig_copy.wait_recv()

    def weight(buf, tile):
        block = buf[(ALL,) * (len(buf.shape) - 1) + (tile,)]
        return block.reshape(-1, block.shape[-1])

    def project(buf, dst, width, tiles):
        @each(tiles)
        def _(j):
            tile = cols(j, width)
            dst[:, tile] = nn(n_s[...], weight(buf, tile)).astype(BF16)

    for item in p_qkv:
        item.arrived()
    project(bq, q_s, 512, 2)
    project(bk, k_s, 512, 1)
    project(bv, v_s, 512, 1)
    scale = HD ** -0.5

    def sequence_head(j):
        seq, head = lax.div(j, 4), lax.rem(j, 4)
        return seq, head, cols(seq, T), cols(head, HD), cols(head, 2 * HD)

    @each(8)
    def _(j):
        seq, _, rows, kv, pair = sequence_head(j)
        cos, sin = trig[seq, :, :HD], trig[seq, :, HD:]
        k_rot = head_forward(k_s[rows, kv], gk, cos, sin)
        kr[rows, kv] = k_rot
        q_pair = q_s[rows, pair]
        q_rot = jnp.concatenate(
            [head_forward(half, gq, cos, sin) for half in (q_pair[:, :HD], q_pair[:, HD:])], axis=0
        )
        qr[j] = q_rot
        scores = nt(q_rot, k_rot) * scale
        row = lax.rem(lax.broadcasted_iota(jnp.int32, (2 * T, T), 0), T)
        col = lax.broadcasted_iota(jnp.int32, (2 * T, T), 1)
        scores = jnp.where(row >= col, scores, -1e30)
        expd = jnp.exp(scores - jnp.max(scores, axis=-1, keepdims=True))
        prob = expd / jnp.sum(expd, axis=-1, keepdims=True)
        probs[j] = prob
        out = nn(prob.astype(BF16), v_s[rows, kv])
        ctx[rows, pair] = jnp.concatenate([out[:T], out[T:]], axis=1).astype(BF16)

    def pair_sum(partial, landing, compute):
        copies = []
        for half in range(2):
            @each(2)
            def _(j):
                i = j + 2 * half
                partial[:, :, cols(i, 256)] = compute(i).reshape(2, T, 256)

            span = (ALL, pl.ds(512 * half, 512))
            copies.append(near_copy(Z, partial.at[(1 - z,) + span], landing.at[span]))
            copies[-1].start()
        return copies

    def received(copies):
        for copy in copies:
            copy.wait_recv()

    for item in p_o:
        item.arrived()
    a_copies = pair_sum(part_a, land_a, lambda i: nn(ctx[...], weight(bo, cols(i, 256))))
    for item in p_g + p_u:
        item.advance(1)
    for item in p_d:
        item.advance(1)

    @each(4)
    def _(i):
        ct_ref[two(i)] = turned(ctx[:, cols(i, 256)]).reshape(2, 128, 2 * T)

    received(a_copies)

    @each(4)
    def _(i):
        rows = cols(i, 32)
        attn = (part_a[z, rows] + land_a[rows]).astype(BF16)
        val = (xp[pair_rows(i)].astype(F32) + attn.astype(F32)).astype(BF16).astype(F32)
        h_s[rows] = val
        m_s[pair_rows(i)] = (val * rms(val) * g2[...]).astype(BF16)

    m_copy = near_copy(Z, m_s.at[mine], m_s.at[mine])
    m_copy.start()
    for item in p_d:
        item.arrived()
    own_dy.wait()
    dy_copy.wait_recv()

    @each(4)
    def _(i):
        dact[:, cols(i, 384)] = nt(dybuf[y, c].reshape(2 * T, D), bd[two(i)].reshape(384, D))

    m_copy.wait_recv()

    @each(4)
    def _(i):
        mbuf[x, c, cols(i, 256)] = turned(m_s[:, cols(i, 256)])

    for item in p_g + p_u:
        item.advance(2)
    p_m.begin()
    p_n.begin()
    p_dy.begin()
    e_c.begin()
    for item in p_g + p_u:
        item.arrived()
    fh = FF // 2

    @each(fh // 256)
    def _(j):
        tile = cols(j, 256)
        gate_val = nn(m_s[...], weight(bg, tile)).astype(BF16).astype(F32)
        up_val = nn(m_s[...], weight(bu, tile)).astype(BF16).astype(F32)
        sig = jax.nn.sigmoid(gate_val)
        act[:, tile] = (gate_val * sig * up_val).astype(BF16)
        d_act = dact[:, tile]
        dgu[:, tile] = (d_act * up_val * sig * (1.0 + gate_val * (1.0 - sig))).astype(BF16)
        dgu[:, cols(j + fh // 256, 256)] = (d_act * gate_val * sig).astype(BF16)

    def d_mlp_in(i):
        rows = two(i)
        return nt(dgu[:, :fh], bg[rows].reshape(256, fh)) + nt(dgu[:, fh:], bu[rows].reshape(256, fh))

    e_gu.begin()
    m_copies = pair_sum(part_m, land_m, d_mlp_in)

    @each(4)
    def _(i):
        at_ref[two(i)] = turned(act[:, cols(i, 384)]).reshape(2, 192, 2 * T)

    e_a.begin()
    received(m_copies)

    def d_res_rows(i, total):
        rows = cols(i, 32)
        val = h_s[rows]
        r_scale = rms(val)
        unit = val * r_scale
        grad = part_m[z, rows] + land_m[rows]
        out = dybuf[y, c, z, rows].astype(F32) + norm_backward(grad * g2[...], unit, r_scale)
        dres[rows] = out
        drbuf[x, c, z, rows] = out.astype(BF16)
        return total + jnp.sum(grad * unit, axis=0, keepdims=True)

    d_g2 = loop(4, d_res_rows, jnp.zeros((1, D), F32))
    r_copy = near_copy(Z, drbuf.at[x, c, z], drbuf.at[x, c, z])
    r_copy.start()
    y_copies = pair_sum(part_y, land_y, lambda i: nn(act[...], weight(bd, cols(i, 256))))
    r_copy.wait_recv()
    p_dr.begin()

    @each(2)
    def _(i):
        dctx[:, cols(i, 512)] = nt(drbuf[x, c].reshape(2 * T, D), bo[i].reshape(512, D)).astype(BF16)

    def attend_back(j, carry):
        q_total, k_total = carry
        seq, head, rows, kv, pair = sequence_head(j)
        cos, sin = trig[seq, :, :HD], trig[seq, :, HD:]
        d_out = dctx[rows, pair]
        d_out = jnp.concatenate([d_out[:, :HD], d_out[:, HD:]], axis=0)
        prob = probs[j]
        d_value = tn(prob.astype(BF16), d_out).astype(BF16)
        d_prob = nt(d_out, v_s[rows, kv])
        d_score = prob * (d_prob - jnp.sum(prob * d_prob, axis=-1, keepdims=True))
        d_score = (d_score * scale).astype(BF16)
        d_q_rot = nn(d_score, kr[rows, kv])
        d_k_rot = tn(d_score, qr[j])
        q_pair = q_s[rows, pair]
        d_q0, g_q0 = head_backward(d_q_rot[:T], q_pair[:, :HD], gq, cos, sin)
        d_q1, g_q1 = head_backward(d_q_rot[T:], q_pair[:, HD:], gq, cos, sin)
        d_k, g_k = head_backward(d_k_rot, k_s[rows, kv], gk, cos, sin)
        dqkv[rows, pair] = jnp.concatenate([d_q0, d_q1], axis=1)
        dqkv[rows, cols(head + 8, HD)] = d_k
        dqkv[rows, cols(head + 12, HD)] = d_value
        return q_total + g_q0 + g_q1, k_total + g_k

    zero = jnp.zeros((1, HD), F32)
    q_total, k_total = loop(8, attend_back, (zero, zero))
    e_qkv.begin()

    def d_normed(i):
        rows = two(i)
        grad = nt(dqkv[:, :D], bq[rows].reshape(256, D)) + nt(dqkv[:, D : D + 512], bk[rows].reshape(256, 512))
        return grad + nt(dqkv[:, D + 512 :], bv[rows].reshape(256, 512))

    n_copies = pair_sum(part_n, land_n, d_normed)
    inv_tokens = 1.0 / (16 * T)

    def column_chunk(acts, grads, out, chunk):
        @each(8)
        def _(i):
            rows = cols(i, 128)
            left = jnp.concatenate([acts[k // 2, k % 2, rows] for k in range(4)], axis=1)
            right = grads[:, :, 256 * chunk : 256 * chunk + 256].reshape(8 * T, 256)
            out[(chunk,) + three(i)] = (nn(left, right) * inv_tokens).reshape(2, 64, 256)

    def half_of(dim, result, chunk):
        bit = place.bit[dim]
        return result.at[(chunk,) + tuple(1 - bit if k == dim else ALL for k in range(4))]

    def row_tiles(left_buf, right_buf, out):
        @each(8)
        def _(j):
            tile = cols(lax.rem(j, 4), 256)
            half = lax.div(j, 4)
            left = jnp.concatenate([left_buf[i, half] for i in range(4)], axis=1)
            out[half, :, tile] = nn(left, weight(right_buf, tile)) * inv_tokens

    p_m.advance(0)
    p_m.arrived()
    e_gu.arrived()
    gu_far = []
    for chunk in range(3):
        column_chunk(mbuf, gubuf, rgu, chunk)
        gu_far.append(near_copy(Y, half_of(Y, rgu, chunk), zgu.at[chunk]))
        gu_far[-1].start()
    p_n.advance(0)
    p_n.arrived()
    e_qkv.arrived()
    qkv_far = []
    for chunk in range(2):
        column_chunk(nbuf, qkvbuf, rqkv, chunk)
        qkv_far.append(near_copy(X, half_of(X, rqkv, chunk), zqkv.at[chunk]))
        qkv_far[-1].start()
    p_dy.advance(0)
    p_dy.arrived()
    e_a.arrived()
    row_tiles(abuf, dybuf, rwd)
    wd_far = near_copy(X, rwd.at[1 - x], zwd)
    wd_far.start()
    p_dr.advance(0)
    p_dr.arrived()
    e_c.arrived()
    row_tiles(cbuf, drbuf, rwo)
    wo_far = near_copy(Y, rwo.at[1 - y], zwo)
    wo_far.start()

    received(n_copies)

    def d_hidden_rows(i, total):
        rows = cols(i, 32)
        val = xp[pair_rows(i)].astype(F32)
        x_scale = rms(val)
        unit = val * x_scale
        grad = part_n[z, rows] + land_n[rows]
        dh_ref[rows] = (dres[rows] + norm_backward(grad * g1[...], unit, x_scale)).astype(BF16)
        return total + jnp.sum(grad * unit, axis=0, keepdims=True)

    d_g1 = loop(4, d_hidden_rows, jnp.zeros((1, D), F32))
    for i in range(8):
        tile = slice(128 * i, 128 * i + 128)
        gpart[i : i + 1, :] = d_g1[:, tile]
        gpart[8 + i : 9 + i, :] = d_g2[:, tile]
    gpart[16:17, :] = q_total
    gpart[17:18, :] = k_total
    gpart[18:24, :] = jnp.zeros((6, 128), F32)

    to_all(gpart, gainbuf, gain_number)
    received(y_copies)

    @each(4)
    def _(i):
        rows = cols(i, 32)
        out = (part_y[z, rows] + land_y[rows]).astype(BF16).astype(F32)
        y_ref[rows] = (h_s[rows] + out).astype(BF16)

    def final(dim, number, result, target, out, chunk, base):
        group = Group(place, tuple(k for k in range(4) if k != dim))
        for bit in list(group.others()) + [place.bit]:
            index = (chunk,) + tuple(bit)
            result[index] = result[index] + target[(chunk,) + tuple(bit[k] for k in group.axes)]
        where = pl.ds(pl.multiple_of(base + 256 * chunk, 128), 256)
        move = Exchange(
            group, number, lambda bit: result.at[(chunk,) + tuple(bit)], out.at[:, where],
            out.at[:, pl.ds(0, 7 * 256)], one,
        )
        move.begin()
        return move

    gu_base = x * FF + z * fh + c * 768
    qkv_base = (1 - y) * (z * D + c * 512) + y * (NQ + c * D + z * 512)
    moves = []
    for kind, chunk in ((0, 0), (1, 0), (0, 1), (1, 1), (0, 2)):
        if kind == 0:
            gu_far[chunk].wait_recv()
            moves.append(final(Y, 4 + chunk, rgu, zgu, ogu, chunk, gu_base))
        else:
            qkv_far[chunk].wait_recv()
            moves.append(final(X, 7 + chunk, rqkv, zqkv, oqkv, chunk, qkv_base))
    wd_far.wait_recv()
    owd[...] = rwd[x] + zwd[...]
    wo_far.wait_recv()
    owo[...] = rwo[y] + zwo[...]
    all_wait(gainbuf, one_recv.at[gain_number])
    gainbuf[me] = gpart[...]
    gainbuf[0] = loop(16, lambda i, total: total + gainbuf[i], jnp.zeros((24, 128), F32)) * inv_tokens
    for i in range(2):
        row = gainbuf[0, pl.ds(8 * i + lax.div(me, 2), 1), :]
        ogain[i : i + 1, :] = jnp.where(c == 0, row, pltpu.roll(row, 64, axis=1))
    ogain[2:4, :] = gainbuf[0, 16:18, :]
    ogain[4:8, :] = jnp.zeros((4, 128), F32)
    for move in moves:
        move.arrived()
    for item in moves + [e_gu, e_qkv, e_a, e_c] + parts:
        item.drain()
    for copy in sent:
        copy.wait_send()
    all_wait(gainbuf, one_send.at[gain_number])
    all_wait(gbuf, one_send.at[norm_number])


def shape(rows, width, dtype):
    return jax.ShapeDtypeStruct((rows, width), dtype)


def many(count, *args):
    return [VM(*args)] * count


def layer_call(*operands):
    vmem = pl.BlockSpec(memory_space=VM)
    hbm = pl.BlockSpec(memory_space=pl.ANY)
    dma = pltpu.SemaphoreType.DMA
    t2, kvh, fh = 2 * T, D // 2, FF // 2
    cube, square, line = (2, 2, 2, 2), (2, 2, 2), (2, 2)
    spreads = 18
    return pl.pallas_call(
        layer_kernel,
        name="layer",
        out_shape=(
            shape(T, D, BF16), shape(T, D, BF16), shape(64, NQ + 2 * D, F32), shape(64, 2 * FF, F32),
            shape(128, D, F32), shape(192, D, F32), shape(8, 128, F32),
        ),
        in_specs=[vmem] * 6 + [hbm] * 9,
        out_specs=(vmem, vmem, hbm, hbm, vmem, vmem, vmem),
        scratch_shapes=[
            VM((8, 128), F32), VM((16, 8, 128), F32), VM(cube + (64, D), BF16), *many(2, cube + (64, kvh), BF16),
            VM(square + (128, D), BF16), *many(2, cube + (64, fh), BF16), VM(square + (192, D), BF16),
            *many(2, (1, D), F32),
            VM((t2, D), BF16), VM((2, T, t2), F32), VM((t2, D), BF16), VM((t2, D), BF16), *many(2, (t2, kvh), BF16),
            VM((8, t2, HD), BF16), VM((t2, kvh), BF16), VM((8, t2, T), F32), VM((t2, D), BF16), VM((T, D), F32),
            VM((t2, D), BF16), VM((8, 128), BF16), VM((t2, fh), BF16), VM((t2, fh), F32), VM((t2, D), BF16),
            VM((T, D), F32), *many(4, (2, T, D), F32), *many(4, (T, D), F32),
            VM(square + (192, t2), BF16), VM(square + (128, t2), BF16), VM((t2, NQ), BF16), VM((t2, FF), BF16),
            VM((24, 128), F32), *many(2, line + (D, t2), BF16), *many(2, line + (2, T, D), BF16),
            VM((4, t2, 768), BF16), VM((4, t2, 512), BF16), VM((4, 2, 192, t2), BF16), VM((4, 2, 128, t2), BF16),
            VM((3,) + cube + (64, 256), F32), VM((2,) + cube + (64, 256), F32), VM((2, 192, D), F32),
            VM((2, 128, D), F32), VM((3,) + square + (64, 256), F32), VM((2,) + square + (64, 256), F32),
            VM((192, D), F32), VM((128, D), F32), VM((16, 24, 128), F32),
            *[dma((spreads, 3))] * 2, *[dma((spreads, 4))] * 2, dma((spreads + 2,)), *[dma((11,))] * 3, *[dma((20,))] * 2,
        ],
        compiler_params=pltpu.CompilerParams(collective_id=0, has_side_effects=True, vmem_limit_bytes=HIGH_VMEM),
    )(*operands)


def deliver_kernel(y_in, dh_in, qkv_in, gu_in, wo_in, wd_in, gain_in, *refs):
    outs, gains_out, scratch, (in_sem, out_sem) = refs[:9], refs[9:13], refs[13:22], refs[22:]
    spans = ((qkv_in, 0, NQ), (qkv_in, NQ, D), (qkv_in, NQ + D, D), (gu_in, 0, FF), (gu_in, FF, FF))
    q_in, k_in, v_in, g_in, u_in = (ref.at[:, pl.ds(start, size)] for ref, start, size in spans)
    sources = (y_in, dh_in, q_in, k_in, v_in, wo_in, g_in, u_in, wd_in)
    loads = [pltpu.make_async_copy(src, buf, in_sem.at[i]) for i, (src, buf) in enumerate(zip(sources, scratch))]
    stores = [pltpu.make_async_copy(buf, out, out_sem.at[i]) for i, (buf, out) in enumerate(zip(scratch, outs))]
    for load in loads:
        load.start()
    for i, out in enumerate(gains_out):
        out[...] = gain_in[i : i + 1, : out.shape[0]].reshape(out.shape)
    for load, store in zip(loads, stores):
        load.wait()
        store.start()
    for store in stores:
        store.wait()


def deliver(*results):
    vmem = pl.BlockSpec(memory_space=VM)
    hbm = pl.BlockSpec(memory_space=pl.ANY)
    dma = pltpu.SemaphoreType.DMA
    sizes = [(T, D, BF16)] * 2 + [(64, width, F32) for width in (NQ, D, D)] + [(128, D, F32)]
    sizes += [(64, FF, F32)] * 2 + [(192, D, F32)]
    small = [jax.ShapeDtypeStruct((size,), F32) for size in (64, 64, 128, 128)]
    return pl.pallas_call(
        deliver_kernel,
        name="deliver",
        out_shape=tuple([shape(*size) for size in sizes] + small),
        in_specs=[hbm] * 6 + [vmem],
        out_specs=tuple([hbm] * 9 + [vmem] * 4),
        scratch_shapes=[VM(size[:2], size[2]) for size in sizes] + [dma((9,)), dma((9,))],
    )(*results)


def rope_tables(positions):
    inv_freq = ROPE_THETA ** (-2.0 * jnp.arange(HD // 2, dtype=F32) / HD)
    angle = positions.reshape(-1, 1).astype(F32) * inv_freq
    cos_half, sin_half = jnp.cos(angle), jnp.sin(angle)
    return cos_half, sin_half


def solution(mesh):
    axis_name = mesh.axis_names[0]
    sharded = P(axis_name)
    in_specs = (sharded,) * 5 + (P(), P()) + (sharded,) * 7
    out_specs = (sharded,) * 4 + (P(), P()) + (sharded,) * 7

    def device_step(hidden, grad_out, positions, norm1, norm2, gain_q, gain_k, w_q, w_k, w_v, w_o, w_gate, w_up, w_down):
        cos, sin = rope_tables(positions)
        x, dy = hidden.reshape(T, D), grad_out.reshape(T, D)
        results = layer_call(cos, sin, norm1, norm2, gain_q, gain_k, x, dy, w_q, w_k, w_v, w_o, w_gate, w_up, w_down)
        out, d_hidden, d_wq, d_wk, d_wv, d_wo, d_wg, d_wu, d_wd, d_n1, d_n2, d_qn, d_kn = deliver(*results)
        out, d_hidden = out.reshape(hidden.shape), d_hidden.reshape(hidden.shape)
        return out, d_hidden, d_n1, d_n2, d_qn, d_kn, d_wq, d_wk, d_wv, d_wo, d_wg, d_wu, d_wd

    return jax.shard_map(device_step, mesh=mesh, in_specs=in_specs, out_specs=out_specs, check_vma=False)
```

```python
import jax
import jax.numpy as jnp
from jax import lax
from jax.experimental import pallas as pl
from jax.experimental.pallas import tpu as pltpu
from jax.sharding import PartitionSpec as P

RMS_EPS = 1e-6
ROPE_THETA = 1000000.0
MESH = pl.DeviceIdType.MESH
F32 = jnp.float32
BF16 = jnp.bfloat16
T = 128
D = 1024
NQ = 2048
FF = 3072
HD = 128
Z, Y, X, C = 0, 1, 2, 3
STRIDE = (8, 4, 2, 1)
ALL = slice(None)
VM = pltpu.VMEM
HIGH_VMEM = 67043328


def nn(left_op, right_op):
    return jnp.dot(left_op, right_op, preferred_element_type=F32)


def nt(left_op, right_op):
    return lax.dot_general(left_op, right_op, (((1,), (1,)), ((), ())), preferred_element_type=F32)


def tn(left_op, right_op):
    return lax.dot_general(left_op, right_op, (((0,), (0,)), ((), ())), preferred_element_type=F32)


def rms(val):
    return lax.rsqrt(jnp.mean(val * val, axis=-1, keepdims=True) + RMS_EPS)


def norm_backward(d_unit, unit_val, scale_val):
    return scale_val * (d_unit - unit_val * jnp.mean(d_unit * unit_val, axis=-1, keepdims=True))


class Place:
    def __init__(self):
        self.me = lax.axis_index("fsdp")
        self.bit = [lax.rem(lax.div(self.me, s), 2) for s in STRIDE]

    def near(self, dim):
        return (self.me + STRIDE[dim] * (1 - 2 * self.bit[dim]),)

    def greet(self, dims):
        barrier = pltpu.get_barrier_semaphore()
        for dim in dims:
            pl.semaphore_signal(barrier, inc=1, device_id=self.near(dim), device_id_type=MESH)
        pl.semaphore_wait(barrier, len(dims))


class Spread:
    def __init__(self, place, own, first, buf, sub, order, axes, sems, part):
        self.place, self.buf, self.sub, self.order, self.axes = place, buf, sub, order, axes
        self.link_send, self.link_recv, self.core_send, self.core_recv, self.local_sem = sems
        self.part, self.last = part, len(order)
        self.source = own
        self.mine = self.block(()) if own is None else own
        self.first = self.mine if first is None else first

    def block(self, full, flip=None):
        index = []
        for dim in self.axes:
            if dim in full:
                index.append(ALL)
            elif dim == flip:
                index.append(1 - self.place.bit[dim])
            else:
                index.append(self.place.bit[dim])
        return self.buf.at[tuple(index) + self.sub]

    def copy_own(self):
        return pltpu.make_async_copy(self.source, self.block(()), self.local_sem.at[self.part])

    def link(self, step):
        dst = self.block(self.order[:step])
        return pltpu.make_async_remote_copy(
            src_ref=self.first if step == 0 else dst,
            dst_ref=dst,
            send_sem=self.link_send.at[self.part, step],
            recv_sem=self.link_recv.at[self.part, step],
            device_id=self.place.near(self.order[step]),
            device_id_type=MESH,
        )

    def core(self, step):
        dst = self.block(()) if step == 0 else self.block(self.order[: step - 1], self.order[step - 1])
        return pltpu.make_async_remote_copy(
            src_ref=self.mine if step == 0 else dst,
            dst_ref=dst,
            send_sem=self.core_send.at[self.part, step],
            recv_sem=self.core_recv.at[self.part, step],
            device_id=self.place.near(C),
            device_id_type=MESH,
        )

    def begin(self):
        self.link(0).start()
        if self.source is not None:
            self.copy_own().start()
        self.core(0).start()

    def advance(self, step):
        if step == 0 and self.source is not None:
            self.copy_own().wait()
        self.link(step).wait_recv()
        if step + 1 < self.last:
            self.link(step + 1).start()
        self.core(step + 1).start()

    def arrived(self):
        for step in range(self.last + 1):
            self.core(step).wait_recv()

    def drain(self):
        for step in range(self.last):
            self.link(step).wait_send()
        for step in range(self.last + 1):
            self.core(step).wait_send()


class Group:
    def __init__(self, place, axes):
        self.place, self.axes = place, axes
        self.position = self.spot(place.bit)

    def others(self):
        for number in range(2 ** len(self.axes) - 1, 0, -1):
            bit = list(self.place.bit)
            for i, dim in enumerate(self.axes):
                if number >> i & 1:
                    bit[dim] = 1 - bit[dim]
            yield bit

    def spot(self, bit):
        total = 0
        for dim in self.axes:
            total = total * 2 + bit[dim]
        return total


def device_of(bit):
    return (sum(stride * value for stride, value in zip(STRIDE, bit)),)


class Exchange:
    def __init__(self, group, number, piece, slot, blocks, sems):
        self.group, self.piece, self.slot, self.blocks = group, piece, slot, blocks
        self.send, self.recv, self.local = (sem.at[number] for sem in sems)

    def own(self):
        return pltpu.make_async_copy(self.piece(self.group.place.bit), self.slot, self.local)

    def begin(self):
        for bit in self.group.others():
            pltpu.make_async_remote_copy(
                src_ref=self.piece(bit),
                dst_ref=self.slot,
                send_sem=self.send,
                recv_sem=self.recv,
                device_id=device_of(bit),
                device_id_type=MESH,
            ).start()
        self.own().start()

    def arrived(self):
        self.own().wait()
        pltpu.make_async_copy(self.blocks, self.blocks, self.recv).wait()

    def drain(self):
        pltpu.make_async_copy(self.blocks, self.blocks, self.send).wait()


def head_forward(proj, gain, cos, sin):
    val = proj.astype(F32)
    scaled = val * rms(val) * gain
    return (scaled * cos + pltpu.roll(scaled, 64, axis=1) * sin).astype(BF16)


def head_backward(d_rot, proj, gain, cos, sin):
    val = proj.astype(F32)
    scale = rms(val)
    unit = val * scale
    d_scaled = d_rot * cos - pltpu.roll(d_rot, 64, axis=1) * sin
    d_gain = jnp.sum(d_scaled * unit, axis=0, keepdims=True)
    return norm_backward(d_scaled * gain, unit, scale).astype(BF16), d_gain


def cols(i, width):
    return pl.ds(pl.multiple_of(i * width, width), width)


def loop(count, body, init=0):
    return lax.fori_loop(0, count, body, init)


def each(count):
    def run(body):
        def step(i, _):
            body(i)
            return 0

        loop(count, step)

    return run


def two(i):
    return lax.div(i, 2), lax.rem(i, 2)


def three(i):
    return two(lax.div(i, 2)) + (lax.rem(i, 2),)


def layer_kernel(
    cos_ref, sin_ref, n1_ref, n2_ref, qn_ref, kn_ref, x_ref, dy_ref, wq, wk, wv, wo, wg, wu, wd,
    y_ref, dh_ref, oqkv, ogu, owo, owd, ogain,
    gains, gbuf, bq, bk, bv, bo, bg, bu, bd, g1, g2,
    xp, trig, n_s, q_s, k_s, v_s, qr, kr, probs, ctx, h_s, m_s, spare, act, dact, dctx, dres,
    part_a, part_y, part_m, part_n, land_a, land_y, land_m, land_n,
    at_ref, ct_ref, dqkv, dgu, gpart,
    nbuf, mbuf, dybuf, drbuf, gubuf, qkvbuf, abuf, cbuf,
    rgu, rqkv, rwd, rwo, zgu, zqkv, zwd, zwo, gainbuf,
    link_send, link_recv, core_send, core_recv, local_sem, one_send, one_recv, one_local, far_send, far_recv,
):
    place = Place()
    me = place.me
    z, y, x, c = place.bit
    sems = (link_send, link_recv, core_send, core_recv, local_sem)
    one = (one_send, one_recv, one_local)
    parts = []

    def spread(own, first, buf, sub, order, axes):
        parts.append(Spread(place, own, first, buf, sub, order, axes, sems, len(parts)))
        return parts[-1]

    both = (ALL, ALL)
    turns = ((Y, X), (X, Y))

    def by_columns(src, buf):
        half = src.shape[1] // 2
        size = half // 2
        made = []
        for i in range(2):
            mine, theirs = (src.at[:, pl.ds(pl.multiple_of(side * half + i * size, size), size)] for side in (z, 1 - z))
            made.append(spread(mine, theirs, buf, (ALL, pl.ds(i * size, size)), (Z,) + turns[i], (Z, Y, X, C)))
        return made

    def by_rows(src, buf):
        size = src.shape[0] // 2
        made = []
        for i in range(2):
            rows = pl.ds(i * size, size)
            made.append(spread(src.at[rows], None, buf, (rows, ALL), turns[i], (Y, X, C)))
        return made

    p_qkv = by_columns(wq, bq) + by_columns(wk, bk) + by_columns(wv, bv)
    p_o, p_d = by_rows(wo, bo), by_rows(wd, bd)
    p_g, p_u = by_columns(wg, bg), by_columns(wu, bu)
    p_m = spread(None, None, mbuf, both, (X,), (X, C))
    p_n = spread(None, None, nbuf, both, (Y,), (Y, C))
    p_dy = spread(None, None, dybuf, (ALL, ALL, ALL), (Y,), (Y, C))
    p_dr = spread(None, None, drbuf, (ALL, ALL, ALL), (X,), (X, C))

    grp_x, grp_y = Group(place, (X, C)), Group(place, (Y, C))

    def share(number, group, piece, buf):
        return Exchange(group, number, piece, buf.at[group.position], buf.at[pl.ds(0, 3)], one)

    def cols_for(group, ref, width):
        return lambda bit: ref.at[:, pl.ds(pl.multiple_of(group.spot(bit) * width, 128), width)]

    e_gu = share(0, grp_x, cols_for(grp_x, dgu, 768), gubuf)
    e_qkv = share(1, grp_y, cols_for(grp_y, dqkv, 512), qkvbuf)
    e_a = share(2, grp_y, lambda bit: at_ref.at[bit[Y], :, bit[C]], abuf)
    e_c = share(3, grp_x, lambda bit: ct_ref.at[:, bit[X], bit[C]], cbuf)
    gain_number, norm_number = 9, 10
    sent = []

    def near_copy(dim, source, target):
        number = len(sent)
        sent.append(
            pltpu.make_async_remote_copy(
                src_ref=source, dst_ref=target, send_sem=far_send.at[number], recv_sem=far_recv.at[number],
                device_id=place.near(dim), device_id_type=MESH,
            )
        )
        return sent[-1]

    mine = cols(z, T)

    def pair_rows(i):
        return cols(4 * z + i, 32)

    barrier = pltpu.get_barrier_semaphore()

    def other(k):
        return (lax.rem(me + k, 16),)

    @each(15)
    def _(k):
        pl.semaphore_signal(barrier, inc=1, device_id=other(k + 1), device_id_type=MESH)

    gains[...] = jnp.zeros((8, 128), F32)
    halves = [ref[...].astype(F32).reshape(1, 64) for ref in (n1_ref, n2_ref)]
    gains[0:1, :] = jnp.concatenate(halves, axis=1)
    gains[1:2, :] = qn_ref[...].astype(F32).reshape(1, 128)
    gains[2:3, :] = kn_ref[...].astype(F32).reshape(1, 128)
    cos_half, sin_half = cos_ref[...], sin_ref[...]
    trig[z] = jnp.concatenate([cos_half, cos_half, -sin_half, sin_half], axis=1)
    pl.semaphore_wait(barrier, 15)

    def to_all(source, buf, number):
        @each(15)
        def _(k):
            pltpu.make_async_remote_copy(
                src_ref=source, dst_ref=buf.at[me], send_sem=one_send.at[number], recv_sem=one_recv.at[number],
                device_id=other(k + 1), device_id_type=MESH,
            ).start()

    def all_wait(buf, sem):
        fifteen = buf.at[pl.ds(0, 15)]
        pltpu.make_async_copy(fifteen, fifteen, sem).wait()

    to_all(gains, gbuf, norm_number)
    for item in p_qkv + p_o:
        item.begin()
    x_copy = near_copy(Z, x_ref, xp.at[mine])
    trig_copy = near_copy(Z, trig.at[z], trig.at[z])
    x_copy.start()
    own_x = pltpu.make_async_copy(x_ref, xp.at[mine], local_sem.at[len(parts)])
    own_x.start()
    for item in p_d + p_g + p_u:
        item.begin()
    trig_copy.start()
    dy_copy = near_copy(Z, dy_ref, dybuf.at[y, c, z])
    dy_copy.start()
    own_dy = pltpu.make_async_copy(dy_ref, dybuf.at[y, c, z], local_sem.at[len(parts) + 1])
    own_dy.start()
    for item in p_qkv + p_o:
        item.advance(0)
    gq, gk = gains[1:2, :], gains[2:3, :]
    all_wait(gbuf, one_recv.at[norm_number])
    gbuf[me] = gains[...]
    lane = lax.broadcasted_iota(jnp.int32, (8, 128), 1) < 64
    for i in range(8):
        first, second = gbuf[2 * i], gbuf[2 * i + 1]
        tile = slice(128 * i, 128 * i + 128)
        g1[:, tile] = jnp.where(lane, first, pltpu.roll(second, 64, axis=1))[:1]
        g2[:, tile] = jnp.where(lane, pltpu.roll(first, 64, axis=1), second)[:1]
    own_x.wait()
    x_copy.wait_recv()

    @each(8)
    def _(i):
        rows = cols(i, 32)
        val = xp[rows].astype(F32)
        n_s[rows] = (val * rms(val) * g1[...]).astype(BF16)

    def turned(val):
        return val.astype(F32).T.astype(BF16)

    for item in p_qkv:
        item.advance(1)
    for item in p_d:
        item.advance(0)

    @each(4)
    def _(i):
        nbuf[y, c, cols(i, 256)] = turned(n_s[:, cols(i, 256)])

    for item in p_o:
        item.advance(1)
    for item in p_g + p_u:
        item.advance(0)
    for item in p_qkv:
        item.advance(2)
    trig_copy.wait_recv()

    def weight(buf, tile):
        block = buf[(ALL,) * (len(buf.shape) - 1) + (tile,)]
        return block.reshape(-1, block.shape[-1])

    def project(buf, dst, width, tiles):
        @each(tiles)
        def _(j):
            tile = cols(j, width)
            dst[:, tile] = nn(n_s[...], weight(buf, tile)).astype(BF16)

    for item in p_qkv:
        item.arrived()
    project(bq, q_s, 512, 2)
    project(bk, k_s, 512, 1)
    project(bv, v_s, 512, 1)
    scale = HD ** -0.5

    def sequence_head(j):
        seq, head = lax.div(j, 4), lax.rem(j, 4)
        return seq, head, cols(seq, T), cols(head, HD), cols(head, 2 * HD)

    @each(8)
    def _(j):
        seq, _, rows, kv, pair = sequence_head(j)
        cos, sin = trig[seq, :, :HD], trig[seq, :, HD:]
        k_rot = head_forward(k_s[rows, kv], gk, cos, sin)
        kr[rows, kv] = k_rot
        q_pair = q_s[rows, pair]
        q_rot = jnp.concatenate(
            [head_forward(half, gq, cos, sin) for half in (q_pair[:, :HD], q_pair[:, HD:])], axis=0
        )
        qr[j] = q_rot
        scores = nt(q_rot, k_rot) * scale
        row = lax.rem(lax.broadcasted_iota(jnp.int32, (2 * T, T), 0), T)
        col = lax.broadcasted_iota(jnp.int32, (2 * T, T), 1)
        scores = jnp.where(row >= col, scores, -1e30)
        expd = jnp.exp(scores - jnp.max(scores, axis=-1, keepdims=True))
        prob = expd / jnp.sum(expd, axis=-1, keepdims=True)
        probs[j] = prob
        out = nn(prob.astype(BF16), v_s[rows, kv])
        ctx[rows, pair] = jnp.concatenate([out[:T], out[T:]], axis=1).astype(BF16)

    def pair_sum(partial, landing, compute):
        copies = []
        for half in range(2):
            @each(2)
            def _(j):
                i = j + 2 * half
                partial[:, :, cols(i, 256)] = compute(i).reshape(2, T, 256)

            span = (ALL, pl.ds(512 * half, 512))
            copies.append(near_copy(Z, partial.at[(1 - z,) + span], landing.at[span]))
            copies[-1].start()
        return copies

    def received(copies):
        for copy in copies:
            copy.wait_recv()

    for item in p_o:
        item.arrived()
    a_copies = pair_sum(part_a, land_a, lambda i: nn(ctx[...], weight(bo, cols(i, 256))))
    for item in p_g + p_u:
        item.advance(1)
    for item in p_d:
        item.advance(1)

    @each(4)
    def _(i):
        ct_ref[two(i)] = turned(ctx[:, cols(i, 256)]).reshape(2, 128, 2 * T)

    received(a_copies)

    @each(4)
    def _(i):
        rows = cols(i, 32)
        attn = (part_a[z, rows] + land_a[rows]).astype(BF16)
        val = (xp[pair_rows(i)].astype(F32) + attn.astype(F32)).astype(BF16).astype(F32)
        h_s[rows] = val
        m_s[pair_rows(i)] = (val * rms(val) * g2[...]).astype(BF16)

    m_copy = near_copy(Z, m_s.at[mine], m_s.at[mine])
    m_copy.start()
    for item in p_d:
        item.arrived()
    own_dy.wait()
    dy_copy.wait_recv()

    @each(4)
    def _(i):
        dact[:, cols(i, 384)] = nt(dybuf[y, c].reshape(2 * T, D), bd[two(i)].reshape(384, D))

    m_copy.wait_recv()

    @each(4)
    def _(i):
        mbuf[x, c, cols(i, 256)] = turned(m_s[:, cols(i, 256)])

    for item in p_g + p_u:
        item.advance(2)
    p_m.begin()
    p_dy.begin()
    e_c.begin()
    for item in p_g + p_u:
        item.arrived()
    fh = FF // 2

    @each(fh // 256)
    def _(j):
        tile = cols(j, 256)
        gate_val = nn(m_s[...], weight(bg, tile)).astype(BF16).astype(F32)
        up_val = nn(m_s[...], weight(bu, tile)).astype(BF16).astype(F32)
        sig = jax.nn.sigmoid(gate_val)
        act[:, tile] = (gate_val * sig * up_val).astype(BF16)
        d_act = dact[:, tile]
        dgu[:, tile] = (d_act * up_val * sig * (1.0 + gate_val * (1.0 - sig))).astype(BF16)
        dgu[:, cols(j + fh // 256, 256)] = (d_act * gate_val * sig).astype(BF16)

    def d_mlp_in(i):
        rows = two(i)
        return nt(dgu[:, :fh], bg[rows].reshape(256, fh)) + nt(dgu[:, fh:], bu[rows].reshape(256, fh))

    e_gu.begin()
    m_copies = pair_sum(part_m, land_m, d_mlp_in)

    @each(4)
    def _(i):
        at_ref[two(i)] = turned(act[:, cols(i, 384)]).reshape(2, 192, 2 * T)

    e_a.begin()
    p_n.begin()
    received(m_copies)

    def d_res_rows(i, total):
        rows = cols(i, 32)
        val = h_s[rows]
        r_scale = rms(val)
        unit = val * r_scale
        grad = part_m[z, rows] + land_m[rows]
        out = dybuf[y, c, z, rows].astype(F32) + norm_backward(grad * g2[...], unit, r_scale)
        dres[rows] = out
        drbuf[x, c, z, rows] = out.astype(BF16)
        return total + jnp.sum(grad * unit, axis=0, keepdims=True)

    d_g2 = loop(4, d_res_rows, jnp.zeros((1, D), F32))
    r_copy = near_copy(Z, drbuf.at[x, c, z], drbuf.at[x, c, z])
    r_copy.start()
    y_copies = pair_sum(part_y, land_y, lambda i: nn(act[...], weight(bd, cols(i, 256))))
    inv_tokens = 1.0 / (16 * T)

    def row_tiles(left_buf, right_buf, out):
        @each(8)
        def _(j):
            tile = cols(lax.rem(j, 4), 256)
            half = lax.div(j, 4)
            left = jnp.concatenate([left_buf[i, half] for i in range(4)], axis=1)
            out[half, :, tile] = nn(left, weight(right_buf, tile)) * inv_tokens

    p_dy.advance(0)
    p_dy.arrived()
    e_a.arrived()
    row_tiles(abuf, dybuf, rwd)
    r_copy.wait_recv()
    p_dr.begin()
    wd_far = near_copy(X, rwd.at[1 - x], zwd)
    wd_far.start()

    @each(2)
    def _(i):
        dctx[:, cols(i, 512)] = nt(drbuf[x, c].reshape(2 * T, D), bo[i].reshape(512, D)).astype(BF16)

    def attend_back(j, carry):
        q_total, k_total = carry
        seq, head, rows, kv, pair = sequence_head(j)
        cos, sin = trig[seq, :, :HD], trig[seq, :, HD:]
        d_out = dctx[rows, pair]
        d_out = jnp.concatenate([d_out[:, :HD], d_out[:, HD:]], axis=0)
        prob = probs[j]
        d_value = tn(prob.astype(BF16), d_out).astype(BF16)
        d_prob = nt(d_out, v_s[rows, kv])
        d_score = prob * (d_prob - jnp.sum(prob * d_prob, axis=-1, keepdims=True))
        d_score = (d_score * scale).astype(BF16)
        d_q_rot = nn(d_score, kr[rows, kv])
        d_k_rot = tn(d_score, qr[j])
        q_pair = q_s[rows, pair]
        d_q0, g_q0 = head_backward(d_q_rot[:T], q_pair[:, :HD], gq, cos, sin)
        d_q1, g_q1 = head_backward(d_q_rot[T:], q_pair[:, HD:], gq, cos, sin)
        d_k, g_k = head_backward(d_k_rot, k_s[rows, kv], gk, cos, sin)
        dqkv[rows, pair] = jnp.concatenate([d_q0, d_q1], axis=1)
        dqkv[rows, cols(head + 8, HD)] = d_k
        dqkv[rows, cols(head + 12, HD)] = d_value
        return q_total + g_q0 + g_q1, k_total + g_k

    zero = jnp.zeros((1, HD), F32)
    q_total, k_total = loop(8, attend_back, (zero, zero))
    e_qkv.begin()

    def d_normed(i):
        rows = two(i)
        grad = nt(dqkv[:, :D], bq[rows].reshape(256, D)) + nt(dqkv[:, D : D + 512], bk[rows].reshape(256, 512))
        return grad + nt(dqkv[:, D + 512 :], bv[rows].reshape(256, 512))

    n_copies = pair_sum(part_n, land_n, d_normed)

    def column_chunk(acts, grads, out, chunk):
        @each(8)
        def _(i):
            rows = cols(i, 128)
            left = jnp.concatenate([acts[k // 2, k % 2, rows] for k in range(4)], axis=1)
            right = grads[:, :, 256 * chunk : 256 * chunk + 256].reshape(8 * T, 256)
            out[(chunk,) + three(i)] = (nn(left, right) * inv_tokens).reshape(2, 64, 256)

    def half_of(dim, result, chunk):
        bit = place.bit[dim]
        return result.at[(chunk,) + tuple(1 - bit if k == dim else ALL for k in range(4))]

    p_m.advance(0)
    p_m.arrived()
    e_gu.arrived()
    gu_far = []
    for chunk in range(3):
        column_chunk(mbuf, gubuf, rgu, chunk)
        gu_far.append(near_copy(Y, half_of(Y, rgu, chunk), zgu.at[chunk]))
        gu_far[-1].start()
    p_n.advance(0)
    p_n.arrived()
    e_qkv.arrived()
    qkv_far = []
    for chunk in range(2):
        column_chunk(nbuf, qkvbuf, rqkv, chunk)
        qkv_far.append(near_copy(X, half_of(X, rqkv, chunk), zqkv.at[chunk]))
        qkv_far[-1].start()
    p_dr.advance(0)
    p_dr.arrived()
    e_c.arrived()
    row_tiles(cbuf, drbuf, rwo)
    wo_far = near_copy(Y, rwo.at[1 - y], zwo)
    wo_far.start()

    received(n_copies)

    def d_hidden_rows(i, total):
        rows = cols(i, 32)
        val = xp[pair_rows(i)].astype(F32)
        x_scale = rms(val)
        unit = val * x_scale
        grad = part_n[z, rows] + land_n[rows]
        dh_ref[rows] = (dres[rows] + norm_backward(grad * g1[...], unit, x_scale)).astype(BF16)
        return total + jnp.sum(grad * unit, axis=0, keepdims=True)

    d_g1 = loop(4, d_hidden_rows, jnp.zeros((1, D), F32))
    for i in range(8):
        tile = slice(128 * i, 128 * i + 128)
        gpart[i : i + 1, :] = d_g1[:, tile]
        gpart[8 + i : 9 + i, :] = d_g2[:, tile]
    gpart[16:17, :] = q_total
    gpart[17:18, :] = k_total
    gpart[18:24, :] = jnp.zeros((6, 128), F32)

    to_all(gpart, gainbuf, gain_number)
    received(y_copies)

    @each(4)
    def _(i):
        rows = cols(i, 32)
        out = (part_y[z, rows] + land_y[rows]).astype(BF16).astype(F32)
        y_ref[rows] = (h_s[rows] + out).astype(BF16)

    def final(dim, number, result, target, out, chunk, base):
        group = Group(place, tuple(k for k in range(4) if k != dim))
        for bit in list(group.others()) + [place.bit]:
            index = (chunk,) + tuple(bit)
            result[index] = result[index] + target[(chunk,) + tuple(bit[k] for k in group.axes)]
        where = pl.ds(pl.multiple_of(base + 256 * chunk, 128), 256)
        move = Exchange(
            group, number, lambda bit: result.at[(chunk,) + tuple(bit)], out.at[:, where],
            out.at[:, pl.ds(0, 7 * 256)], one,
        )
        move.begin()
        return move

    gu_base = x * FF + z * fh + c * 768
    qkv_base = (1 - y) * (z * D + c * 512) + y * (NQ + c * D + z * 512)
    moves = []
    for kind, chunk in ((0, 0), (1, 0), (0, 1), (1, 1), (0, 2)):
        if kind == 0:
            gu_far[chunk].wait_recv()
            moves.append(final(Y, 4 + chunk, rgu, zgu, ogu, chunk, gu_base))
        else:
            qkv_far[chunk].wait_recv()
            moves.append(final(X, 7 + chunk, rqkv, zqkv, oqkv, chunk, qkv_base))
    wd_far.wait_recv()
    owd[...] = rwd[x] + zwd[...]
    wo_far.wait_recv()
    owo[...] = rwo[y] + zwo[...]
    all_wait(gainbuf, one_recv.at[gain_number])
    gainbuf[me] = gpart[...]
    gainbuf[0] = loop(16, lambda i, total: total + gainbuf[i], jnp.zeros((24, 128), F32)) * inv_tokens
    for i in range(2):
        row = gainbuf[0, pl.ds(8 * i + lax.div(me, 2), 1), :]
        ogain[i : i + 1, :] = jnp.where(c == 0, row, pltpu.roll(row, 64, axis=1))
    ogain[2:4, :] = gainbuf[0, 16:18, :]
    ogain[4:8, :] = jnp.zeros((4, 128), F32)
    for move in moves:
        move.arrived()
    for item in moves + [e_gu, e_qkv, e_a, e_c] + parts:
        item.drain()
    for copy in sent:
        copy.wait_send()
    all_wait(gainbuf, one_send.at[gain_number])
    all_wait(gbuf, one_send.at[norm_number])


def shape(rows, width, dtype):
    return jax.ShapeDtypeStruct((rows, width), dtype)


def many(count, *args):
    return [VM(*args)] * count


def layer_call(*operands):
    vmem = pl.BlockSpec(memory_space=VM)
    hbm = pl.BlockSpec(memory_space=pl.ANY)
    dma = pltpu.SemaphoreType.DMA
    t2, kvh, fh = 2 * T, D // 2, FF // 2
    cube, square, line = (2, 2, 2, 2), (2, 2, 2), (2, 2)
    spreads = 18
    return pl.pallas_call(
        layer_kernel,
        name="layer",
        out_shape=(
            shape(T, D, BF16), shape(T, D, BF16), shape(64, NQ + 2 * D, F32), shape(64, 2 * FF, F32),
            shape(128, D, F32), shape(192, D, F32), shape(8, 128, F32),
        ),
        in_specs=[vmem] * 6 + [hbm] * 9,
        out_specs=(vmem, vmem, hbm, hbm, vmem, vmem, vmem),
        scratch_shapes=[
            VM((8, 128), F32), VM((16, 8, 128), F32), VM(cube + (64, D), BF16), *many(2, cube + (64, kvh), BF16),
            VM(square + (128, D), BF16), *many(2, cube + (64, fh), BF16), VM(square + (192, D), BF16),
            *many(2, (1, D), F32),
            VM((t2, D), BF16), VM((2, T, t2), F32), VM((t2, D), BF16), VM((t2, D), BF16), *many(2, (t2, kvh), BF16),
            VM((8, t2, HD), BF16), VM((t2, kvh), BF16), VM((8, t2, T), F32), VM((t2, D), BF16), VM((T, D), F32),
            VM((t2, D), BF16), VM((8, 128), BF16), VM((t2, fh), BF16), VM((t2, fh), F32), VM((t2, D), BF16),
            VM((T, D), F32), *many(4, (2, T, D), F32), *many(4, (T, D), F32),
            VM(square + (192, t2), BF16), VM(square + (128, t2), BF16), VM((t2, NQ), BF16), VM((t2, FF), BF16),
            VM((24, 128), F32), *many(2, line + (D, t2), BF16), *many(2, line + (2, T, D), BF16),
            VM((4, t2, 768), BF16), VM((4, t2, 512), BF16), VM((4, 2, 192, t2), BF16), VM((4, 2, 128, t2), BF16),
            VM((3,) + cube + (64, 256), F32), VM((2,) + cube + (64, 256), F32), VM((2, 192, D), F32),
            VM((2, 128, D), F32), VM((3,) + square + (64, 256), F32), VM((2,) + square + (64, 256), F32),
            VM((192, D), F32), VM((128, D), F32), VM((16, 24, 128), F32),
            *[dma((spreads, 3))] * 2, *[dma((spreads, 4))] * 2, dma((spreads + 2,)), *[dma((11,))] * 3, *[dma((20,))] * 2,
        ],
        compiler_params=pltpu.CompilerParams(collective_id=0, has_side_effects=True, vmem_limit_bytes=HIGH_VMEM),
    )(*operands)


def deliver_kernel(y_in, dh_in, qkv_in, gu_in, wo_in, wd_in, gain_in, *refs):
    outs, gains_out, scratch, (in_sem, out_sem) = refs[:9], refs[9:13], refs[13:22], refs[22:]
    spans = ((qkv_in, 0, NQ), (qkv_in, NQ, D), (qkv_in, NQ + D, D), (gu_in, 0, FF), (gu_in, FF, FF))
    q_in, k_in, v_in, g_in, u_in = (ref.at[:, pl.ds(start, size)] for ref, start, size in spans)
    sources = (y_in, dh_in, q_in, k_in, v_in, wo_in, g_in, u_in, wd_in)
    loads = [pltpu.make_async_copy(src, buf, in_sem.at[i]) for i, (src, buf) in enumerate(zip(sources, scratch))]
    stores = [pltpu.make_async_copy(buf, out, out_sem.at[i]) for i, (buf, out) in enumerate(zip(scratch, outs))]
    for load in loads:
        load.start()
    for i, out in enumerate(gains_out):
        out[...] = gain_in[i : i + 1, : out.shape[0]].reshape(out.shape)
    for load, store in zip(loads, stores):
        load.wait()
        store.start()
    for store in stores:
        store.wait()


def deliver(*results):
    vmem = pl.BlockSpec(memory_space=VM)
    hbm = pl.BlockSpec(memory_space=pl.ANY)
    dma = pltpu.SemaphoreType.DMA
    sizes = [(T, D, BF16)] * 2 + [(64, width, F32) for width in (NQ, D, D)] + [(128, D, F32)]
    sizes += [(64, FF, F32)] * 2 + [(192, D, F32)]
    small = [jax.ShapeDtypeStruct((size,), F32) for size in (64, 64, 128, 128)]
    return pl.pallas_call(
        deliver_kernel,
        name="deliver",
        out_shape=tuple([shape(*size) for size in sizes] + small),
        in_specs=[hbm] * 6 + [vmem],
        out_specs=tuple([hbm] * 9 + [vmem] * 4),
        scratch_shapes=[VM(size[:2], size[2]) for size in sizes] + [dma((9,)), dma((9,))],
    )(*results)


def rope_tables(positions):
    inv_freq = ROPE_THETA ** (-2.0 * jnp.arange(HD // 2, dtype=F32) / HD)
    angle = positions.reshape(-1, 1).astype(F32) * inv_freq
    cos_half, sin_half = jnp.cos(angle), jnp.sin(angle)
    return cos_half, sin_half


def solution(mesh):
    axis_name = mesh.axis_names[0]
    sharded = P(axis_name)
    in_specs = (sharded,) * 5 + (P(), P()) + (sharded,) * 7
    out_specs = (sharded,) * 4 + (P(), P()) + (sharded,) * 7

    def device_step(hidden, grad_out, positions, norm1, norm2, gain_q, gain_k, w_q, w_k, w_v, w_o, w_gate, w_up, w_down):
        cos, sin = rope_tables(positions)
        x, dy = hidden.reshape(T, D), grad_out.reshape(T, D)
        results = layer_call(cos, sin, norm1, norm2, gain_q, gain_k, x, dy, w_q, w_k, w_v, w_o, w_gate, w_up, w_down)
        out, d_hidden, d_wq, d_wk, d_wv, d_wo, d_wg, d_wu, d_wd, d_n1, d_n2, d_qn, d_kn = deliver(*results)
        out, d_hidden = out.reshape(hidden.shape), d_hidden.reshape(hidden.shape)
        return out, d_hidden, d_n1, d_n2, d_qn, d_kn, d_wq, d_wk, d_wv, d_wo, d_wg, d_wu, d_wd

    return jax.shard_map(device_step, mesh=mesh, in_specs=in_specs, out_specs=out_specs, check_vma=False)
```

```python
import jax
import jax.numpy as jnp
from jax import lax
from jax.experimental import pallas as pl
from jax.experimental.pallas import tpu as pltpu
from jax.sharding import PartitionSpec as P

RMS_EPS = 1e-6
ROPE_THETA = 1000000.0
MESH = pl.DeviceIdType.MESH
F32 = jnp.float32
BF16 = jnp.bfloat16
T = 128
D = 1024
NQ = 2048
FF = 3072
HD = 128
Z, Y, X, C = 0, 1, 2, 3
STRIDE = (8, 4, 2, 1)
ALL = slice(None)
VM = pltpu.VMEM
HIGH_VMEM = 67043328


def nn(left_op, right_op):
    return jnp.dot(left_op, right_op, preferred_element_type=F32)


def nt(left_op, right_op):
    return lax.dot_general(left_op, right_op, (((1,), (1,)), ((), ())), preferred_element_type=F32)


def tn(left_op, right_op):
    return lax.dot_general(left_op, right_op, (((0,), (0,)), ((), ())), preferred_element_type=F32)


def rms(val):
    return lax.rsqrt(jnp.mean(val * val, axis=-1, keepdims=True) + RMS_EPS)


def norm_backward(d_unit, unit_val, scale_val):
    return scale_val * (d_unit - unit_val * jnp.mean(d_unit * unit_val, axis=-1, keepdims=True))


class Place:
    def __init__(self):
        self.me = lax.axis_index("fsdp")
        self.bit = [lax.rem(lax.div(self.me, s), 2) for s in STRIDE]

    def near(self, dim):
        return (self.me + STRIDE[dim] * (1 - 2 * self.bit[dim]),)

    def greet(self, dims):
        barrier = pltpu.get_barrier_semaphore()
        for dim in dims:
            pl.semaphore_signal(barrier, inc=1, device_id=self.near(dim), device_id_type=MESH)
        pl.semaphore_wait(barrier, len(dims))


class Spread:
    def __init__(self, place, own, first, buf, sub, order, axes, sems, part):
        self.place, self.buf, self.sub, self.order, self.axes = place, buf, sub, order, axes
        self.link_send, self.link_recv, self.core_send, self.core_recv, self.local_sem = sems
        self.part, self.last = part, len(order)
        self.source = own
        self.mine = self.block(()) if own is None else own
        self.first = self.mine if first is None else first

    def block(self, full, flip=None):
        index = []
        for dim in self.axes:
            if dim in full:
                index.append(ALL)
            elif dim == flip:
                index.append(1 - self.place.bit[dim])
            else:
                index.append(self.place.bit[dim])
        return self.buf.at[tuple(index) + self.sub]

    def copy_own(self):
        return pltpu.make_async_copy(self.source, self.block(()), self.local_sem.at[self.part])

    def link(self, step):
        dst = self.block(self.order[:step])
        return pltpu.make_async_remote_copy(
            src_ref=self.first if step == 0 else dst,
            dst_ref=dst,
            send_sem=self.link_send.at[self.part, step],
            recv_sem=self.link_recv.at[self.part, step],
            device_id=self.place.near(self.order[step]),
            device_id_type=MESH,
        )

    def core(self, step):
        dst = self.block(()) if step == 0 else self.block(self.order[: step - 1], self.order[step - 1])
        return pltpu.make_async_remote_copy(
            src_ref=self.mine if step == 0 else dst,
            dst_ref=dst,
            send_sem=self.core_send.at[self.part, step],
            recv_sem=self.core_recv.at[self.part, step],
            device_id=self.place.near(C),
            device_id_type=MESH,
        )

    def begin(self):
        self.link(0).start()
        if self.source is not None:
            self.copy_own().start()
        self.core(0).start()

    def advance(self, step):
        if step == 0 and self.source is not None:
            self.copy_own().wait()
        self.link(step).wait_recv()
        if step + 1 < self.last:
            self.link(step + 1).start()
        self.core(step + 1).start()

    def arrived(self):
        for step in range(self.last + 1):
            self.core(step).wait_recv()

    def drain(self):
        for step in range(self.last):
            self.link(step).wait_send()
        for step in range(self.last + 1):
            self.core(step).wait_send()


class Group:
    def __init__(self, place, axes):
        self.place, self.axes = place, axes
        self.position = self.spot(place.bit)

    def others(self):
        for number in range(2 ** len(self.axes) - 1, 0, -1):
            bit = list(self.place.bit)
            for i, dim in enumerate(self.axes):
                if number >> i & 1:
                    bit[dim] = 1 - bit[dim]
            yield bit

    def spot(self, bit):
        total = 0
        for dim in self.axes:
            total = total * 2 + bit[dim]
        return total


def device_of(bit):
    return (sum(stride * value for stride, value in zip(STRIDE, bit)),)


class Exchange:
    def __init__(self, group, number, piece, slot, blocks, sems):
        self.group, self.piece, self.slot, self.blocks = group, piece, slot, blocks
        self.send, self.recv, self.local = (sem.at[number] for sem in sems)

    def own(self):
        return pltpu.make_async_copy(self.piece(self.group.place.bit), self.slot, self.local)

    def begin(self):
        for bit in self.group.others():
            pltpu.make_async_remote_copy(
                src_ref=self.piece(bit),
                dst_ref=self.slot,
                send_sem=self.send,
                recv_sem=self.recv,
                device_id=device_of(bit),
                device_id_type=MESH,
            ).start()
        self.own().start()

    def arrived(self):
        self.own().wait()
        pltpu.make_async_copy(self.blocks, self.blocks, self.recv).wait()

    def drain(self):
        pltpu.make_async_copy(self.blocks, self.blocks, self.send).wait()


def head_forward(proj, gain, cos, sin):
    val = proj.astype(F32)
    scaled = val * rms(val) * gain
    return (scaled * cos + pltpu.roll(scaled, 64, axis=1) * sin).astype(BF16)


def head_backward(d_rot, proj, gain, cos, sin):
    val = proj.astype(F32)
    scale = rms(val)
    unit = val * scale
    d_scaled = d_rot * cos - pltpu.roll(d_rot, 64, axis=1) * sin
    d_gain = jnp.sum(d_scaled * unit, axis=0, keepdims=True)
    return norm_backward(d_scaled * gain, unit, scale).astype(BF16), d_gain


def cols(i, width):
    return pl.ds(pl.multiple_of(i * width, width), width)


def loop(count, body, init=0):
    return lax.fori_loop(0, count, body, init)


def each(count):
    def run(body):
        def step(i, _):
            body(i)
            return 0

        loop(count, step)

    return run


def two(i):
    return lax.div(i, 2), lax.rem(i, 2)


def three(i):
    return two(lax.div(i, 2)) + (lax.rem(i, 2),)


def layer_kernel(
    pos_ref, freq_ref, n1_ref, n2_ref, qn_ref, kn_ref, x_ref, dy_ref, wq, wk, wv, wo, wg, wu, wd,
    y_ref, dh_ref, oqkv, ogu, owo, owd, ogain,
    gains, gbuf, bq, bk, bv, bo, bg, bu, bd, g1, g2,
    xp, trig, n_s, q_s, k_s, v_s, qr, kr, probs, ctx, h_s, m_s, spare, act, dact, dctx, dres,
    part_a, part_y, part_m, part_n, land_a, land_y, land_m, land_n,
    at_ref, ct_ref, dqkv, dgu, gpart,
    nbuf, mbuf, dybuf, drbuf, gubuf, qkvbuf, abuf, cbuf,
    rgu, rqkv, rwd, rwo, zgu, zqkv, zwd, zwo, gainbuf,
    link_send, link_recv, core_send, core_recv, local_sem, one_send, one_recv, one_local, far_send, far_recv,
):
    place = Place()
    me = place.me
    z, y, x, c = place.bit
    sems = (link_send, link_recv, core_send, core_recv, local_sem)
    one = (one_send, one_recv, one_local)
    parts = []

    def spread(own, first, buf, sub, order, axes):
        parts.append(Spread(place, own, first, buf, sub, order, axes, sems, len(parts)))
        return parts[-1]

    both = (ALL, ALL)
    turns = ((Y, X), (X, Y))

    def by_columns(src, buf):
        half = src.shape[1] // 2
        size = half // 2
        made = []
        for i in range(2):
            mine, theirs = (src.at[:, pl.ds(pl.multiple_of(side * half + i * size, size), size)] for side in (z, 1 - z))
            made.append(spread(mine, theirs, buf, (ALL, pl.ds(i * size, size)), (Z,) + turns[i], (Z, Y, X, C)))
        return made

    def by_rows(src, buf):
        size = src.shape[0] // 2
        made = []
        for i in range(2):
            rows = pl.ds(i * size, size)
            made.append(spread(src.at[rows], None, buf, (rows, ALL), turns[i], (Y, X, C)))
        return made

    p_qkv = by_columns(wq, bq) + by_columns(wk, bk) + by_columns(wv, bv)
    p_o, p_d = by_rows(wo, bo), by_rows(wd, bd)
    p_g, p_u = by_columns(wg, bg), by_columns(wu, bu)
    p_m = spread(None, None, mbuf, both, (X,), (X, C))
    p_n = spread(None, None, nbuf, both, (Y,), (Y, C))
    p_dy = spread(None, None, dybuf, (ALL, ALL, ALL), (Y,), (Y, C))
    p_dr = spread(None, None, drbuf, (ALL, ALL, ALL), (X,), (X, C))

    grp_x, grp_y = Group(place, (X, C)), Group(place, (Y, C))

    def share(number, group, piece, buf):
        return Exchange(group, number, piece, buf.at[group.position], buf.at[pl.ds(0, 3)], one)

    def cols_for(group, ref, width):
        return lambda bit: ref.at[:, pl.ds(pl.multiple_of(group.spot(bit) * width, 128), width)]

    e_gu = share(0, grp_x, cols_for(grp_x, dgu, 768), gubuf)
    e_qkv = share(1, grp_y, cols_for(grp_y, dqkv, 512), qkvbuf)
    e_a = share(2, grp_y, lambda bit: at_ref.at[bit[Y], :, bit[C]], abuf)
    e_c = share(3, grp_x, lambda bit: ct_ref.at[:, bit[X], bit[C]], cbuf)
    gain_number, norm_number = 9, 10
    sent = []

    def near_copy(dim, source, target):
        number = len(sent)
        sent.append(
            pltpu.make_async_remote_copy(
                src_ref=source, dst_ref=target, send_sem=far_send.at[number], recv_sem=far_recv.at[number],
                device_id=place.near(dim), device_id_type=MESH,
            )
        )
        return sent[-1]

    mine = cols(z, T)

    def pair_rows(i):
        return cols(4 * z + i, 32)

    barrier = pltpu.get_barrier_semaphore()

    def other(k):
        return (lax.rem(me + k, 16),)

    @each(15)
    def _(k):
        pl.semaphore_signal(barrier, inc=1, device_id=other(k + 1), device_id_type=MESH)

    gains[...] = jnp.zeros((8, 128), F32)
    halves = [ref[...].astype(F32).reshape(1, 64) for ref in (n1_ref, n2_ref)]
    gains[0:1, :] = jnp.concatenate(halves, axis=1)
    gains[1:2, :] = qn_ref[...].astype(F32).reshape(1, 128)
    gains[2:3, :] = kn_ref[...].astype(F32).reshape(1, 128)
    angle = jnp.broadcast_to(pos_ref[...].astype(F32), (T, T)).T[:, : HD // 2] * freq_ref[...]
    cos_half, sin_half = jnp.cos(angle), jnp.sin(angle)
    trig[z] = jnp.concatenate([cos_half, cos_half, -sin_half, sin_half], axis=1)
    pl.semaphore_wait(barrier, 15)

    def to_all(source, buf, number):
        @each(15)
        def _(k):
            pltpu.make_async_remote_copy(
                src_ref=source, dst_ref=buf.at[me], send_sem=one_send.at[number], recv_sem=one_recv.at[number],
                device_id=other(k + 1), device_id_type=MESH,
            ).start()

    def all_wait(buf, sem):
        fifteen = buf.at[pl.ds(0, 15)]
        pltpu.make_async_copy(fifteen, fifteen, sem).wait()

    to_all(gains, gbuf, norm_number)
    for item in p_qkv + p_o:
        item.begin()
    x_copy = near_copy(Z, x_ref, xp.at[mine])
    trig_copy = near_copy(Z, trig.at[z], trig.at[z])
    x_copy.start()
    own_x = pltpu.make_async_copy(x_ref, xp.at[mine], local_sem.at[len(parts)])
    own_x.start()
    for item in p_d + p_g + p_u:
        item.begin()
    trig_copy.start()
    dy_copy = near_copy(Z, dy_ref, dybuf.at[y, c, z])
    dy_copy.start()
    own_dy = pltpu.make_async_copy(dy_ref, dybuf.at[y, c, z], local_sem.at[len(parts) + 1])
    own_dy.start()
    for item in p_qkv + p_o:
        item.advance(0)
    gq, gk = gains[1:2, :], gains[2:3, :]
    all_wait(gbuf, one_recv.at[norm_number])
    gbuf[me] = gains[...]
    lane = lax.broadcasted_iota(jnp.int32, (8, 128), 1) < 64
    for i in range(8):
        first, second = gbuf[2 * i], gbuf[2 * i + 1]
        tile = slice(128 * i, 128 * i + 128)
        g1[:, tile] = jnp.where(lane, first, pltpu.roll(second, 64, axis=1))[:1]
        g2[:, tile] = jnp.where(lane, pltpu.roll(first, 64, axis=1), second)[:1]
    own_x.wait()
    x_copy.wait_recv()

    @each(8)
    def _(i):
        rows = cols(i, 32)
        val = xp[rows].astype(F32)
        n_s[rows] = (val * rms(val) * g1[...]).astype(BF16)

    def turned(val):
        return val.astype(F32).T.astype(BF16)

    for item in p_qkv:
        item.advance(1)
    for item in p_d:
        item.advance(0)

    @each(4)
    def _(i):
        nbuf[y, c, cols(i, 256)] = turned(n_s[:, cols(i, 256)])

    for item in p_o:
        item.advance(1)
    for item in p_g + p_u:
        item.advance(0)
    for item in p_qkv:
        item.advance(2)
    trig_copy.wait_recv()

    def weight(buf, tile):
        block = buf[(ALL,) * (len(buf.shape) - 1) + (tile,)]
        return block.reshape(-1, block.shape[-1])

    def project(buf, dst, width, tiles):
        @each(tiles)
        def _(j):
            tile = cols(j, width)
            dst[:, tile] = nn(n_s[...], weight(buf, tile)).astype(BF16)

    for item in p_qkv:
        item.arrived()
    project(bq, q_s, 512, 2)
    project(bk, k_s, 512, 1)
    project(bv, v_s, 512, 1)
    scale = HD ** -0.5

    def sequence_head(j):
        seq, head = lax.div(j, 4), lax.rem(j, 4)
        return seq, head, cols(seq, T), cols(head, HD), cols(head, 2 * HD)

    @each(8)
    def _(j):
        seq, _, rows, kv, pair = sequence_head(j)
        cos, sin = trig[seq, :, :HD], trig[seq, :, HD:]
        k_rot = head_forward(k_s[rows, kv], gk, cos, sin)
        kr[rows, kv] = k_rot
        q_pair = q_s[rows, pair]
        q_rot = jnp.concatenate(
            [head_forward(half, gq, cos, sin) for half in (q_pair[:, :HD], q_pair[:, HD:])], axis=0
        )
        qr[j] = q_rot
        scores = nt(q_rot, k_rot) * scale
        row = lax.rem(lax.broadcasted_iota(jnp.int32, (2 * T, T), 0), T)
        col = lax.broadcasted_iota(jnp.int32, (2 * T, T), 1)
        scores = jnp.where(row >= col, scores, -1e30)
        expd = jnp.exp(scores - jnp.max(scores, axis=-1, keepdims=True))
        prob = expd / jnp.sum(expd, axis=-1, keepdims=True)
        probs[j] = prob
        out = nn(prob.astype(BF16), v_s[rows, kv])
        ctx[rows, pair] = jnp.concatenate([out[:T], out[T:]], axis=1).astype(BF16)

    def pair_sum(partial, landing, compute):
        copies = []
        for half in range(2):
            @each(2)
            def _(j):
                i = j + 2 * half
                partial[:, :, cols(i, 256)] = compute(i).reshape(2, T, 256)

            span = (ALL, pl.ds(512 * half, 512))
            copies.append(near_copy(Z, partial.at[(1 - z,) + span], landing.at[span]))
            copies[-1].start()
        return copies

    def received(copies):
        for copy in copies:
            copy.wait_recv()

    for item in p_o:
        item.arrived()
    a_copies = pair_sum(part_a, land_a, lambda i: nn(ctx[...], weight(bo, cols(i, 256))))
    for item in p_g + p_u:
        item.advance(1)
    for item in p_d:
        item.advance(1)

    @each(4)
    def _(i):
        ct_ref[two(i)] = turned(ctx[:, cols(i, 256)]).reshape(2, 128, 2 * T)

    received(a_copies)

    @each(4)
    def _(i):
        rows = cols(i, 32)
        attn = (part_a[z, rows] + land_a[rows]).astype(BF16)
        val = (xp[pair_rows(i)].astype(F32) + attn.astype(F32)).astype(BF16).astype(F32)
        h_s[rows] = val
        m_s[pair_rows(i)] = (val * rms(val) * g2[...]).astype(BF16)

    m_copy = near_copy(Z, m_s.at[mine], m_s.at[mine])
    m_copy.start()
    for item in p_d:
        item.arrived()
    own_dy.wait()
    dy_copy.wait_recv()

    @each(4)
    def _(i):
        dact[:, cols(i, 384)] = nt(dybuf[y, c].reshape(2 * T, D), bd[two(i)].reshape(384, D))

    m_copy.wait_recv()

    @each(4)
    def _(i):
        mbuf[x, c, cols(i, 256)] = turned(m_s[:, cols(i, 256)])

    for item in p_g + p_u:
        item.advance(2)
    p_m.begin()
    p_dy.begin()
    e_c.begin()
    for item in p_g + p_u:
        item.arrived()
    fh = FF // 2

    @each(fh // 256)
    def _(j):
        tile = cols(j, 256)
        gate_val = nn(m_s[...], weight(bg, tile)).astype(BF16).astype(F32)
        up_val = nn(m_s[...], weight(bu, tile)).astype(BF16).astype(F32)
        sig = jax.nn.sigmoid(gate_val)
        act[:, tile] = (gate_val * sig * up_val).astype(BF16)
        d_act = dact[:, tile]
        dgu[:, tile] = (d_act * up_val * sig * (1.0 + gate_val * (1.0 - sig))).astype(BF16)
        dgu[:, cols(j + fh // 256, 256)] = (d_act * gate_val * sig).astype(BF16)

    def d_mlp_in(i):
        rows = two(i)
        return nt(dgu[:, :fh], bg[rows].reshape(256, fh)) + nt(dgu[:, fh:], bu[rows].reshape(256, fh))

    e_gu.begin()
    m_copies = pair_sum(part_m, land_m, d_mlp_in)

    @each(4)
    def _(i):
        at_ref[two(i)] = turned(act[:, cols(i, 384)]).reshape(2, 192, 2 * T)

    e_a.begin()
    p_n.begin()
    received(m_copies)

    def d_res_rows(i, total):
        rows = cols(i, 32)
        val = h_s[rows]
        r_scale = rms(val)
        unit = val * r_scale
        grad = part_m[z, rows] + land_m[rows]
        out = dybuf[y, c, z, rows].astype(F32) + norm_backward(grad * g2[...], unit, r_scale)
        dres[rows] = out
        drbuf[x, c, z, rows] = out.astype(BF16)
        return total + jnp.sum(grad * unit, axis=0, keepdims=True)

    d_g2 = loop(4, d_res_rows, jnp.zeros((1, D), F32))
    r_copy = near_copy(Z, drbuf.at[x, c, z], drbuf.at[x, c, z])
    r_copy.start()
    y_copies = pair_sum(part_y, land_y, lambda i: nn(act[...], weight(bd, cols(i, 256))))
    inv_tokens = 1.0 / (16 * T)

    def row_tiles(left_buf, right_buf, out):
        @each(8)
        def _(j):
            tile = cols(lax.rem(j, 4), 256)
            half = lax.div(j, 4)
            left = jnp.concatenate([left_buf[i, half] for i in range(4)], axis=1)
            out[half, :, tile] = nn(left, weight(right_buf, tile)) * inv_tokens

    p_dy.advance(0)
    p_dy.arrived()
    e_a.arrived()
    row_tiles(abuf, dybuf, rwd)
    r_copy.wait_recv()
    p_dr.begin()
    wd_far = near_copy(X, rwd.at[1 - x], zwd)
    wd_far.start()

    @each(2)
    def _(i):
        dctx[:, cols(i, 512)] = nt(drbuf[x, c].reshape(2 * T, D), bo[i].reshape(512, D)).astype(BF16)

    def attend_back(j, carry):
        q_total, k_total = carry
        seq, head, rows, kv, pair = sequence_head(j)
        cos, sin = trig[seq, :, :HD], trig[seq, :, HD:]
        d_out = dctx[rows, pair]
        d_out = jnp.concatenate([d_out[:, :HD], d_out[:, HD:]], axis=0)
        prob = probs[j]
        d_value = tn(prob.astype(BF16), d_out).astype(BF16)
        d_prob = nt(d_out, v_s[rows, kv])
        d_score = prob * (d_prob - jnp.sum(prob * d_prob, axis=-1, keepdims=True))
        d_score = (d_score * scale).astype(BF16)
        d_q_rot = nn(d_score, kr[rows, kv])
        d_k_rot = tn(d_score, qr[j])
        q_pair = q_s[rows, pair]
        d_q0, g_q0 = head_backward(d_q_rot[:T], q_pair[:, :HD], gq, cos, sin)
        d_q1, g_q1 = head_backward(d_q_rot[T:], q_pair[:, HD:], gq, cos, sin)
        d_k, g_k = head_backward(d_k_rot, k_s[rows, kv], gk, cos, sin)
        dqkv[rows, pair] = jnp.concatenate([d_q0, d_q1], axis=1)
        dqkv[rows, cols(head + 8, HD)] = d_k
        dqkv[rows, cols(head + 12, HD)] = d_value
        return q_total + g_q0 + g_q1, k_total + g_k

    zero = jnp.zeros((1, HD), F32)
    q_total, k_total = loop(8, attend_back, (zero, zero))
    e_qkv.begin()

    def d_normed(i):
        rows = two(i)
        grad = nt(dqkv[:, :D], bq[rows].reshape(256, D)) + nt(dqkv[:, D : D + 512], bk[rows].reshape(256, 512))
        return grad + nt(dqkv[:, D + 512 :], bv[rows].reshape(256, 512))

    n_copies = pair_sum(part_n, land_n, d_normed)

    def column_chunk(acts, grads, out, chunk):
        @each(8)
        def _(i):
            rows = cols(i, 128)
            left = jnp.concatenate([acts[k // 2, k % 2, rows] for k in range(4)], axis=1)
            right = grads[:, :, 256 * chunk : 256 * chunk + 256].reshape(8 * T, 256)
            out[(chunk,) + three(i)] = (nn(left, right) * inv_tokens).reshape(2, 64, 256)

    def half_of(dim, result, chunk):
        bit = place.bit[dim]
        return result.at[(chunk,) + tuple(1 - bit if k == dim else ALL for k in range(4))]

    p_m.advance(0)
    p_m.arrived()
    e_gu.arrived()
    gu_far = []
    for chunk in range(3):
        column_chunk(mbuf, gubuf, rgu, chunk)
        gu_far.append(near_copy(Y, half_of(Y, rgu, chunk), zgu.at[chunk]))
        gu_far[-1].start()
    p_n.advance(0)
    p_n.arrived()
    e_qkv.arrived()
    qkv_far = []
    for chunk in range(2):
        column_chunk(nbuf, qkvbuf, rqkv, chunk)
        qkv_far.append(near_copy(X, half_of(X, rqkv, chunk), zqkv.at[chunk]))
        qkv_far[-1].start()
    p_dr.advance(0)
    p_dr.arrived()
    e_c.arrived()
    row_tiles(cbuf, drbuf, rwo)
    wo_far = near_copy(Y, rwo.at[1 - y], zwo)
    wo_far.start()

    received(n_copies)

    def d_hidden_rows(i, total):
        rows = cols(i, 32)
        val = xp[pair_rows(i)].astype(F32)
        x_scale = rms(val)
        unit = val * x_scale
        grad = part_n[z, rows] + land_n[rows]
        dh_ref[rows] = (dres[rows] + norm_backward(grad * g1[...], unit, x_scale)).astype(BF16)
        return total + jnp.sum(grad * unit, axis=0, keepdims=True)

    d_g1 = loop(4, d_hidden_rows, jnp.zeros((1, D), F32))
    for i in range(8):
        tile = slice(128 * i, 128 * i + 128)
        gpart[i : i + 1, :] = d_g1[:, tile]
        gpart[8 + i : 9 + i, :] = d_g2[:, tile]
    gpart[16:17, :] = q_total
    gpart[17:18, :] = k_total
    gpart[18:24, :] = jnp.zeros((6, 128), F32)

    to_all(gpart, gainbuf, gain_number)
    received(y_copies)

    @each(4)
    def _(i):
        rows = cols(i, 32)
        out = (part_y[z, rows] + land_y[rows]).astype(BF16).astype(F32)
        y_ref[rows] = (h_s[rows] + out).astype(BF16)

    def final(dim, number, result, target, out, chunk, base):
        group = Group(place, tuple(k for k in range(4) if k != dim))
        for bit in list(group.others()) + [place.bit]:
            index = (chunk,) + tuple(bit)
            result[index] = result[index] + target[(chunk,) + tuple(bit[k] for k in group.axes)]
        where = pl.ds(pl.multiple_of(base + 256 * chunk, 128), 256)
        move = Exchange(
            group, number, lambda bit: result.at[(chunk,) + tuple(bit)], out.at[:, where],
            out.at[:, pl.ds(0, 7 * 256)], one,
        )
        move.begin()
        return move

    gu_base = x * FF + z * fh + c * 768
    qkv_base = (1 - y) * (z * D + c * 512) + y * (NQ + c * D + z * 512)
    moves = []
    for kind, chunk in ((0, 0), (1, 0), (0, 1), (1, 1), (0, 2)):
        if kind == 0:
            gu_far[chunk].wait_recv()
            moves.append(final(Y, 4 + chunk, rgu, zgu, ogu, chunk, gu_base))
        else:
            qkv_far[chunk].wait_recv()
            moves.append(final(X, 7 + chunk, rqkv, zqkv, oqkv, chunk, qkv_base))
    wd_far.wait_recv()
    owd[...] = rwd[x] + zwd[...]
    wo_far.wait_recv()
    owo[...] = rwo[y] + zwo[...]
    all_wait(gainbuf, one_recv.at[gain_number])
    gainbuf[me] = gpart[...]
    gainbuf[0] = loop(16, lambda i, total: total + gainbuf[i], jnp.zeros((24, 128), F32)) * inv_tokens
    for i in range(2):
        row = gainbuf[0, pl.ds(8 * i + lax.div(me, 2), 1), :]
        ogain[i : i + 1, :] = jnp.where(c == 0, row, pltpu.roll(row, 64, axis=1))
    ogain[2:4, :] = gainbuf[0, 16:18, :]
    ogain[4:8, :] = jnp.zeros((4, 128), F32)
    for move in moves:
        move.arrived()
    for item in moves + [e_gu, e_qkv, e_a, e_c] + parts:
        item.drain()
    for copy in sent:
        copy.wait_send()
    all_wait(gainbuf, one_send.at[gain_number])
    all_wait(gbuf, one_send.at[norm_number])


def shape(rows, width, dtype):
    return jax.ShapeDtypeStruct((rows, width), dtype)


def many(count, *args):
    return [VM(*args)] * count


def layer_call(*operands):
    vmem = pl.BlockSpec(memory_space=VM)
    hbm = pl.BlockSpec(memory_space=pl.ANY)
    dma = pltpu.SemaphoreType.DMA
    t2, kvh, fh = 2 * T, D // 2, FF // 2
    cube, square, line = (2, 2, 2, 2), (2, 2, 2), (2, 2)
    spreads = 18
    return pl.pallas_call(
        layer_kernel,
        name="layer",
        out_shape=(
            shape(T, D, BF16), shape(T, D, BF16), shape(64, NQ + 2 * D, F32), shape(64, 2 * FF, F32),
            shape(128, D, F32), shape(192, D, F32), shape(8, 128, F32),
        ),
        in_specs=[vmem] * 6 + [hbm] * 9,
        out_specs=(vmem, vmem, hbm, hbm, vmem, vmem, vmem),
        scratch_shapes=[
            VM((8, 128), F32), VM((16, 8, 128), F32), VM(cube + (64, D), BF16), *many(2, cube + (64, kvh), BF16),
            VM(square + (128, D), BF16), *many(2, cube + (64, fh), BF16), VM(square + (192, D), BF16),
            *many(2, (1, D), F32),
            VM((t2, D), BF16), VM((2, T, t2), F32), VM((t2, D), BF16), VM((t2, D), BF16), *many(2, (t2, kvh), BF16),
            VM((8, t2, HD), BF16), VM((t2, kvh), BF16), VM((8, t2, T), F32), VM((t2, D), BF16), VM((T, D), F32),
            VM((t2, D), BF16), VM((8, 128), BF16), VM((t2, fh), BF16), VM((t2, fh), F32), VM((t2, D), BF16),
            VM((T, D), F32), *many(4, (2, T, D), F32), *many(4, (T, D), F32),
            VM(square + (192, t2), BF16), VM(square + (128, t2), BF16), VM((t2, NQ), BF16), VM((t2, FF), BF16),
            VM((24, 128), F32), *many(2, line + (D, t2), BF16), *many(2, line + (2, T, D), BF16),
            VM((4, t2, 768), BF16), VM((4, t2, 512), BF16), VM((4, 2, 192, t2), BF16), VM((4, 2, 128, t2), BF16),
            VM((3,) + cube + (64, 256), F32), VM((2,) + cube + (64, 256), F32), VM((2, 192, D), F32),
            VM((2, 128, D), F32), VM((3,) + square + (64, 256), F32), VM((2,) + square + (64, 256), F32),
            VM((192, D), F32), VM((128, D), F32), VM((16, 24, 128), F32),
            *[dma((spreads, 3))] * 2, *[dma((spreads, 4))] * 2, dma((spreads + 2,)), *[dma((11,))] * 3, *[dma((20,))] * 2,
        ],
        compiler_params=pltpu.CompilerParams(collective_id=0, has_side_effects=True, vmem_limit_bytes=HIGH_VMEM),
    )(*operands)


def deliver_kernel(y_in, dh_in, qkv_in, gu_in, wo_in, wd_in, gain_in, *refs):
    rest = iter(refs)
    outs, small_outs, scratch, small = ([next(rest) for _ in range(count)] for count in (9, 4, 9, 4))
    gain, in_sem, out_sem = rest
    spans = ((qkv_in, 0, NQ), (qkv_in, NQ, D), (qkv_in, NQ + D, D), (gu_in, 0, FF), (gu_in, FF, FF))
    q_in, k_in, v_in, g_in, u_in = (ref.at[:, pl.ds(start, size)] for ref, start, size in spans)
    sources = (gain_in, y_in, dh_in, q_in, k_in, v_in, wo_in, g_in, u_in, wd_in)
    buffers = [gain] + scratch
    loads = [pltpu.make_async_copy(src, buf, in_sem.at[i]) for i, (src, buf) in enumerate(zip(sources, buffers))]
    pairs = zip(small + scratch, small_outs + outs)
    stores = [pltpu.make_async_copy(buf, out, out_sem.at[i]) for i, (buf, out) in enumerate(pairs)]
    for load in loads:
        load.start()
    loads[0].wait()
    for i, (buf, store) in enumerate(zip(small, stores)):
        buf[...] = gain[i : i + 1, : buf.shape[0]].reshape(buf.shape)
        store.start()
    for load, store in zip(loads[1:], stores[len(small) :]):
        load.wait()
        store.start()
    for store in stores:
        store.wait()


def deliver(*results):
    hbm = pl.BlockSpec(memory_space=pl.ANY)
    dma = pltpu.SemaphoreType.DMA
    sizes = [(T, D, BF16)] * 2 + [(64, width, F32) for width in (NQ, D, D)] + [(128, D, F32)]
    sizes += [(64, FF, F32)] * 2 + [(192, D, F32)]
    small = (64, 64, 128, 128)
    scratch = [VM(size[:2], size[2]) for size in sizes] + [VM((size,), F32) for size in small]
    return pl.pallas_call(
        deliver_kernel,
        name="deliver",
        out_shape=tuple([shape(*size) for size in sizes] + [jax.ShapeDtypeStruct((size,), F32) for size in small]),
        in_specs=[hbm] * len(results),
        out_specs=(hbm,) * len(scratch),
        scratch_shapes=scratch + [VM((8, 128), F32), dma((16,)), dma((16,))],
    )(*results)


def solution(mesh):
    axis_name = mesh.axis_names[0]
    sharded = P(axis_name)
    in_specs = (sharded,) * 5 + (P(), P()) + (sharded,) * 7
    out_specs = (sharded,) * 4 + (P(), P()) + (sharded,) * 7

    def device_step(hidden, grad_out, positions, norm1, norm2, gain_q, gain_k, w_q, w_k, w_v, w_o, w_gate, w_up, w_down):
        inv_freq = ROPE_THETA ** (-2.0 * jnp.arange(HD // 2, dtype=F32) / HD)
        x, dy = hidden.reshape(T, D), grad_out.reshape(T, D)
        results = layer_call(positions, inv_freq[None, :], norm1, norm2, gain_q, gain_k, x, dy, w_q, w_k, w_v, w_o, w_gate, w_up, w_down)
        out, d_hidden, d_wq, d_wk, d_wv, d_wo, d_wg, d_wu, d_wd, d_n1, d_n2, d_qn, d_kn = deliver(*results)
        out, d_hidden = out.reshape(hidden.shape), d_hidden.reshape(hidden.shape)
        return out, d_hidden, d_n1, d_n2, d_qn, d_kn, d_wq, d_wk, d_wv, d_wo, d_wg, d_wu, d_wd

    return jax.shard_map(device_step, mesh=mesh, in_specs=in_specs, out_specs=out_specs, check_vma=False)
```

```python
import jax
import jax.numpy as jnp
from jax import lax
from jax.experimental import pallas as pl
from jax.experimental.pallas import tpu as pltpu
from jax.sharding import PartitionSpec as P

RMS_EPS = 1e-6
ROPE_THETA = 1000000.0
MESH = pl.DeviceIdType.MESH
F32 = jnp.float32
BF16 = jnp.bfloat16
T = 128
D = 1024
NQ = 2048
FF = 3072
HD = 128
Z, Y, X, C = 0, 1, 2, 3
STRIDE = (8, 4, 2, 1)
ALL = slice(None)
VM = pltpu.VMEM
HIGH_VMEM = 67043328


def nn(left_op, right_op):
    return jnp.dot(left_op, right_op, preferred_element_type=F32)


def nt(left_op, right_op):
    return lax.dot_general(left_op, right_op, (((1,), (1,)), ((), ())), preferred_element_type=F32)


def tn(left_op, right_op):
    return lax.dot_general(left_op, right_op, (((0,), (0,)), ((), ())), preferred_element_type=F32)


def rms(val):
    return lax.rsqrt(jnp.mean(val * val, axis=-1, keepdims=True) + RMS_EPS)


def norm_backward(d_unit, unit_val, scale_val):
    return scale_val * (d_unit - unit_val * jnp.mean(d_unit * unit_val, axis=-1, keepdims=True))


class Place:
    def __init__(self):
        self.me = lax.axis_index("fsdp")
        self.bit = [lax.rem(lax.div(self.me, s), 2) for s in STRIDE]

    def near(self, dim):
        return (self.me + STRIDE[dim] * (1 - 2 * self.bit[dim]),)

    def greet(self, dims):
        barrier = pltpu.get_barrier_semaphore()
        for dim in dims:
            pl.semaphore_signal(barrier, inc=1, device_id=self.near(dim), device_id_type=MESH)
        pl.semaphore_wait(barrier, len(dims))


class Spread:
    def __init__(self, place, own, first, buf, sub, order, axes, sems, part):
        self.place, self.buf, self.sub, self.order, self.axes = place, buf, sub, order, axes
        self.link_send, self.link_recv, self.core_send, self.core_recv, self.local_sem = sems
        self.part, self.last = part, len(order)
        self.source = own
        self.mine = self.block(()) if own is None else own
        self.first = self.mine if first is None else first

    def block(self, full, flip=None):
        index = []
        for dim in self.axes:
            if dim in full:
                index.append(ALL)
            elif dim == flip:
                index.append(1 - self.place.bit[dim])
            else:
                index.append(self.place.bit[dim])
        return self.buf.at[tuple(index) + self.sub]

    def copy_own(self):
        return pltpu.make_async_copy(self.source, self.block(()), self.local_sem.at[self.part])

    def link(self, step):
        dst = self.block(self.order[:step])
        return pltpu.make_async_remote_copy(
            src_ref=self.first if step == 0 else dst,
            dst_ref=dst,
            send_sem=self.link_send.at[self.part, step],
            recv_sem=self.link_recv.at[self.part, step],
            device_id=self.place.near(self.order[step]),
            device_id_type=MESH,
        )

    def core(self, step):
        dst = self.block(()) if step == 0 else self.block(self.order[: step - 1], self.order[step - 1])
        return pltpu.make_async_remote_copy(
            src_ref=self.mine if step == 0 else dst,
            dst_ref=dst,
            send_sem=self.core_send.at[self.part, step],
            recv_sem=self.core_recv.at[self.part, step],
            device_id=self.place.near(C),
            device_id_type=MESH,
        )

    def begin(self):
        self.link(0).start()
        if self.source is not None:
            self.copy_own().start()
        self.core(0).start()

    def advance(self, step):
        if step == 0 and self.source is not None:
            self.copy_own().wait()
        self.link(step).wait_recv()
        if step + 1 < self.last:
            self.link(step + 1).start()
        self.core(step + 1).start()

    def arrived(self):
        for step in range(self.last + 1):
            self.core(step).wait_recv()

    def drain(self):
        for step in range(self.last):
            self.link(step).wait_send()
        for step in range(self.last + 1):
            self.core(step).wait_send()


class Group:
    def __init__(self, place, axes):
        self.place, self.axes = place, axes
        self.position = self.spot(place.bit)

    def others(self):
        for number in range(2 ** len(self.axes) - 1, 0, -1):
            bit = list(self.place.bit)
            for i, dim in enumerate(self.axes):
                if number >> i & 1:
                    bit[dim] = 1 - bit[dim]
            yield bit

    def spot(self, bit):
        total = 0
        for dim in self.axes:
            total = total * 2 + bit[dim]
        return total


def device_of(bit):
    return (sum(stride * value for stride, value in zip(STRIDE, bit)),)


class Exchange:
    def __init__(self, group, number, piece, slot, blocks, sems):
        self.group, self.piece, self.slot, self.blocks = group, piece, slot, blocks
        self.send, self.recv, self.local = (sem.at[number] for sem in sems)

    def own(self):
        return pltpu.make_async_copy(self.piece(self.group.place.bit), self.slot, self.local)

    def begin(self):
        for bit in self.group.others():
            pltpu.make_async_remote_copy(
                src_ref=self.piece(bit),
                dst_ref=self.slot,
                send_sem=self.send,
                recv_sem=self.recv,
                device_id=device_of(bit),
                device_id_type=MESH,
            ).start()
        self.own().start()

    def arrived(self):
        self.own().wait()
        pltpu.make_async_copy(self.blocks, self.blocks, self.recv).wait()

    def drain(self):
        pltpu.make_async_copy(self.blocks, self.blocks, self.send).wait()


def head_forward(proj, gain, cos, sin):
    val = proj.astype(F32)
    scaled = val * rms(val) * gain
    return (scaled * cos + pltpu.roll(scaled, 64, axis=1) * sin).astype(BF16)


def head_backward(d_rot, proj, gain, cos, sin):
    val = proj.astype(F32)
    scale = rms(val)
    unit = val * scale
    d_scaled = d_rot * cos - pltpu.roll(d_rot, 64, axis=1) * sin
    d_gain = jnp.sum(d_scaled * unit, axis=0, keepdims=True)
    return norm_backward(d_scaled * gain, unit, scale).astype(BF16), d_gain


def cols(i, width):
    return pl.ds(pl.multiple_of(i * width, width), width)


def loop(count, body, init=0):
    return lax.fori_loop(0, count, body, init)


def each(count):
    def run(body):
        def step(i, _):
            body(i)
            return 0

        loop(count, step)

    return run


def two(i):
    return lax.div(i, 2), lax.rem(i, 2)


def three(i):
    return two(lax.div(i, 2)) + (lax.rem(i, 2),)


def layer_kernel(
    pos_ref, freq_ref, n1_ref, n2_ref, qn_ref, kn_ref, x_ref, dy_ref, wq, wk, wv, wo, wg, wu, wd,
    y_out, dh_out, oqkv, ogu, wo_out, wd_out, gain_out,
    y_ref, dh_ref, owo, owd, ogain,
    gains, gbuf, bq, bk, bv, bo, bg, bu, bd, g1, g2,
    xp, trig, n_s, q_s, k_s, v_s, qr, kr, probs, ctx, h_s, m_s, spare, act, dact, dctx, dres,
    part_a, part_y, part_m, part_n, land_a, land_y, land_m, land_n,
    at_ref, ct_ref, dqkv, dgu, gpart,
    nbuf, mbuf, dybuf, drbuf, gubuf, qkvbuf, abuf, cbuf,
    rgu, rqkv, rwd, rwo, zgu, zqkv, zwd, zwo, gainbuf,
    link_send, link_recv, core_send, core_recv, local_sem, one_send, one_recv, one_local, far_send, far_recv,
):
    place = Place()
    me = place.me
    z, y, x, c = place.bit
    sems = (link_send, link_recv, core_send, core_recv, local_sem)
    one = (one_send, one_recv, one_local)
    parts = []

    def spread(own, first, buf, sub, order, axes):
        parts.append(Spread(place, own, first, buf, sub, order, axes, sems, len(parts)))
        return parts[-1]

    both = (ALL, ALL)
    turns = ((Y, X), (X, Y))

    def by_columns(src, buf):
        half = src.shape[1] // 2
        size = half // 2
        made = []
        for i in range(2):
            mine, theirs = (src.at[:, pl.ds(pl.multiple_of(side * half + i * size, size), size)] for side in (z, 1 - z))
            made.append(spread(mine, theirs, buf, (ALL, pl.ds(i * size, size)), (Z,) + turns[i], (Z, Y, X, C)))
        return made

    def by_rows(src, buf):
        size = src.shape[0] // 2
        made = []
        for i in range(2):
            rows = pl.ds(i * size, size)
            made.append(spread(src.at[rows], None, buf, (rows, ALL), turns[i], (Y, X, C)))
        return made

    p_qkv = by_columns(wq, bq) + by_columns(wk, bk) + by_columns(wv, bv)
    p_o, p_d = by_rows(wo, bo), by_rows(wd, bd)
    p_g, p_u = by_columns(wg, bg), by_columns(wu, bu)
    p_m = spread(None, None, mbuf, both, (X,), (X, C))
    p_n = spread(None, None, nbuf, both, (Y,), (Y, C))
    p_dy = spread(None, None, dybuf, (ALL, ALL, ALL), (Y,), (Y, C))
    p_dr = spread(None, None, drbuf, (ALL, ALL, ALL), (X,), (X, C))

    grp_x, grp_y = Group(place, (X, C)), Group(place, (Y, C))

    def share(number, group, piece, buf):
        return Exchange(group, number, piece, buf.at[group.position], buf.at[pl.ds(0, 3)], one)

    def cols_for(group, ref, width):
        return lambda bit: ref.at[:, pl.ds(pl.multiple_of(group.spot(bit) * width, 128), width)]

    e_gu = share(0, grp_x, cols_for(grp_x, dgu, 768), gubuf)
    e_qkv = share(1, grp_y, cols_for(grp_y, dqkv, 512), qkvbuf)
    e_a = share(2, grp_y, lambda bit: at_ref.at[bit[Y], :, bit[C]], abuf)
    e_c = share(3, grp_x, lambda bit: ct_ref.at[:, bit[X], bit[C]], cbuf)
    gain_number, norm_number = 9, 10
    sent = []

    leaving = []

    def leave(buf, out):
        leaving.append(pltpu.make_async_copy(buf, out, local_sem.at[len(parts) + 2 + len(leaving)]))
        leaving[-1].start()

    def near_copy(dim, source, target):
        number = len(sent)
        sent.append(
            pltpu.make_async_remote_copy(
                src_ref=source, dst_ref=target, send_sem=far_send.at[number], recv_sem=far_recv.at[number],
                device_id=place.near(dim), device_id_type=MESH,
            )
        )
        return sent[-1]

    mine = cols(z, T)

    def pair_rows(i):
        return cols(4 * z + i, 32)

    barrier = pltpu.get_barrier_semaphore()

    def other(k):
        return (lax.rem(me + k, 16),)

    @each(15)
    def _(k):
        pl.semaphore_signal(barrier, inc=1, device_id=other(k + 1), device_id_type=MESH)

    gains[...] = jnp.zeros(gains.shape, F32)
    halves = [ref[...].astype(F32).reshape(1, 64) for ref in (n1_ref, n2_ref)]
    gains[0:1, :] = jnp.concatenate(halves, axis=1)
    gains[1:2, :] = qn_ref[...].astype(F32).reshape(1, 128)
    gains[2:3, :] = kn_ref[...].astype(F32).reshape(1, 128)
    angle = jnp.broadcast_to(pos_ref[...].astype(F32), (T, T)).T[:, : HD // 2] * freq_ref[...]
    cos_half, sin_half = jnp.cos(angle), jnp.sin(angle)
    trig[z] = jnp.concatenate([cos_half, cos_half, -sin_half, sin_half], axis=1)
    pl.semaphore_wait(barrier, 15)

    def to_all(source, buf, number):
        @each(15)
        def _(k):
            pltpu.make_async_remote_copy(
                src_ref=source, dst_ref=buf.at[me], send_sem=one_send.at[number], recv_sem=one_recv.at[number],
                device_id=other(k + 1), device_id_type=MESH,
            ).start()

    def all_wait(buf, sem):
        fifteen = buf.at[pl.ds(0, 15)]
        pltpu.make_async_copy(fifteen, fifteen, sem).wait()

    to_all(gains, gbuf, norm_number)
    for item in p_qkv + p_o:
        item.begin()
    x_copy = near_copy(Z, x_ref, xp.at[mine])
    trig_copy = near_copy(Z, trig.at[z], trig.at[z])
    x_copy.start()
    own_x = pltpu.make_async_copy(x_ref, xp.at[mine], local_sem.at[len(parts)])
    own_x.start()
    for item in p_d + p_g + p_u:
        item.begin()
    trig_copy.start()
    dy_copy = near_copy(Z, dy_ref, dybuf.at[y, c, z])
    dy_copy.start()
    own_dy = pltpu.make_async_copy(dy_ref, dybuf.at[y, c, z], local_sem.at[len(parts) + 1])
    own_dy.start()
    for item in p_qkv + p_o:
        item.advance(0)
    gq, gk = gains[1:2, :], gains[2:3, :]
    all_wait(gbuf, one_recv.at[norm_number])
    gbuf[me] = gains[...]
    lane = lax.broadcasted_iota(jnp.int32, (8, 128), 1) < 64
    for i in range(8):
        first, second = gbuf[2 * i], gbuf[2 * i + 1]
        tile = slice(128 * i, 128 * i + 128)
        g1[:, tile] = jnp.where(lane, first, pltpu.roll(second, 64, axis=1))[:1]
        g2[:, tile] = jnp.where(lane, pltpu.roll(first, 64, axis=1), second)[:1]
    own_x.wait()
    x_copy.wait_recv()

    @each(8)
    def _(i):
        rows = cols(i, 32)
        val = xp[rows].astype(F32)
        n_s[rows] = (val * rms(val) * g1[...]).astype(BF16)

    def turned(val):
        return val.astype(F32).T.astype(BF16)

    for item in p_qkv:
        item.advance(1)
    for item in p_d:
        item.advance(0)

    @each(4)
    def _(i):
        nbuf[y, c, cols(i, 256)] = turned(n_s[:, cols(i, 256)])

    for item in p_o:
        item.advance(1)
    for item in p_g + p_u:
        item.advance(0)
    for item in p_qkv:
        item.advance(2)
    trig_copy.wait_recv()

    def weight(buf, tile):
        block = buf[(ALL,) * (len(buf.shape) - 1) + (tile,)]
        return block.reshape(-1, block.shape[-1])

    def project(buf, dst, width, tiles):
        @each(tiles)
        def _(j):
            tile = cols(j, width)
            dst[:, tile] = nn(n_s[...], weight(buf, tile)).astype(BF16)

    for item in p_qkv:
        item.arrived()
    project(bq, q_s, 512, 2)
    project(bk, k_s, 512, 1)
    project(bv, v_s, 512, 1)
    scale = HD ** -0.5

    def sequence_head(j):
        seq, head = lax.div(j, 4), lax.rem(j, 4)
        return seq, head, cols(seq, T), cols(head, HD), cols(head, 2 * HD)

    @each(8)
    def _(j):
        seq, _, rows, kv, pair = sequence_head(j)
        cos, sin = trig[seq, :, :HD], trig[seq, :, HD:]
        k_rot = head_forward(k_s[rows, kv], gk, cos, sin)
        kr[rows, kv] = k_rot
        q_pair = q_s[rows, pair]
        q_rot = jnp.concatenate(
            [head_forward(half, gq, cos, sin) for half in (q_pair[:, :HD], q_pair[:, HD:])], axis=0
        )
        qr[j] = q_rot
        scores = nt(q_rot, k_rot) * scale
        row = lax.rem(lax.broadcasted_iota(jnp.int32, (2 * T, T), 0), T)
        col = lax.broadcasted_iota(jnp.int32, (2 * T, T), 1)
        scores = jnp.where(row >= col, scores, -1e30)
        expd = jnp.exp(scores - jnp.max(scores, axis=-1, keepdims=True))
        prob = expd / jnp.sum(expd, axis=-1, keepdims=True)
        probs[j] = prob
        out = nn(prob.astype(BF16), v_s[rows, kv])
        ctx[rows, pair] = jnp.concatenate([out[:T], out[T:]], axis=1).astype(BF16)

    def pair_sum(partial, landing, compute):
        copies = []
        for half in range(2):
            @each(2)
            def _(j):
                i = j + 2 * half
                partial[:, :, cols(i, 256)] = compute(i).reshape(2, T, 256)

            span = (ALL, pl.ds(512 * half, 512))
            copies.append(near_copy(Z, partial.at[(1 - z,) + span], landing.at[span]))
            copies[-1].start()
        return copies

    def received(copies):
        for copy in copies:
            copy.wait_recv()

    for item in p_o:
        item.arrived()
    a_copies = pair_sum(part_a, land_a, lambda i: nn(ctx[...], weight(bo, cols(i, 256))))
    for item in p_g + p_u:
        item.advance(1)
    for item in p_d:
        item.advance(1)

    @each(4)
    def _(i):
        ct_ref[two(i)] = turned(ctx[:, cols(i, 256)]).reshape(2, 128, 2 * T)

    received(a_copies)

    @each(4)
    def _(i):
        rows = cols(i, 32)
        attn = (part_a[z, rows] + land_a[rows]).astype(BF16)
        val = (xp[pair_rows(i)].astype(F32) + attn.astype(F32)).astype(BF16).astype(F32)
        h_s[rows] = val
        m_s[pair_rows(i)] = (val * rms(val) * g2[...]).astype(BF16)

    m_copy = near_copy(Z, m_s.at[mine], m_s.at[mine])
    m_copy.start()
    for item in p_d:
        item.arrived()
    own_dy.wait()
    dy_copy.wait_recv()

    @each(4)
    def _(i):
        dact[:, cols(i, 384)] = nt(dybuf[y, c].reshape(2 * T, D), bd[two(i)].reshape(384, D))

    m_copy.wait_recv()

    @each(4)
    def _(i):
        mbuf[x, c, cols(i, 256)] = turned(m_s[:, cols(i, 256)])

    for item in p_g + p_u:
        item.advance(2)
    p_m.begin()
    p_dy.begin()
    e_c.begin()
    for item in p_g + p_u:
        item.arrived()
    fh = FF // 2

    @each(fh // 256)
    def _(j):
        tile = cols(j, 256)
        gate_val = nn(m_s[...], weight(bg, tile)).astype(BF16).astype(F32)
        up_val = nn(m_s[...], weight(bu, tile)).astype(BF16).astype(F32)
        sig = jax.nn.sigmoid(gate_val)
        act[:, tile] = (gate_val * sig * up_val).astype(BF16)
        d_act = dact[:, tile]
        dgu[:, tile] = (d_act * up_val * sig * (1.0 + gate_val * (1.0 - sig))).astype(BF16)
        dgu[:, cols(j + fh // 256, 256)] = (d_act * gate_val * sig).astype(BF16)

    def d_mlp_in(i):
        rows = two(i)
        return nt(dgu[:, :fh], bg[rows].reshape(256, fh)) + nt(dgu[:, fh:], bu[rows].reshape(256, fh))

    e_gu.begin()
    m_copies = pair_sum(part_m, land_m, d_mlp_in)

    @each(4)
    def _(i):
        at_ref[two(i)] = turned(act[:, cols(i, 384)]).reshape(2, 192, 2 * T)

    e_a.begin()
    p_n.begin()
    received(m_copies)

    def d_res_rows(i, total):
        rows = cols(i, 32)
        val = h_s[rows]
        r_scale = rms(val)
        unit = val * r_scale
        grad = part_m[z, rows] + land_m[rows]
        out = dybuf[y, c, z, rows].astype(F32) + norm_backward(grad * g2[...], unit, r_scale)
        dres[rows] = out
        drbuf[x, c, z, rows] = out.astype(BF16)
        return total + jnp.sum(grad * unit, axis=0, keepdims=True)

    d_g2 = loop(4, d_res_rows, jnp.zeros((1, D), F32))
    r_copy = near_copy(Z, drbuf.at[x, c, z], drbuf.at[x, c, z])
    r_copy.start()
    y_copies = pair_sum(part_y, land_y, lambda i: nn(act[...], weight(bd, cols(i, 256))))
    inv_tokens = 1.0 / (16 * T)

    def row_tiles(left_buf, right_buf, out):
        @each(8)
        def _(j):
            tile = cols(lax.rem(j, 4), 256)
            half = lax.div(j, 4)
            left = jnp.concatenate([left_buf[i, half] for i in range(4)], axis=1)
            out[half, :, tile] = nn(left, weight(right_buf, tile)) * inv_tokens

    p_dy.advance(0)
    p_dy.arrived()
    e_a.arrived()
    row_tiles(abuf, dybuf, rwd)
    r_copy.wait_recv()
    p_dr.begin()
    wd_far = near_copy(X, rwd.at[1 - x], zwd)
    wd_far.start()

    @each(2)
    def _(i):
        dctx[:, cols(i, 512)] = nt(drbuf[x, c].reshape(2 * T, D), bo[i].reshape(512, D)).astype(BF16)

    def attend_back(j, carry):
        q_total, k_total = carry
        seq, head, rows, kv, pair = sequence_head(j)
        cos, sin = trig[seq, :, :HD], trig[seq, :, HD:]
        d_out = dctx[rows, pair]
        d_out = jnp.concatenate([d_out[:, :HD], d_out[:, HD:]], axis=0)
        prob = probs[j]
        d_value = tn(prob.astype(BF16), d_out).astype(BF16)
        d_prob = nt(d_out, v_s[rows, kv])
        d_score = prob * (d_prob - jnp.sum(prob * d_prob, axis=-1, keepdims=True))
        d_score = (d_score * scale).astype(BF16)
        d_q_rot = nn(d_score, kr[rows, kv])
        d_k_rot = tn(d_score, qr[j])
        q_pair = q_s[rows, pair]
        d_q0, g_q0 = head_backward(d_q_rot[:T], q_pair[:, :HD], gq, cos, sin)
        d_q1, g_q1 = head_backward(d_q_rot[T:], q_pair[:, HD:], gq, cos, sin)
        d_k, g_k = head_backward(d_k_rot, k_s[rows, kv], gk, cos, sin)
        dqkv[rows, pair] = jnp.concatenate([d_q0, d_q1], axis=1)
        dqkv[rows, cols(head + 8, HD)] = d_k
        dqkv[rows, cols(head + 12, HD)] = d_value
        return q_total + g_q0 + g_q1, k_total + g_k

    zero = jnp.zeros((1, HD), F32)
    q_total, k_total = loop(8, attend_back, (zero, zero))
    e_qkv.begin()

    def d_normed(i):
        rows = two(i)
        grad = nt(dqkv[:, :D], bq[rows].reshape(256, D)) + nt(dqkv[:, D : D + 512], bk[rows].reshape(256, 512))
        return grad + nt(dqkv[:, D + 512 :], bv[rows].reshape(256, 512))

    n_copies = pair_sum(part_n, land_n, d_normed)

    def column_chunk(acts, grads, out, chunk):
        @each(8)
        def _(i):
            rows = cols(i, 128)
            left = jnp.concatenate([acts[k // 2, k % 2, rows] for k in range(4)], axis=1)
            right = grads[:, :, 256 * chunk : 256 * chunk + 256].reshape(8 * T, 256)
            out[(chunk,) + three(i)] = (nn(left, right) * inv_tokens).reshape(2, 64, 256)

    def half_of(dim, result, chunk):
        bit = place.bit[dim]
        return result.at[(chunk,) + tuple(1 - bit if k == dim else ALL for k in range(4))]

    p_m.advance(0)
    p_m.arrived()
    e_gu.arrived()
    gu_far = []
    for chunk in range(3):
        column_chunk(mbuf, gubuf, rgu, chunk)
        gu_far.append(near_copy(Y, half_of(Y, rgu, chunk), zgu.at[chunk]))
        gu_far[-1].start()
    p_n.advance(0)
    p_n.arrived()
    e_qkv.arrived()
    qkv_far = []
    for chunk in range(2):
        column_chunk(nbuf, qkvbuf, rqkv, chunk)
        qkv_far.append(near_copy(X, half_of(X, rqkv, chunk), zqkv.at[chunk]))
        qkv_far[-1].start()
    p_dr.advance(0)
    p_dr.arrived()
    e_c.arrived()
    row_tiles(cbuf, drbuf, rwo)
    wo_far = near_copy(Y, rwo.at[1 - y], zwo)
    wo_far.start()

    received(n_copies)

    def d_hidden_rows(i, total):
        rows = cols(i, 32)
        val = xp[pair_rows(i)].astype(F32)
        x_scale = rms(val)
        unit = val * x_scale
        grad = part_n[z, rows] + land_n[rows]
        dh_ref[rows] = (dres[rows] + norm_backward(grad * g1[...], unit, x_scale)).astype(BF16)
        return total + jnp.sum(grad * unit, axis=0, keepdims=True)

    d_g1 = loop(4, d_hidden_rows, jnp.zeros((1, D), F32))
    leave(dh_ref, dh_out)
    gpart[...] = jnp.zeros(gpart.shape, F32)
    for i in range(8):
        tile = slice(128 * i, 128 * i + 128)
        gpart[i : i + 1, :] = d_g1[:, tile]
        gpart[8 + i : 9 + i, :] = d_g2[:, tile]
    gpart[16:17, :] = q_total
    gpart[17:18, :] = k_total

    to_all(gpart, gainbuf, gain_number)
    received(y_copies)

    @each(4)
    def _(i):
        rows = cols(i, 32)
        out = (part_y[z, rows] + land_y[rows]).astype(BF16).astype(F32)
        y_ref[rows] = (h_s[rows] + out).astype(BF16)

    leave(y_ref, y_out)

    def final(dim, number, result, target, out, chunk, base):
        group = Group(place, tuple(k for k in range(4) if k != dim))
        for bit in list(group.others()) + [place.bit]:
            index = (chunk,) + tuple(bit)
            result[index] = result[index] + target[(chunk,) + tuple(bit[k] for k in group.axes)]
        where = pl.ds(pl.multiple_of(base + 256 * chunk, 128), 256)
        move = Exchange(
            group, number, lambda bit: result.at[(chunk,) + tuple(bit)], out.at[:, where],
            out.at[:, pl.ds(0, 7 * 256)], one,
        )
        move.begin()
        return move

    gu_base = x * FF + z * fh + c * 768
    qkv_base = (1 - y) * (z * D + c * 512) + y * (NQ + c * D + z * 512)
    moves = []
    for kind, chunk in ((0, 0), (1, 0), (0, 1), (1, 1), (0, 2)):
        if kind == 0:
            gu_far[chunk].wait_recv()
            moves.append(final(Y, 4 + chunk, rgu, zgu, ogu, chunk, gu_base))
        else:
            qkv_far[chunk].wait_recv()
            moves.append(final(X, 7 + chunk, rqkv, zqkv, oqkv, chunk, qkv_base))
    wd_far.wait_recv()
    owd[...] = rwd[x] + zwd[...]
    leave(owd, wd_out)
    wo_far.wait_recv()
    owo[...] = rwo[y] + zwo[...]
    leave(owo, wo_out)
    all_wait(gainbuf, one_recv.at[gain_number])
    gainbuf[me] = gpart[...]
    gainbuf[0] = loop(16, lambda i, total: total + gainbuf[i], jnp.zeros((24, 128), F32)) * inv_tokens
    for i in range(2):
        row = gainbuf[0, pl.ds(8 * i + lax.div(me, 2), 1), :]
        ogain[i : i + 1, :] = jnp.where(c == 0, row, pltpu.roll(row, 64, axis=1))
    ogain[2:4, :] = gainbuf[0, 16:18, :]
    ogain[4:8, :] = jnp.zeros((4, 128), F32)
    leave(ogain, gain_out)
    for move in moves:
        move.arrived()
    for item in moves + [e_gu, e_qkv, e_a, e_c] + parts:
        item.drain()
    for copy in sent:
        copy.wait_send()
    for copy in leaving:
        copy.wait()
    all_wait(gainbuf, one_send.at[gain_number])
    all_wait(gbuf, one_send.at[norm_number])


def shape(rows, width, dtype):
    return jax.ShapeDtypeStruct((rows, width), dtype)


def many(count, *args):
    return [VM(*args)] * count


def layer_call(*operands):
    vmem = pl.BlockSpec(memory_space=VM)
    hbm = pl.BlockSpec(memory_space=pl.ANY)
    dma = pltpu.SemaphoreType.DMA
    t2, kvh, fh = 2 * T, D // 2, FF // 2
    cube, square, line = (2, 2, 2, 2), (2, 2, 2), (2, 2)
    spreads = 18
    return pl.pallas_call(
        layer_kernel,
        name="layer",
        out_shape=(
            shape(T, D, BF16), shape(T, D, BF16), shape(64, NQ + 2 * D, F32), shape(64, 2 * FF, F32),
            shape(128, D, F32), shape(192, D, F32), shape(8, 128, F32),
        ),
        in_specs=[vmem] * 6 + [hbm] * 9,
        out_specs=(hbm,) * 7,
        scratch_shapes=[
            *many(2, (T, D), BF16), VM((T, D), F32), VM((192, D), F32), VM((8, 128), F32),
            VM((8, 128), F32), VM((16, 8, 128), F32), VM(cube + (64, D), BF16), *many(2, cube + (64, kvh), BF16),
            VM(square + (128, D), BF16), *many(2, cube + (64, fh), BF16), VM(square + (192, D), BF16),
            *many(2, (1, D), F32),
            VM((t2, D), BF16), VM((2, T, t2), F32), VM((t2, D), BF16), VM((t2, D), BF16), *many(2, (t2, kvh), BF16),
            VM((8, t2, HD), BF16), VM((t2, kvh), BF16), VM((8, t2, T), F32), VM((t2, D), BF16), VM((T, D), F32),
            VM((t2, D), BF16), VM((8, 128), BF16), VM((t2, fh), BF16), VM((t2, fh), F32), VM((t2, D), BF16),
            VM((T, D), F32), *many(4, (2, T, D), F32), *many(4, (T, D), F32),
            VM(square + (192, t2), BF16), VM(square + (128, t2), BF16), VM((t2, NQ), BF16), VM((t2, FF), BF16),
            VM((24, 128), F32), *many(2, line + (D, t2), BF16), *many(2, line + (2, T, D), BF16),
            VM((4, t2, 768), BF16), VM((4, t2, 512), BF16), VM((4, 2, 192, t2), BF16), VM((4, 2, 128, t2), BF16),
            VM((3,) + cube + (64, 256), F32), VM((2,) + cube + (64, 256), F32), VM((2, 192, D), F32),
            VM((2, 128, D), F32), VM((3,) + square + (64, 256), F32), VM((2,) + square + (64, 256), F32),
            VM((192, D), F32), VM((128, D), F32), VM((16, 24, 128), F32),
            *[dma((spreads, 3))] * 2, *[dma((spreads, 4))] * 2, dma((spreads + 7,)), *[dma((11,))] * 3, *[dma((20,))] * 2,
        ],
        compiler_params=pltpu.CompilerParams(collective_id=0, has_side_effects=True, vmem_limit_bytes=HIGH_VMEM),
    )(*operands)


def deliver_kernel(y_in, dh_in, qkv_in, gu_in, wo_in, wd_in, gain_in, *refs):
    rest = iter(refs)
    outs, small_outs, scratch, small = ([next(rest) for _ in range(count)] for count in (9, 4, 9, 4))
    gain, in_sem, out_sem = rest
    spans = ((qkv_in, 0, NQ), (qkv_in, NQ, D), (qkv_in, NQ + D, D), (gu_in, 0, FF), (gu_in, FF, FF))
    q_in, k_in, v_in, g_in, u_in = (ref.at[:, pl.ds(start, size)] for ref, start, size in spans)
    sources = (gain_in, y_in, dh_in, q_in, k_in, v_in, wo_in, g_in, u_in, wd_in)
    buffers = [gain] + scratch
    loads = [pltpu.make_async_copy(src, buf, in_sem.at[i]) for i, (src, buf) in enumerate(zip(sources, buffers))]
    pairs = zip(small + scratch, small_outs + outs)
    stores = [pltpu.make_async_copy(buf, out, out_sem.at[i]) for i, (buf, out) in enumerate(pairs)]
    for load in loads:
        load.start()
    loads[0].wait()
    for i, (buf, store) in enumerate(zip(small, stores)):
        buf[...] = gain[i : i + 1, : buf.shape[0]].reshape(buf.shape)
        store.start()
    for load, store in zip(loads[1:], stores[len(small) :]):
        load.wait()
        store.start()
    for store in stores:
        store.wait()


def deliver(*results):
    hbm = pl.BlockSpec(memory_space=pl.ANY)
    dma = pltpu.SemaphoreType.DMA
    sizes = [(T, D, BF16)] * 2 + [(64, width, F32) for width in (NQ, D, D)] + [(128, D, F32)]
    sizes += [(64, FF, F32)] * 2 + [(192, D, F32)]
    small = (64, 64, 128, 128)
    scratch = [VM(size[:2], size[2]) for size in sizes] + [VM((size,), F32) for size in small]
    return pl.pallas_call(
        deliver_kernel,
        name="deliver",
        out_shape=tuple([shape(*size) for size in sizes] + [jax.ShapeDtypeStruct((size,), F32) for size in small]),
        in_specs=[hbm] * len(results),
        out_specs=(hbm,) * len(scratch),
        scratch_shapes=scratch + [VM((8, 128), F32), dma((16,)), dma((16,))],
    )(*results)


def solution(mesh):
    axis_name = mesh.axis_names[0]
    sharded = P(axis_name)
    in_specs = (sharded,) * 5 + (P(), P()) + (sharded,) * 7
    out_specs = (sharded,) * 4 + (P(), P()) + (sharded,) * 7

    def device_step(hidden, grad_out, positions, norm1, norm2, gain_q, gain_k, w_q, w_k, w_v, w_o, w_gate, w_up, w_down):
        inv_freq = ROPE_THETA ** (-2.0 * jnp.arange(HD // 2, dtype=F32) / HD)
        x, dy = hidden.reshape(T, D), grad_out.reshape(T, D)
        results = layer_call(positions, inv_freq[None, :], norm1, norm2, gain_q, gain_k, x, dy, w_q, w_k, w_v, w_o, w_gate, w_up, w_down)
        out, d_hidden, d_wq, d_wk, d_wv, d_wo, d_wg, d_wu, d_wd, d_n1, d_n2, d_qn, d_kn = deliver(*results)
        out, d_hidden = out.reshape(hidden.shape), d_hidden.reshape(hidden.shape)
        return out, d_hidden, d_n1, d_n2, d_qn, d_kn, d_wq, d_wk, d_wv, d_wo, d_wg, d_wu, d_wd

    return jax.shard_map(device_step, mesh=mesh, in_specs=in_specs, out_specs=out_specs, check_vma=False)
```

```python
import jax
import jax.numpy as jnp
from jax import lax
from jax.experimental import pallas as pl
from jax.experimental.pallas import tpu as pltpu
from jax.sharding import PartitionSpec as P

RMS_EPS = 1e-6
ROPE_THETA = 1000000.0
MESH = pl.DeviceIdType.MESH
F32 = jnp.float32
BF16 = jnp.bfloat16
T = 128
D = 1024
NQ = 2048
FF = 3072
HD = 128
Z, Y, X, C = 0, 1, 2, 3
STRIDE = (8, 4, 2, 1)
ALL = slice(None)
VM = pltpu.VMEM
HIGH_VMEM = 67043328


def nn(left_op, right_op):
    return jnp.dot(left_op, right_op, preferred_element_type=F32)


def nt(left_op, right_op):
    return lax.dot_general(left_op, right_op, (((1,), (1,)), ((), ())), preferred_element_type=F32)


def tn(left_op, right_op):
    return lax.dot_general(left_op, right_op, (((0,), (0,)), ((), ())), preferred_element_type=F32)


def rms(val):
    return lax.rsqrt(jnp.mean(val * val, axis=-1, keepdims=True) + RMS_EPS)


def norm_backward(d_unit, unit_val, scale_val):
    return scale_val * (d_unit - unit_val * jnp.mean(d_unit * unit_val, axis=-1, keepdims=True))


class Place:
    def __init__(self):
        self.me = lax.axis_index("fsdp")
        self.bit = [lax.rem(lax.div(self.me, s), 2) for s in STRIDE]

    def near(self, dim):
        return (self.me + STRIDE[dim] * (1 - 2 * self.bit[dim]),)

    def greet(self, dims):
        barrier = pltpu.get_barrier_semaphore()
        for dim in dims:
            pl.semaphore_signal(barrier, inc=1, device_id=self.near(dim), device_id_type=MESH)
        pl.semaphore_wait(barrier, len(dims))


class Spread:
    def __init__(self, place, own, first, buf, sub, order, axes, sems, part):
        self.place, self.buf, self.sub, self.order, self.axes = place, buf, sub, order, axes
        self.link_send, self.link_recv, self.core_send, self.core_recv, self.local_sem = sems
        self.part, self.last = part, len(order)
        self.source = own
        self.mine = self.block(()) if own is None else own
        self.first = self.mine if first is None else first

    def block(self, full, flip=None):
        index = []
        for dim in self.axes:
            if dim in full:
                index.append(ALL)
            elif dim == flip:
                index.append(1 - self.place.bit[dim])
            else:
                index.append(self.place.bit[dim])
        return self.buf.at[tuple(index) + self.sub]

    def copy_own(self):
        return pltpu.make_async_copy(self.source, self.block(()), self.local_sem.at[self.part])

    def link(self, step):
        dst = self.block(self.order[:step])
        return pltpu.make_async_remote_copy(
            src_ref=self.first if step == 0 else dst,
            dst_ref=dst,
            send_sem=self.link_send.at[self.part, step],
            recv_sem=self.link_recv.at[self.part, step],
            device_id=self.place.near(self.order[step]),
            device_id_type=MESH,
        )

    def core(self, step):
        dst = self.block(()) if step == 0 else self.block(self.order[: step - 1], self.order[step - 1])
        return pltpu.make_async_remote_copy(
            src_ref=self.mine if step == 0 else dst,
            dst_ref=dst,
            send_sem=self.core_send.at[self.part, step],
            recv_sem=self.core_recv.at[self.part, step],
            device_id=self.place.near(C),
            device_id_type=MESH,
        )

    def begin(self):
        self.link(0).start()
        if self.source is not None:
            self.copy_own().start()
        self.core(0).start()

    def advance(self, step):
        if step == 0 and self.source is not None:
            self.copy_own().wait()
        self.link(step).wait_recv()
        if step + 1 < self.last:
            self.link(step + 1).start()
        self.core(step + 1).start()

    def arrived(self):
        for step in range(self.last + 1):
            self.core(step).wait_recv()

    def drain(self):
        for step in range(self.last):
            self.link(step).wait_send()
        for step in range(self.last + 1):
            self.core(step).wait_send()


class Group:
    def __init__(self, place, axes):
        self.place, self.axes = place, axes
        self.position = self.spot(place.bit)

    def others(self):
        for number in range(2 ** len(self.axes) - 1, 0, -1):
            bit = list(self.place.bit)
            for i, dim in enumerate(self.axes):
                if number >> i & 1:
                    bit[dim] = 1 - bit[dim]
            yield bit

    def spot(self, bit):
        total = 0
        for dim in self.axes:
            total = total * 2 + bit[dim]
        return total


def device_of(bit):
    return (sum(stride * value for stride, value in zip(STRIDE, bit)),)


class Exchange:
    def __init__(self, group, number, piece, slot, blocks, sems):
        self.group, self.piece, self.slot, self.blocks = group, piece, slot, blocks
        self.send, self.recv, self.local = (sem.at[number] for sem in sems)

    def own(self):
        return pltpu.make_async_copy(self.piece(self.group.place.bit), self.slot, self.local)

    def begin(self):
        for bit in self.group.others():
            pltpu.make_async_remote_copy(
                src_ref=self.piece(bit),
                dst_ref=self.slot,
                send_sem=self.send,
                recv_sem=self.recv,
                device_id=device_of(bit),
                device_id_type=MESH,
            ).start()
        self.own().start()

    def arrived(self):
        self.own().wait()
        pltpu.make_async_copy(self.blocks, self.blocks, self.recv).wait()

    def drain(self):
        pltpu.make_async_copy(self.blocks, self.blocks, self.send).wait()


def head_forward(proj, gain, cos, sin):
    val = proj.astype(F32)
    scaled = val * rms(val) * gain
    return (scaled * cos + pltpu.roll(scaled, 64, axis=1) * sin).astype(BF16)


def head_backward(d_rot, proj, gain, cos, sin):
    val = proj.astype(F32)
    scale = rms(val)
    unit = val * scale
    d_scaled = d_rot * cos - pltpu.roll(d_rot, 64, axis=1) * sin
    d_gain = jnp.sum(d_scaled * unit, axis=0, keepdims=True)
    return norm_backward(d_scaled * gain, unit, scale).astype(BF16), d_gain


def cols(i, width):
    return pl.ds(pl.multiple_of(i * width, width), width)


def loop(count, body, init=0):
    return lax.fori_loop(0, count, body, init)


def each(count):
    def run(body):
        def step(i, _):
            body(i)
            return 0

        loop(count, step)

    return run


def two(i):
    return lax.div(i, 2), lax.rem(i, 2)


def three(i):
    return two(lax.div(i, 2)) + (lax.rem(i, 2),)


def layer_kernel(
    pos_ref, freq_ref, n1_ref, n2_ref, qn_ref, kn_ref, x_ref, dy_ref, wq, wk, wv, wo, wg, wu, wd,
    y_out, dh_out, oqkv, ogu, wo_out, wd_out, gain_out,
    y_ref, dh_ref, owo, owd, ogain,
    gains, gbuf, bq, bk, bv, bo, bg, bu, bd, g1, g2,
    xp, trig, n_s, q_s, k_s, v_s, qr, kr, probs, ctx, h_s, m_s, spare, act, dact, dctx, dres,
    part_a, part_y, part_m, part_n, land_a, land_y, land_m, land_n,
    at_ref, ct_ref, dqkv, dgu, gpart,
    nbuf, mbuf, dybuf, drbuf, gubuf, qkvbuf, abuf, cbuf,
    rgu, rqkv, rwd, rwo, zgu, zqkv, zwd, zwo, gainbuf,
    link_send, link_recv, core_send, core_recv, local_sem, one_send, one_recv, one_local, far_send, far_recv,
):
    place = Place()
    me = place.me
    z, y, x, c = place.bit
    sems = (link_send, link_recv, core_send, core_recv, local_sem)
    one = (one_send, one_recv, one_local)
    parts = []

    def spread(own, first, buf, sub, order, axes):
        parts.append(Spread(place, own, first, buf, sub, order, axes, sems, len(parts)))
        return parts[-1]

    both = (ALL, ALL)
    turns = ((Y, X), (X, Y))

    def by_columns(src, buf):
        half = src.shape[1] // 2
        size = half // 2
        made = []
        for i in range(2):
            mine, theirs = (src.at[:, pl.ds(pl.multiple_of(side * half + i * size, size), size)] for side in (z, 1 - z))
            made.append(spread(mine, theirs, buf, (ALL, pl.ds(i * size, size)), (Z,) + turns[i], (Z, Y, X, C)))
        return made

    def by_rows(src, buf):
        size = src.shape[0] // 2
        made = []
        for i in range(2):
            rows = pl.ds(i * size, size)
            made.append(spread(src.at[rows], None, buf, (rows, ALL), turns[i], (Y, X, C)))
        return made

    p_qkv = by_columns(wq, bq) + by_columns(wk, bk) + by_columns(wv, bv)
    p_o, p_d = by_rows(wo, bo), by_rows(wd, bd)
    p_g, p_u = by_columns(wg, bg), by_columns(wu, bu)
    p_m = spread(None, None, mbuf, both, (X,), (X, C))
    p_n = spread(None, None, nbuf, both, (Y,), (Y, C))
    p_dy = spread(None, None, dybuf, (ALL, ALL, ALL), (Y,), (Y, C))
    p_dr = spread(None, None, drbuf, (ALL, ALL, ALL), (X,), (X, C))

    grp_x, grp_y = Group(place, (X, C)), Group(place, (Y, C))

    def share(number, group, piece, buf):
        return Exchange(group, number, piece, buf.at[group.position], buf.at[pl.ds(0, 3)], one)

    def cols_for(group, ref, width):
        return lambda bit: ref.at[:, pl.ds(pl.multiple_of(group.spot(bit) * width, 128), width)]

    e_gu = share(0, grp_x, cols_for(grp_x, dgu, 768), gubuf)
    e_qkv = share(1, grp_y, cols_for(grp_y, dqkv, 512), qkvbuf)
    e_a = share(2, grp_y, lambda bit: at_ref.at[bit[Y], :, bit[C]], abuf)
    e_c = share(3, grp_x, lambda bit: ct_ref.at[:, bit[X], bit[C]], cbuf)
    gain_number, norm_number = 9, 10
    sent = []

    leaving = []

    def leave(buf, out):
        leaving.append(pltpu.make_async_copy(buf, out, local_sem.at[len(parts) + 2 + len(leaving)]))
        leaving[-1].start()

    def near_copy(dim, source, target):
        number = len(sent)
        sent.append(
            pltpu.make_async_remote_copy(
                src_ref=source, dst_ref=target, send_sem=far_send.at[number], recv_sem=far_recv.at[number],
                device_id=place.near(dim), device_id_type=MESH,
            )
        )
        return sent[-1]

    mine = cols(z, T)

    def pair_rows(i):
        return cols(4 * z + i, 32)

    barrier = pltpu.get_barrier_semaphore()

    def other(k):
        return (lax.rem(me + k, 16),)

    @each(15)
    def _(k):
        pl.semaphore_signal(barrier, inc=1, device_id=other(k + 1), device_id_type=MESH)

    gains[...] = jnp.zeros(gains.shape, F32)
    halves = [ref[...].astype(F32).reshape(1, 64) for ref in (n1_ref, n2_ref)]
    gains[0:1, :] = jnp.concatenate(halves, axis=1)
    gains[1:2, :] = qn_ref[...].astype(F32).reshape(1, 128)
    gains[2:3, :] = kn_ref[...].astype(F32).reshape(1, 128)
    angle = jnp.broadcast_to(pos_ref[...].astype(F32), (T, T)).T[:, : HD // 2] * freq_ref[...]
    cos_half, sin_half = jnp.cos(angle), jnp.sin(angle)
    trig[z] = jnp.concatenate([cos_half, cos_half, -sin_half, sin_half], axis=1)
    pl.semaphore_wait(barrier, 15)

    def to_all(source, buf, number):
        @each(15)
        def _(k):
            pltpu.make_async_remote_copy(
                src_ref=source, dst_ref=buf.at[me], send_sem=one_send.at[number], recv_sem=one_recv.at[number],
                device_id=other(k + 1), device_id_type=MESH,
            ).start()

    def all_wait(buf, sem):
        fifteen = buf.at[pl.ds(0, 15)]
        pltpu.make_async_copy(fifteen, fifteen, sem).wait()

    to_all(gains, gbuf, norm_number)
    for item in p_qkv + p_o:
        item.begin()
    x_copy = near_copy(Z, x_ref, xp.at[mine])
    trig_copy = near_copy(Z, trig.at[z], trig.at[z])
    x_copy.start()
    own_x = pltpu.make_async_copy(x_ref, xp.at[mine], local_sem.at[len(parts)])
    own_x.start()
    for item in p_d + p_g + p_u:
        item.begin()
    trig_copy.start()
    dy_copy = near_copy(Z, dy_ref, dybuf.at[y, c, z])
    dy_copy.start()
    own_dy = pltpu.make_async_copy(dy_ref, dybuf.at[y, c, z], local_sem.at[len(parts) + 1])
    own_dy.start()
    for item in p_qkv + p_o:
        item.advance(0)
    gq, gk = gains[1:2, :], gains[2:3, :]
    all_wait(gbuf, one_recv.at[norm_number])
    gbuf[me] = gains[...]
    lane = lax.broadcasted_iota(jnp.int32, (8, 128), 1) < 64
    for i in range(8):
        first, second = gbuf[2 * i], gbuf[2 * i + 1]
        tile = slice(128 * i, 128 * i + 128)
        g1[:, tile] = jnp.where(lane, first, pltpu.roll(second, 64, axis=1))[:1]
        g2[:, tile] = jnp.where(lane, pltpu.roll(first, 64, axis=1), second)[:1]
    own_x.wait()
    x_copy.wait_recv()

    @each(8)
    def _(i):
        rows = cols(i, 32)
        val = xp[rows].astype(F32)
        n_s[rows] = (val * rms(val) * g1[...]).astype(BF16)

    def turned(val):
        return val.astype(F32).T.astype(BF16)

    for item in p_qkv:
        item.advance(1)
    for item in p_d:
        item.advance(0)

    @each(4)
    def _(i):
        nbuf[y, c, cols(i, 256)] = turned(n_s[:, cols(i, 256)])

    for item in p_o:
        item.advance(1)
    for item in p_g + p_u:
        item.advance(0)
    for item in p_qkv:
        item.advance(2)
    trig_copy.wait_recv()

    def weight(buf, tile):
        block = buf[(ALL,) * (len(buf.shape) - 1) + (tile,)]
        return block.reshape(-1, block.shape[-1])

    def project(buf, dst, width, tiles):
        @each(tiles)
        def _(j):
            tile = cols(j, width)
            dst[:, tile] = nn(n_s[...], weight(buf, tile)).astype(BF16)

    for item in p_qkv:
        item.arrived()
    project(bq, q_s, 512, 2)
    project(bk, k_s, 512, 1)
    project(bv, v_s, 512, 1)
    scale = HD ** -0.5

    def sequence_head(j):
        seq, head = lax.div(j, 4), lax.rem(j, 4)
        return seq, head, cols(seq, T), cols(head, HD), cols(head, 2 * HD)

    @each(8)
    def _(j):
        seq, _, rows, kv, pair = sequence_head(j)
        cos, sin = trig[seq, :, :HD], trig[seq, :, HD:]
        k_rot = head_forward(k_s[rows, kv], gk, cos, sin)
        kr[rows, kv] = k_rot
        q_pair = q_s[rows, pair]
        q_rot = jnp.concatenate(
            [head_forward(half, gq, cos, sin) for half in (q_pair[:, :HD], q_pair[:, HD:])], axis=0
        )
        qr[j] = q_rot
        scores = nt(q_rot, k_rot) * scale
        row = lax.rem(lax.broadcasted_iota(jnp.int32, (2 * T, T), 0), T)
        col = lax.broadcasted_iota(jnp.int32, (2 * T, T), 1)
        scores = jnp.where(row >= col, scores, -1e30)
        expd = jnp.exp(scores - jnp.max(scores, axis=-1, keepdims=True))
        prob = expd / jnp.sum(expd, axis=-1, keepdims=True)
        probs[j] = prob
        out = nn(prob.astype(BF16), v_s[rows, kv])
        ctx[rows, pair] = jnp.concatenate([out[:T], out[T:]], axis=1).astype(BF16)

    def pair_sum(partial, landing, compute):
        copies = []
        for half in range(2):
            @each(2)
            def _(j):
                i = j + 2 * half
                partial[:, :, cols(i, 256)] = compute(i).reshape(2, T, 256)

            span = (ALL, pl.ds(512 * half, 512))
            copies.append(near_copy(Z, partial.at[(1 - z,) + span], landing.at[span]))
            copies[-1].start()
        return copies

    def received(copies):
        for copy in copies:
            copy.wait_recv()

    for item in p_o:
        item.arrived()
    a_copies = pair_sum(part_a, land_a, lambda i: nn(ctx[...], weight(bo, cols(i, 256))))
    for item in p_g + p_u:
        item.advance(1)
    for item in p_d:
        item.advance(1)

    @each(4)
    def _(i):
        ct_ref[two(i)] = turned(ctx[:, cols(i, 256)]).reshape(2, 128, 2 * T)

    received(a_copies)

    @each(4)
    def _(i):
        rows = cols(i, 32)
        attn = (part_a[z, rows] + land_a[rows]).astype(BF16)
        val = (xp[pair_rows(i)].astype(F32) + attn.astype(F32)).astype(BF16).astype(F32)
        h_s[rows] = val
        m_s[pair_rows(i)] = (val * rms(val) * g2[...]).astype(BF16)

    m_copy = near_copy(Z, m_s.at[mine], m_s.at[mine])
    m_copy.start()
    for item in p_d:
        item.arrived()
    own_dy.wait()
    dy_copy.wait_recv()

    @each(4)
    def _(i):
        dact[:, cols(i, 384)] = nt(dybuf[y, c].reshape(2 * T, D), bd[two(i)].reshape(384, D))

    m_copy.wait_recv()

    @each(4)
    def _(i):
        mbuf[x, c, cols(i, 256)] = turned(m_s[:, cols(i, 256)])

    for item in p_g + p_u:
        item.advance(2)
    p_m.begin()
    p_dy.begin()
    e_c.begin()
    for item in p_g + p_u:
        item.arrived()
    fh = FF // 2

    @each(fh // 256)
    def _(j):
        tile = cols(j, 256)
        gate_val = nn(m_s[...], weight(bg, tile)).astype(BF16).astype(F32)
        up_val = nn(m_s[...], weight(bu, tile)).astype(BF16).astype(F32)
        sig = jax.nn.sigmoid(gate_val)
        act[:, tile] = (gate_val * sig * up_val).astype(BF16)
        d_act = dact[:, tile]
        dgu[:, tile] = (d_act * up_val * sig * (1.0 + gate_val * (1.0 - sig))).astype(BF16)
        dgu[:, cols(j + fh // 256, 256)] = (d_act * gate_val * sig).astype(BF16)

    def d_mlp_in(i):
        rows = two(i)
        return nt(dgu[:, :fh], bg[rows].reshape(256, fh)) + nt(dgu[:, fh:], bu[rows].reshape(256, fh))

    e_gu.begin()
    m_copies = pair_sum(part_m, land_m, d_mlp_in)

    @each(4)
    def _(i):
        at_ref[two(i)] = turned(act[:, cols(i, 384)]).reshape(2, 192, 2 * T)

    e_a.begin()
    p_n.begin()
    received(m_copies)

    def d_res_rows(i, total):
        rows = cols(i, 32)
        val = h_s[rows]
        r_scale = rms(val)
        unit = val * r_scale
        grad = part_m[z, rows] + land_m[rows]
        out = dybuf[y, c, z, rows].astype(F32) + norm_backward(grad * g2[...], unit, r_scale)
        dres[rows] = out
        drbuf[x, c, z, rows] = out.astype(BF16)
        return total + jnp.sum(grad * unit, axis=0, keepdims=True)

    d_g2 = loop(4, d_res_rows, jnp.zeros((1, D), F32))
    r_copy = near_copy(Z, drbuf.at[x, c, z], drbuf.at[x, c, z])
    r_copy.start()
    y_copies = pair_sum(part_y, land_y, lambda i: nn(act[...], weight(bd, cols(i, 256))))
    inv_tokens = 1.0 / (16 * T)

    def row_tiles(left_buf, right_buf, out):
        @each(8)
        def _(j):
            tile = cols(lax.rem(j, 4), 256)
            half = lax.div(j, 4)
            left = jnp.concatenate([left_buf[i, half] for i in range(4)], axis=1)
            out[half, :, tile] = nn(left, weight(right_buf, tile)) * inv_tokens

    p_dy.advance(0)
    p_dy.arrived()
    e_a.arrived()
    row_tiles(abuf, dybuf, rwd)
    r_copy.wait_recv()
    p_dr.begin()
    wd_far = near_copy(X, rwd.at[1 - x], zwd)
    wd_far.start()

    @each(2)
    def _(i):
        dctx[:, cols(i, 512)] = nt(drbuf[x, c].reshape(2 * T, D), bo[i].reshape(512, D)).astype(BF16)

    def attend_back(j, carry):
        q_total, k_total = carry
        seq, head, rows, kv, pair = sequence_head(j)
        cos, sin = trig[seq, :, :HD], trig[seq, :, HD:]
        d_out = dctx[rows, pair]
        d_out = jnp.concatenate([d_out[:, :HD], d_out[:, HD:]], axis=0)
        prob = probs[j]
        d_value = tn(prob.astype(BF16), d_out).astype(BF16)
        d_prob = nt(d_out, v_s[rows, kv])
        d_score = prob * (d_prob - jnp.sum(prob * d_prob, axis=-1, keepdims=True))
        d_score = (d_score * scale).astype(BF16)
        d_q_rot = nn(d_score, kr[rows, kv])
        d_k_rot = tn(d_score, qr[j])
        q_pair = q_s[rows, pair]
        d_q0, g_q0 = head_backward(d_q_rot[:T], q_pair[:, :HD], gq, cos, sin)
        d_q1, g_q1 = head_backward(d_q_rot[T:], q_pair[:, HD:], gq, cos, sin)
        d_k, g_k = head_backward(d_k_rot, k_s[rows, kv], gk, cos, sin)
        dqkv[rows, pair] = jnp.concatenate([d_q0, d_q1], axis=1)
        dqkv[rows, cols(head + 8, HD)] = d_k
        dqkv[rows, cols(head + 12, HD)] = d_value
        return q_total + g_q0 + g_q1, k_total + g_k

    zero = jnp.zeros((1, HD), F32)
    q_total, k_total = loop(8, attend_back, (zero, zero))
    e_qkv.begin()

    def d_normed(i):
        rows = two(i)
        grad = nt(dqkv[:, :D], bq[rows].reshape(256, D)) + nt(dqkv[:, D : D + 512], bk[rows].reshape(256, 512))
        return grad + nt(dqkv[:, D + 512 :], bv[rows].reshape(256, 512))

    n_copies = pair_sum(part_n, land_n, d_normed)

    def column_chunk(acts, grads, out, chunk):
        @each(8)
        def _(i):
            rows = cols(i, 128)
            left = jnp.concatenate([acts[k // 2, k % 2, rows] for k in range(4)], axis=1)
            right = grads[:, :, 256 * chunk : 256 * chunk + 256].reshape(8 * T, 256)
            out[(chunk,) + three(i)] = (nn(left, right) * inv_tokens).reshape(2, 64, 256)

    def half_of(dim, result, chunk):
        bit = place.bit[dim]
        return result.at[(chunk,) + tuple(1 - bit if k == dim else ALL for k in range(4))]

    p_m.advance(0)
    p_m.arrived()
    e_gu.arrived()
    gu_far = []
    for chunk in range(3):
        column_chunk(mbuf, gubuf, rgu, chunk)
        gu_far.append(near_copy(Y, half_of(Y, rgu, chunk), zgu.at[chunk]))
        gu_far[-1].start()
    p_dr.advance(0)
    p_dr.arrived()
    e_c.arrived()
    row_tiles(cbuf, drbuf, rwo)
    wo_far = near_copy(Y, rwo.at[1 - y], zwo)
    wo_far.start()
    p_n.advance(0)
    p_n.arrived()
    e_qkv.arrived()
    qkv_far = []
    for chunk in range(2):
        column_chunk(nbuf, qkvbuf, rqkv, chunk)
        qkv_far.append(near_copy(X, half_of(X, rqkv, chunk), zqkv.at[chunk]))
        qkv_far[-1].start()
    received(n_copies)

    def d_hidden_rows(i, total):
        rows = cols(i, 32)
        val = xp[pair_rows(i)].astype(F32)
        x_scale = rms(val)
        unit = val * x_scale
        grad = part_n[z, rows] + land_n[rows]
        dh_ref[rows] = (dres[rows] + norm_backward(grad * g1[...], unit, x_scale)).astype(BF16)
        return total + jnp.sum(grad * unit, axis=0, keepdims=True)

    d_g1 = loop(4, d_hidden_rows, jnp.zeros((1, D), F32))
    leave(dh_ref, dh_out)
    gpart[...] = jnp.zeros(gpart.shape, F32)
    for i in range(8):
        tile = slice(128 * i, 128 * i + 128)
        gpart[i : i + 1, :] = d_g1[:, tile]
        gpart[8 + i : 9 + i, :] = d_g2[:, tile]
    gpart[16:17, :] = q_total
    gpart[17:18, :] = k_total

    to_all(gpart, gainbuf, gain_number)
    received(y_copies)

    @each(4)
    def _(i):
        rows = cols(i, 32)
        out = (part_y[z, rows] + land_y[rows]).astype(BF16).astype(F32)
        y_ref[rows] = (h_s[rows] + out).astype(BF16)

    leave(y_ref, y_out)

    def final(dim, number, result, target, out, chunk, base):
        group = Group(place, tuple(k for k in range(4) if k != dim))
        for bit in list(group.others()) + [place.bit]:
            index = (chunk,) + tuple(bit)
            result[index] = result[index] + target[(chunk,) + tuple(bit[k] for k in group.axes)]
        where = pl.ds(pl.multiple_of(base + 256 * chunk, 128), 256)
        move = Exchange(
            group, number, lambda bit: result.at[(chunk,) + tuple(bit)], out.at[:, where],
            out.at[:, pl.ds(0, 7 * 256)], one,
        )
        move.begin()
        return move

    gu_base = x * FF + z * fh + c * 768
    qkv_base = (1 - y) * (z * D + c * 512) + y * (NQ + c * D + z * 512)
    moves = []
    for kind, chunk in ((0, 0), (1, 0), (0, 1), (1, 1), (0, 2)):
        if kind == 0:
            gu_far[chunk].wait_recv()
            moves.append(final(Y, 4 + chunk, rgu, zgu, ogu, chunk, gu_base))
        else:
            qkv_far[chunk].wait_recv()
            moves.append(final(X, 7 + chunk, rqkv, zqkv, oqkv, chunk, qkv_base))
    wd_far.wait_recv()
    owd[...] = rwd[x] + zwd[...]
    leave(owd, wd_out)
    wo_far.wait_recv()
    owo[...] = rwo[y] + zwo[...]
    leave(owo, wo_out)
    all_wait(gainbuf, one_recv.at[gain_number])
    gainbuf[me] = gpart[...]
    gainbuf[0] = loop(16, lambda i, total: total + gainbuf[i], jnp.zeros((24, 128), F32)) * inv_tokens
    for i in range(2):
        row = gainbuf[0, pl.ds(8 * i + lax.div(me, 2), 1), :]
        ogain[i : i + 1, :] = jnp.where(c == 0, row, pltpu.roll(row, 64, axis=1))
    ogain[2:4, :] = gainbuf[0, 16:18, :]
    ogain[4:8, :] = jnp.zeros((4, 128), F32)
    leave(ogain, gain_out)
    for move in moves:
        move.arrived()
    for item in moves + [e_gu, e_qkv, e_a, e_c] + parts:
        item.drain()
    for copy in sent:
        copy.wait_send()
    for copy in leaving:
        copy.wait()
    all_wait(gainbuf, one_send.at[gain_number])
    all_wait(gbuf, one_send.at[norm_number])


def shape(rows, width, dtype):
    return jax.ShapeDtypeStruct((rows, width), dtype)


def many(count, *args):
    return [VM(*args)] * count


def layer_call(*operands):
    vmem = pl.BlockSpec(memory_space=VM)
    hbm = pl.BlockSpec(memory_space=pl.ANY)
    dma = pltpu.SemaphoreType.DMA
    t2, kvh, fh = 2 * T, D // 2, FF // 2
    cube, square, line = (2, 2, 2, 2), (2, 2, 2), (2, 2)
    spreads = 18
    return pl.pallas_call(
        layer_kernel,
        name="layer",
        out_shape=(
            shape(T, D, BF16), shape(T, D, BF16), shape(64, NQ + 2 * D, F32), shape(64, 2 * FF, F32),
            shape(128, D, F32), shape(192, D, F32), shape(8, 128, F32),
        ),
        in_specs=[vmem] * 6 + [hbm] * 9,
        out_specs=(hbm,) * 7,
        scratch_shapes=[
            *many(2, (T, D), BF16), VM((T, D), F32), VM((192, D), F32), VM((8, 128), F32),
            VM((8, 128), F32), VM((16, 8, 128), F32), VM(cube + (64, D), BF16), *many(2, cube + (64, kvh), BF16),
            VM(square + (128, D), BF16), *many(2, cube + (64, fh), BF16), VM(square + (192, D), BF16),
            *many(2, (1, D), F32),
            VM((t2, D), BF16), VM((2, T, t2), F32), VM((t2, D), BF16), VM((t2, D), BF16), *many(2, (t2, kvh), BF16),
            VM((8, t2, HD), BF16), VM((t2, kvh), BF16), VM((8, t2, T), F32), VM((t2, D), BF16), VM((T, D), F32),
            VM((t2, D), BF16), VM((8, 128), BF16), VM((t2, fh), BF16), VM((t2, fh), F32), VM((t2, D), BF16),
            VM((T, D), F32), *many(4, (2, T, D), F32), *many(4, (T, D), F32),
            VM(square + (192, t2), BF16), VM(square + (128, t2), BF16), VM((t2, NQ), BF16), VM((t2, FF), BF16),
            VM((24, 128), F32), *many(2, line + (D, t2), BF16), *many(2, line + (2, T, D), BF16),
            VM((4, t2, 768), BF16), VM((4, t2, 512), BF16), VM((4, 2, 192, t2), BF16), VM((4, 2, 128, t2), BF16),
            VM((3,) + cube + (64, 256), F32), VM((2,) + cube + (64, 256), F32), VM((2, 192, D), F32),
            VM((2, 128, D), F32), VM((3,) + square + (64, 256), F32), VM((2,) + square + (64, 256), F32),
            VM((192, D), F32), VM((128, D), F32), VM((16, 24, 128), F32),
            *[dma((spreads, 3))] * 2, *[dma((spreads, 4))] * 2, dma((spreads + 7,)), *[dma((11,))] * 3, *[dma((20,))] * 2,
        ],
        compiler_params=pltpu.CompilerParams(collective_id=0, has_side_effects=True, vmem_limit_bytes=HIGH_VMEM),
    )(*operands)


def deliver_kernel(y_in, dh_in, qkv_in, gu_in, wo_in, wd_in, gain_in, *refs):
    rest = iter(refs)
    outs, small_outs, scratch, small = ([next(rest) for _ in range(count)] for count in (9, 4, 9, 4))
    gain, in_sem, out_sem = rest
    spans = ((qkv_in, 0, NQ), (qkv_in, NQ, D), (qkv_in, NQ + D, D), (gu_in, 0, FF), (gu_in, FF, FF))
    q_in, k_in, v_in, g_in, u_in = (ref.at[:, pl.ds(start, size)] for ref, start, size in spans)
    sources = (gain_in, y_in, dh_in, q_in, k_in, v_in, wo_in, g_in, u_in, wd_in)
    buffers = [gain] + scratch
    loads = [pltpu.make_async_copy(src, buf, in_sem.at[i]) for i, (src, buf) in enumerate(zip(sources, buffers))]
    pairs = zip(small + scratch, small_outs + outs)
    stores = [pltpu.make_async_copy(buf, out, out_sem.at[i]) for i, (buf, out) in enumerate(pairs)]
    for load in loads:
        load.start()
    loads[0].wait()
    for i, (buf, store) in enumerate(zip(small, stores)):
        buf[...] = gain[i : i + 1, : buf.shape[0]].reshape(buf.shape)
        store.start()
    for load, store in zip(loads[1:], stores[len(small) :]):
        load.wait()
        store.start()
    for store in stores:
        store.wait()


def deliver(*results):
    hbm = pl.BlockSpec(memory_space=pl.ANY)
    dma = pltpu.SemaphoreType.DMA
    sizes = [(T, D, BF16)] * 2 + [(64, width, F32) for width in (NQ, D, D)] + [(128, D, F32)]
    sizes += [(64, FF, F32)] * 2 + [(192, D, F32)]
    small = (64, 64, 128, 128)
    scratch = [VM(size[:2], size[2]) for size in sizes] + [VM((size,), F32) for size in small]
    return pl.pallas_call(
        deliver_kernel,
        name="deliver",
        out_shape=tuple([shape(*size) for size in sizes] + [jax.ShapeDtypeStruct((size,), F32) for size in small]),
        in_specs=[hbm] * len(results),
        out_specs=(hbm,) * len(scratch),
        scratch_shapes=scratch + [VM((8, 128), F32), dma((16,)), dma((16,))],
    )(*results)


def solution(mesh):
    axis_name = mesh.axis_names[0]
    sharded = P(axis_name)
    in_specs = (sharded,) * 5 + (P(), P()) + (sharded,) * 7
    out_specs = (sharded,) * 4 + (P(), P()) + (sharded,) * 7

    def device_step(hidden, grad_out, positions, norm1, norm2, gain_q, gain_k, w_q, w_k, w_v, w_o, w_gate, w_up, w_down):
        inv_freq = ROPE_THETA ** (-2.0 * jnp.arange(HD // 2, dtype=F32) / HD)
        x, dy = hidden.reshape(T, D), grad_out.reshape(T, D)
        results = layer_call(positions, inv_freq[None, :], norm1, norm2, gain_q, gain_k, x, dy, w_q, w_k, w_v, w_o, w_gate, w_up, w_down)
        out, d_hidden, d_wq, d_wk, d_wv, d_wo, d_wg, d_wu, d_wd, d_n1, d_n2, d_qn, d_kn = deliver(*results)
        out, d_hidden = out.reshape(hidden.shape), d_hidden.reshape(hidden.shape)
        return out, d_hidden, d_n1, d_n2, d_qn, d_kn, d_wq, d_wk, d_wv, d_wo, d_wg, d_wu, d_wd

    return jax.shard_map(device_step, mesh=mesh, in_specs=in_specs, out_specs=out_specs, check_vma=False)
```
